64 devices in a mesh: dp: 4 (over x, y), cp: 16 (over z, core).
Axes of the slice: x: 2, y: 2, z: 8, core: 2. Of those that a mesh axis runs over, the one named last changes fastest.
The devices are a block of a 4x4x8 slice.
Arguments:
- x_in: bfloat16 [24, 2048, 2304], P('dp', 'cp'), parts along dimension 0
- ln_w: bfloat16 [2, 4, 2304], replicated
- qk_w: bfloat16 [2, 2, 256], replicated
- w_q: bfloat16 [2, 2304, 2048], replicated
- w_k: bfloat16 [2, 2304, 1024], replicated
- w_v: bfloat16 [2, 2304, 1024], replicated
- w_o: bfloat16 [2, 2048, 2304], replicated
- w_gate: bfloat16 [2, 2304, 9216], replicated
- w_up: bfloat16 [2, 2304, 9216], replicated
- w_down: bfloat16 [2, 9216, 2304], replicated
Outputs:
- output: bfloat16 [24, 2048, 2304], P('dp', 'cp'), parts along dimension 0
There are 4 independent parts. The reference program is written for one: setup_inputs(seed, part) draws one part's arguments, and reference() takes and returns one part's arrays. A program takes and returns all parts, laid end to end along the dimension named above; an argument that names none is the same for every part.
All inputs are finite; a program needn't handle non-finite values.
Results may differ from the reference program's by a relative error of at most 0.02.
Values are sent between devices in bfloat16 or wider.
A program may use at most 768 MiB of HBM per device.

```python
import jax
import jax.numpy as jnp
from jax import lax

BATCH = 6
TOK_DEV = 128
SEQ_LEN = 2048
D_MODEL = 2304
N_HEADS = 8
KV_HEADS = 4
HEAD_DIM = 256
FF_DIM = 9216
WINDOW = 1024
N_BLOCKS = SEQ_LEN // TOK_DEV
NORM_EPS = 1e-6
LOCAL_BASE = 10000.0
GLOBAL_BASE = 1000000.0
GLOBAL_SCALE = 8.0


def setup_inputs(seed: int = 0, part: int = 0) -> dict:
    base_key = jax.random.key(seed)
    part_key = jax.random.fold_in(base_key, part)
    w_keys = jax.random.split(base_key, 9)
    q_dim = N_HEADS * HEAD_DIM
    kv_dim = KV_HEADS * HEAD_DIM

    def scaled_normal(rng_key, arr_shape, fan_in):
        return (jax.random.normal(rng_key, arr_shape, jnp.float32) * fan_in ** -0.5).astype(jnp.bfloat16)

    x_in = jax.random.normal(part_key, (BATCH, SEQ_LEN, D_MODEL), jnp.float32).astype(jnp.bfloat16)
    ln_w = (0.3 * jax.random.normal(w_keys[0], (2, 4, D_MODEL), jnp.float32)).astype(jnp.bfloat16)
    qk_w = (0.3 * jax.random.normal(w_keys[1], (2, 2, HEAD_DIM), jnp.float32)).astype(jnp.bfloat16)
    return {
        "x_in": x_in,
        "ln_w": ln_w,
        "qk_w": qk_w,
        "w_q": scaled_normal(w_keys[2], (2, D_MODEL, q_dim), D_MODEL),
        "w_k": scaled_normal(w_keys[3], (2, D_MODEL, kv_dim), D_MODEL),
        "w_v": scaled_normal(w_keys[4], (2, D_MODEL, kv_dim), D_MODEL),
        "w_o": scaled_normal(w_keys[5], (2, q_dim, D_MODEL), q_dim),
        "w_gate": scaled_normal(w_keys[6], (2, D_MODEL, FF_DIM), D_MODEL),
        "w_up": scaled_normal(w_keys[7], (2, D_MODEL, FF_DIM), D_MODEL),
        "w_down": scaled_normal(w_keys[8], (2, FF_DIM, D_MODEL), FF_DIM),
    }


def rms_scale(values_in, gain):
    vals_f32 = values_in.astype(jnp.float32)
    inv_rms = lax.rsqrt(jnp.mean(vals_f32 * vals_f32, axis=-1, keepdims=True) + NORM_EPS)
    return vals_f32 * inv_rms * (1.0 + gain.astype(jnp.float32))


def rope_apply(head_vals, positions, rope_base, pos_scale):
    half_dim = HEAD_DIM // 2
    inv_freq = rope_base ** (-2.0 * jnp.arange(half_dim, dtype=jnp.float32) / HEAD_DIM)
    ang_all = (positions.astype(jnp.float32) / pos_scale)[:, None] * inv_freq[None, :]
    cos_ang = jnp.cos(ang_all)[:, None, :]
    sin_ang = jnp.sin(ang_all)[:, None, :]
    first_half = head_vals[..., :half_dim]
    second_half = head_vals[..., half_dim:]
    return jnp.concatenate([first_half * cos_ang - second_half * sin_ang, second_half * cos_ang + first_half * sin_ang], axis=-1)


def dense(act_vals, weight):
    flat_acts = act_vals.reshape(-1, act_vals.shape[-1])
    prod_f32 = jnp.dot(flat_acts, weight, preferred_element_type=jnp.float32)
    return prod_f32.reshape(act_vals.shape[:-1] + (weight.shape[-1],))


def layer_ref(x_all, params, window, rope_base, pos_scale):
    ln_w, qk_w, w_q, w_k, w_v, w_o, w_gate, w_up, w_down = params
    groups = N_HEADS // KV_HEADS
    positions = jnp.arange(SEQ_LEN)
    a_all = rms_scale(x_all, ln_w[0]).astype(jnp.bfloat16)
    k_raw = dense(a_all, w_k).astype(jnp.bfloat16).reshape(BATCH, SEQ_LEN, KV_HEADS, HEAD_DIM)
    k_ready = rope_apply(rms_scale(k_raw, qk_w[1]), positions, rope_base, pos_scale).astype(jnp.bfloat16)
    v_all = dense(a_all, w_v).astype(jnp.bfloat16).reshape(BATCH, SEQ_LEN, KV_HEADS, HEAD_DIM)

    def block_fn(blk_idx):
        blk_start = blk_idx * TOK_DEV
        x_blk = lax.dynamic_slice_in_dim(x_all, blk_start, TOK_DEV, axis=1)
        a_blk = lax.dynamic_slice_in_dim(a_all, blk_start, TOK_DEV, axis=1)
        q_pos = blk_start + jnp.arange(TOK_DEV)
        q_raw = dense(a_blk, w_q).astype(jnp.bfloat16).reshape(BATCH, TOK_DEV, N_HEADS, HEAD_DIM)
        q_ready = rope_apply(rms_scale(q_raw, qk_w[0]), q_pos, rope_base, pos_scale).astype(jnp.bfloat16)
        q_ready = q_ready.reshape(BATCH, TOK_DEV, KV_HEADS, groups, HEAD_DIM)
        scores = jnp.einsum("btgrd,bugd->bgrtu", q_ready.astype(jnp.float32), k_ready.astype(jnp.float32)) * HEAD_DIM ** -0.5
        pos_diff = q_pos[:, None] - positions[None, :]
        keep_mask = (pos_diff >= 0) & (pos_diff < window)
        scores = jnp.where(keep_mask, scores, -1e30)
        attn_probs = jax.nn.softmax(scores, axis=-1).astype(jnp.bfloat16)
        attn_o = jnp.einsum("bgrtu,bugd->btgrd", attn_probs.astype(jnp.float32), v_all.astype(jnp.float32)).astype(jnp.bfloat16)
        attn_o = attn_o.reshape(BATCH, TOK_DEV, N_HEADS * HEAD_DIM)
        attn_out = dense(attn_o, w_o).astype(jnp.bfloat16)
        x_mid = (x_blk.astype(jnp.float32) + rms_scale(attn_out, ln_w[1])).astype(jnp.bfloat16)
        ffn_in = rms_scale(x_mid, ln_w[2]).astype(jnp.bfloat16)
        gate_val = dense(ffn_in, w_gate)
        up_val = dense(ffn_in, w_up)
        act_val = (jax.nn.gelu(gate_val, approximate=True) * up_val).astype(jnp.bfloat16)
        mlp_out = dense(act_val, w_down).astype(jnp.bfloat16)
        return (x_mid.astype(jnp.float32) + rms_scale(mlp_out, ln_w[3])).astype(jnp.bfloat16)

    out_blocks = lax.map(block_fn, jnp.arange(N_BLOCKS))
    return jnp.moveaxis(out_blocks, 0, 1).reshape(BATCH, SEQ_LEN, D_MODEL)


def reference(x_in, ln_w, qk_w, w_q, w_k, w_v, w_o, w_gate, w_up, w_down):
    stacked = (ln_w, qk_w, w_q, w_k, w_v, w_o, w_gate, w_up, w_down)
    first_params = tuple(weight_arr[0] for weight_arr in stacked)
    second_params = tuple(weight_arr[1] for weight_arr in stacked)
    x_mid = layer_ref(x_in, first_params, WINDOW, LOCAL_BASE, 1.0)
    return layer_ref(x_mid, second_params, SEQ_LEN, GLOBAL_BASE, GLOBAL_SCALE)
```

```python
import functools

import jax
import jax.numpy as jnp
from jax import lax
from jax.experimental import pallas as pl
from jax.experimental.pallas import tpu as pltpu
from jax.sharding import PartitionSpec as P

WINDOW = 1024
NORM_EPS = 1e-6
LOCAL_BASE = 10000.0
GLOBAL_BASE = 1000000.0
GLOBAL_SCALE = 8.0
NEG = -1e30

ROW_CHIP = (0, 3, 4, 1, 5, 6)
SPECIAL = (2, 7)
VMEM_LIMIT = 64 * 1024 * 1024 - 128 * 1024


def pick(idx, table):
    out = jnp.int32(table[-1])
    for i in range(len(table) - 2, -1, -1):
        out = jnp.where(idx == i, jnp.int32(table[i]), out)
    return out


def placement():
    me = lax.axis_index("cp")
    chip, core = me // 2, me % 2
    roles = [0] * 8
    rows = [0] * 8
    for b, c in enumerate(ROW_CHIP):
        rows[c] = b
    for i, c in enumerate(SPECIAL):
        roles[c] = 1
        rows[c] = 3 * i
    return me, chip, core, pick(chip, roles), pick(chip, rows)


def slot_place(s, core, special, row):
    k = s % 2
    blk = jnp.where(special == 1, 2 * k + (k + core) % 2, 4 + 2 * s + (s + core) % 2)
    b = jnp.where(special == 1, row + s // 2, row)
    return b, blk


def home_of(b, blk):
    core = ((blk + 1) // 2) % 2
    half = blk // 2
    chip = jnp.where(blk < 4, SPECIAL[b // 3], ROW_CHIP[b])
    slot = jnp.where(blk < 4, (b % 3) * 2 + half, half - 2)
    return chip * 2 + core, slot


def group_barrier(n_dev):
    me = lax.axis_index("cp")
    barrier = pltpu.get_barrier_semaphore()
    for d in range(1, n_dev):
        dev = lax.rem(me + d, n_dev)
        pl.semaphore_signal(barrier, inc=1, device_id={"cp": dev}, device_id_type=pl.DeviceIdType.MESH)
    pl.semaphore_wait(barrier, n_dev - 1)


def remote(src, dst, send, recv, dev):
    return pltpu.make_async_remote_copy(
        src_ref=src, dst_ref=dst, send_sem=send, recv_sem=recv, device_id={"cp": dev},
        device_id_type=pl.DeviceIdType.MESH,
    )


def exchange_kernel(to_home, n_dev, x_ref, o_ref, buf, send, recv, sem):
    me, _, core, special, row = placement()
    n = x_ref.shape[0]
    homes = [home_of(b, me) for b in range(n)]
    places = [slot_place(s, core, special, row) for s in range(n)]
    places = [(blk, b) for b, blk in places]
    dest, origin = (homes, places) if to_home else (places, homes)
    for i, (dev, dst) in enumerate(dest):

        @pl.when(dev == me)
        def _():
            pltpu.make_async_copy(x_ref.at[i], buf.at[i], sem.at[i]).start()

    group_barrier(n_dev)
    for i, (dev, dst) in enumerate(dest):

        @pl.when(dev != me)
        def _():
            remote(x_ref.at[i], o_ref.at[dst], send.at[i], recv.at[dst], dev).start()

    for i, (dev, dst) in enumerate(dest):

        @pl.when(dev == me)
        def _():
            pltpu.make_async_copy(x_ref.at[i], buf.at[i], sem.at[i]).wait()
            pltpu.make_async_copy(buf.at[i], o_ref.at[dst], sem.at[i]).start()
            pltpu.make_async_copy(buf.at[i], o_ref.at[dst], sem.at[i]).wait()

    for i, (dev, _) in enumerate(origin):

        @pl.when(dev != me)
        def _():
            remote(x_ref.at[i], o_ref.at[i], send.at[i], recv.at[i], dev).wait_recv()

    for i, (dev, dst) in enumerate(dest):

        @pl.when(dev != me)
        def _():
            remote(x_ref.at[i], o_ref.at[dst], send.at[i], recv.at[dst], dev).wait_send()


def exchange(to_home, n_dev, x, cid):
    n = x.shape[0]
    dma = pltpu.SemaphoreType.DMA
    return pl.pallas_call(
        functools.partial(exchange_kernel, to_home, n_dev),
        out_shape=jax.ShapeDtypeStruct(x.shape, x.dtype),
        in_specs=[pl.BlockSpec(memory_space=pl.ANY)],
        out_specs=pl.BlockSpec(memory_space=pl.ANY),
        scratch_shapes=[pltpu.VMEM(x.shape, x.dtype), dma((n,)), dma((n,)), dma((n,))],
        compiler_params=pltpu.CompilerParams(collective_id=cid, has_side_effects=True),
    )(x)


def norm_rows(vals, gain):
    inv = lax.rsqrt(jnp.mean(vals * vals, axis=-1, keepdims=True) + NORM_EPS)
    return vals * inv * (1.0 + gain)


def qkv_kernel(layer, nq, nk, slots, x_ref, ln_ref, qk_ref, cos_ref, sin_ref, wq_ref, wk_ref, wv_ref, q_ref, k_ref, v_ref, a_ref):
    i = pl.program_id(0)
    rows = x_ref.shape[0] // slots
    hd = wq_ref.shape[-1]
    half = hd // 2

    @pl.when(i == 0)
    def _():
        gain = ln_ref[layer, 0:1, :].astype(jnp.float32)
        for s in range(slots):
            r = pl.ds(s * rows, rows)
            a_ref[r, :] = norm_rows(x_ref[r, :].astype(jnp.float32), gain).astype(jnp.bfloat16)

    def product(s, w_ref):
        return jnp.dot(a_ref[pl.ds(s * rows, rows), :], w_ref[0], preferred_element_type=jnp.float32).astype(jnp.bfloat16)

    def turned(s, w_ref, which):
        vals = norm_rows(product(s, w_ref).astype(jnp.float32), qk_ref[layer, which : which + 1, :].astype(jnp.float32))
        first, second = vals[:, :half], vals[:, half:]
        r = pl.ds(s * rows, rows)
        cos, sin = cos_ref[r, :], sin_ref[r, :]
        return jnp.concatenate([first * cos - second * sin, second * cos + first * sin], axis=-1).astype(jnp.bfloat16)

    @pl.when(i < nq)
    def _():
        for s in range(slots):
            q_ref[s, 0] = turned(s, wq_ref, 0) * jnp.bfloat16(hd**-0.5)

    @pl.when((i >= nq) & (i < nq + nk))
    def _():
        for s in range(slots):
            k_ref[s] = turned(s, wk_ref, 1)

    @pl.when(i >= nq + nk)
    def _():
        for s in range(slots):
            v_ref[s] = product(s, wv_ref)


def qkv(layer, x, ln_w, qk_w, cos, sin, w_q, w_k, w_v):
    slots, rows, dim = x.shape
    hd = qk_w.shape[-1]
    nq, nk = w_q.shape[-1] // hd, w_k.shape[-1] // hd
    x2 = x.reshape(slots * rows, dim)
    whole = lambda a: pl.BlockSpec(a.shape, lambda i: (0,) * a.ndim)
    at = lambda lo, n: (lambda i: jnp.clip(i - lo, 0, n - 1))
    iq, ik, iv = at(0, nq), at(nq, nk), at(nq + nk, nk)
    wspec = lambda f: pl.BlockSpec((1, dim, hd), lambda i: (layer, 0, f(i)))
    return pl.pallas_call(
        functools.partial(qkv_kernel, layer, nq, nk, slots),
        grid=(nq + 2 * nk,),
        in_specs=[whole(x2), whole(ln_w), whole(qk_w), whole(cos), whole(sin), wspec(iq), wspec(ik), wspec(iv)],
        out_specs=[
            pl.BlockSpec((slots, 1, rows, hd), lambda i: (0, iq(i), 0, 0)),
            pl.BlockSpec((slots, rows, hd), lambda i: (0, 0, ik(i))),
            pl.BlockSpec((slots, rows, hd), lambda i: (0, 0, iv(i))),
        ],
        out_shape=[
            jax.ShapeDtypeStruct((slots, nq, rows, hd), jnp.bfloat16),
            jax.ShapeDtypeStruct((slots, rows, nk * hd), jnp.bfloat16),
            jax.ShapeDtypeStruct((slots, rows, nk * hd), jnp.bfloat16),
        ],
        scratch_shapes=[pltpu.VMEM(x2.shape, jnp.bfloat16)],
        compiler_params=pltpu.CompilerParams(dimension_semantics=("arbitrary",), vmem_limit_bytes=VMEM_LIMIT),
    )(x2, ln_w, qk_w, cos, sin, w_q, w_k, w_v)


def attn_kernel(window_blocks, q_ref, k_ref, v_ref, o_ref, kbuf, vbuf, qbuf, obuf, acc, mx, sm, bias,
                qsem, ksem, vsem, ksend, vsend, fsend, krecv, vrecv, osem):
    me, chip, core, special, row = placement()
    mate = chip * 2 + (1 - core)
    slots, nq, rows, hd = q_ref.shape
    nk = k_ref.shape[-1] // hd
    rep = nq // nk
    tile = 2 * rows
    barrier = pltpu.get_barrier_semaphore()

    def tell(dev):
        pl.semaphore_signal(barrier, inc=1, device_id={"cp": dev}, device_id_type=pl.DeviceIdType.MESH)

    def buf_index(s, c):
        b, blk = slot_place(s, c, special, row)
        return jnp.where(special == 1, (s // 2) * 4 + blk, blk)

    serve_chip = [jnp.where(row == 0, ROW_CHIP[r], ROW_CHIP[r + 3]) for r in range(3)]
    my_special = jnp.where(row < 3, SPECIAL[0], SPECIAL[1]) * 2 + core

    for s in range(slots):
        idx = buf_index(s, core)
        pltpu.make_async_copy(k_ref.at[s], kbuf.at[idx], ksem.at[s]).start()
        pltpu.make_async_copy(v_ref.at[s], vbuf.at[idx], vsem.at[s]).start()
        pltpu.make_async_copy(q_ref.at[s], qbuf.at[s], qsem.at[s]).start()

    tell(mate)

    @pl.when(special == 1)
    def _():
        for r in range(3):
            tell(serve_chip[r] * 2 + core)
        pl.semaphore_wait(barrier, 4)

    @pl.when(special == 0)
    def _():
        tell(my_special)
        pl.semaphore_wait(barrier, 2)

    @pl.when(special == 1)
    def _():
        for k in range(2):
            for r in range(3):
                s = 2 * r + k
                blk = 2 * k + (k + core) % 2
                dev = serve_chip[r] * 2 + core
                remote(k_ref.at[s], kbuf.at[blk], ksend.at[1, s], krecv.at[blk], dev).start()
                remote(v_ref.at[s], vbuf.at[blk], vsend.at[1, s], vrecv.at[blk], dev).start()

    for s in range(slots):
        idx = buf_index(s, core)
        remote(k_ref.at[s], kbuf.at[idx], ksend.at[0, s], krecv.at[idx], mate).start()
        remote(v_ref.at[s], vbuf.at[idx], vsend.at[0, s], vrecv.at[idx], mate).start()

    qi = lax.broadcasted_iota(jnp.int32, (rows, tile), 0)
    ki = lax.broadcasted_iota(jnp.int32, (rows, tile), 1)
    bias[0] = jnp.zeros((rows, tile), jnp.float32)
    bias[1] = jnp.where(ki <= qi, 0.0, NEG)
    bias[2] = jnp.where(ki <= qi + rows, 0.0, NEG)
    bias[3] = jnp.where(ki > qi, 0.0, NEG)
    bias[4] = jnp.where(ki > qi + rows, 0.0, NEG)

    def one_tile(s, t, base, blk):
        last = blk // 2
        edge = jnp.where(t == last, 1 + blk % 2, 0)
        if window_blocks is not None:
            old = (blk - window_blocks) // 2
            edge = jnp.where((blk >= window_blocks) & (t == old), 3 + (blk - window_blocks) % 2, edge)
        off = bias[edge]
        off2 = jnp.concatenate([off] * rep, axis=0)
        kt = kbuf.at[pl.ds(base + 2 * t, 2)]
        vt = vbuf.at[pl.ds(base + 2 * t, 2)]
        for g in range(nk):
            u = s * nk + g
            q2 = qbuf[s, g * rep : (g + 1) * rep].reshape(rep * rows, hd)
            kk = kt[:, :, g * hd : (g + 1) * hd].reshape(tile, hd)
            vv = vt[:, :, g * hd : (g + 1) * hd].reshape(tile, hd)
            sc = lax.dot_general(q2, kk, (((1,), (1,)), ((), ())), preferred_element_type=jnp.float32) + off2
            m_old = mx[u][:, :1]
            m_new = jnp.maximum(m_old, jnp.max(sc, axis=-1, keepdims=True))
            p = jnp.exp(sc - m_new)
            alpha = jnp.exp(m_old - m_new)
            sm[u] = jnp.broadcast_to(alpha * sm[u][:, :1] + jnp.sum(p, axis=-1, keepdims=True), sm.shape[1:])
            mx[u] = jnp.broadcast_to(m_new, mx.shape[1:])
            acc[u] = alpha * acc[u] + jnp.dot(p.astype(jnp.bfloat16), vv, preferred_element_type=jnp.float32)

    def start_tile(blk):
        if window_blocks is None:
            return jnp.int32(0)
        return jnp.maximum(blk - window_blocks, 0) // 2

    mx[...] = jnp.full(mx.shape, NEG, jnp.float32)
    sm[...] = jnp.zeros(sm.shape, jnp.float32)
    acc[...] = jnp.zeros(acc.shape, jnp.float32)

    for s in range(slots):
        pltpu.make_async_copy(k_ref.at[s], kbuf.at[buf_index(s, core)], ksem.at[s]).wait()
        pltpu.make_async_copy(v_ref.at[s], vbuf.at[buf_index(s, core)], vsem.at[s]).wait()
        pltpu.make_async_copy(q_ref.at[s], qbuf.at[s], qsem.at[s]).wait()
    for s in range(slots):
        idx = buf_index(s, 1 - core)
        remote(k_ref.at[s], kbuf.at[idx], ksend.at[0, s], krecv.at[idx], mate).wait()
        remote(v_ref.at[s], vbuf.at[idx], vsend.at[0, s], vrecv.at[idx], mate).wait()

    @pl.loop(0, slots)
    def _(s):
        b, blk = slot_place(s, core, special, row)
        base = jnp.where(special == 1, (s // 2) * 4, 0)
        first = jnp.where(special == 1, 0, jnp.maximum(start_tile(blk), 2))

        @pl.loop(first, blk // 2 + 1)
        def _(t):
            one_tile(s, t, base, blk)

    @pl.when(special == 0)
    def _():
        mine = [2 * k + (k + core) % 2 for k in range(2)]
        theirs = [2 * k + (k + 1 - core) % 2 for k in range(2)]
        for k in range(2):
            blk = mine[k]
            remote(k_ref.at[k], kbuf.at[blk], fsend.at[0, k], krecv.at[blk], mate).wait_recv()
            remote(kbuf.at[blk], kbuf.at[blk], fsend.at[0, k], krecv.at[blk], mate).start()
            remote(v_ref.at[k], vbuf.at[blk], fsend.at[1, k], vrecv.at[blk], mate).wait_recv()
            remote(vbuf.at[blk], vbuf.at[blk], fsend.at[1, k], vrecv.at[blk], mate).start()
        for k in range(2):
            blk = theirs[k]
            remote(kbuf.at[blk], kbuf.at[blk], fsend.at[0, k], krecv.at[blk], mate).wait()
            remote(vbuf.at[blk], vbuf.at[blk], fsend.at[1, k], vrecv.at[blk], mate).wait()

        @pl.loop(0, slots)
        def _(s):
            _, blk = slot_place(s, core, special, row)

            @pl.loop(start_tile(blk), 2)
            def _(t):
                one_tile(s, t, 0, blk)

    @pl.when(special == 1)
    def _():
        for s in range(slots):
            remote(k_ref.at[s], kbuf.at[0], ksend.at[1, s], krecv.at[0], mate).wait_send()
            remote(v_ref.at[s], vbuf.at[0], vsend.at[1, s], vrecv.at[0], mate).wait_send()

    @pl.loop(0, slots)
    def _(s):
        for g in range(nk):
            u = s * nk + g
            out = (acc[u] / sm[u][:, :1]).astype(jnp.bfloat16)
            for h in range(rep):
                lo = (g * rep + h) * hd
                obuf[s, :, lo : lo + hd] = out[h * rows : (h + 1) * rows]

    copy = pltpu.make_async_copy(obuf, o_ref, osem)
    copy.start()
    copy.wait()


def attention(window, q, k, v, cid):
    slots, nq, rows, hd = q.shape
    nk = k.shape[-1] // hd
    blocks = 16
    units = slots * nk
    dma = pltpu.SemaphoreType.DMA
    any_spec = pl.BlockSpec(memory_space=pl.ANY)
    body = functools.partial(attn_kernel, None if window is None else window // rows)
    return pl.pallas_call(
        body,
        out_shape=jax.ShapeDtypeStruct((slots, rows, nq * hd), jnp.bfloat16),
        in_specs=[any_spec] * 3,
        out_specs=any_spec,
        scratch_shapes=[
            pltpu.VMEM((blocks, rows, nk * hd), jnp.bfloat16),
            pltpu.VMEM((blocks, rows, nk * hd), jnp.bfloat16),
            pltpu.VMEM(q.shape, jnp.bfloat16),
            pltpu.VMEM((slots, rows, nq * hd), jnp.bfloat16),
            pltpu.VMEM((units, nq // nk * rows, hd), jnp.float32),
            pltpu.VMEM((units, nq // nk * rows, 128), jnp.float32),
            pltpu.VMEM((units, nq // nk * rows, 128), jnp.float32),
            pltpu.VMEM((5, rows, 2 * rows), jnp.float32),
            dma((slots,)), dma((slots,)), dma((slots,)),
            dma((2, slots)), dma((2, slots)), dma((2, 2)),
            dma((blocks,)), dma((blocks,)), dma,
        ],
        compiler_params=pltpu.CompilerParams(collective_id=cid, has_side_effects=True, vmem_limit_bytes=VMEM_LIMIT),
    )(q, k, v)


def rope_tables(pos, hd):
    half = hd // 2
    out = []
    for base, scale in ((LOCAL_BASE, 1.0), (GLOBAL_BASE, GLOBAL_SCALE)):
        freq = base ** (-2.0 * jnp.arange(half, dtype=jnp.float32) / hd)
        ang = (pos.astype(jnp.float32) / scale)[:, None] * freq[None, :]
        out += [jnp.cos(ang), jnp.sin(ang)]
    return out


def solution(mesh):
    n_dev = mesh.shape["cp"]

    def device_fn(x_loc, ln_w, qk_w, w_q, w_k, w_v, w_o, w_gate, w_up, w_down):
        slots, rows, dim = x_loc.shape
        hd = qk_w.shape[-1]
        _, _, core, special, row = placement()
        blk = jnp.stack([slot_place(s, core, special, row)[1] for s in range(slots)])
        pos = (blk[:, None] * rows + jnp.arange(rows)[None, :]).reshape(-1)
        tables = rope_tables(pos, hd)

        def layer(x, l, window):
            q, k, v = qkv(l, x, ln_w, qk_w, tables[2 * l], tables[2 * l + 1], w_q, w_k, w_v)
            o = attention(window, q, k, v, 1 + l).reshape(slots * rows, -1)
            x2 = x.reshape(slots * rows, dim)
            f32 = jnp.float32
            gain = ln_w[l].astype(f32)
            att = jnp.dot(o, w_o[l], preferred_element_type=f32).astype(jnp.bfloat16)
            y = (x2.astype(f32) + norm_rows(att.astype(f32), gain[1])).astype(jnp.bfloat16)
            c = norm_rows(y.astype(f32), gain[2]).astype(jnp.bfloat16)
            gate = jnp.dot(c, w_gate[l], preferred_element_type=f32)
            up = jnp.dot(c, w_up[l], preferred_element_type=f32)
            act = (jax.nn.gelu(gate, approximate=True) * up).astype(jnp.bfloat16)
            m = jnp.dot(act, w_down[l], preferred_element_type=f32).astype(jnp.bfloat16)
            out = (y.astype(f32) + norm_rows(m.astype(f32), gain[3])).astype(jnp.bfloat16)
            return out.reshape(slots, rows, dim)

        x = exchange(True, n_dev, x_loc, 0)
        x = layer(x, 0, WINDOW)
        x = layer(x, 1, None)
        return exchange(False, n_dev, x, 3)

    act_part = P("dp", "cp", None)
    return jax.shard_map(device_fn, mesh=mesh, in_specs=(act_part,) + (P(),) * 9, out_specs=act_part, check_vma=False)
```

```python
import functools

import jax
import jax.numpy as jnp
from jax import lax
from jax.experimental import pallas as pl
from jax.experimental.pallas import tpu as pltpu
from jax.sharding import PartitionSpec as P

WINDOW = 1024
NORM_EPS = 1e-6
LOCAL_BASE = 10000.0
GLOBAL_BASE = 1000000.0
GLOBAL_SCALE = 8.0
NEG = -1e30

ROW_CHIP = (0, 3, 4, 1, 5, 6)
SPECIAL = (2, 7)
VMEM_LIMIT = 64 * 1024 * 1024 - 128 * 1024


def pick(idx, table):
    out = jnp.int32(table[-1])
    for i in range(len(table) - 2, -1, -1):
        out = jnp.where(idx == i, jnp.int32(table[i]), out)
    return out


def placement():
    me = lax.axis_index("cp")
    chip, core = me // 2, me % 2
    roles = [0] * 8
    rows = [0] * 8
    for b, c in enumerate(ROW_CHIP):
        rows[c] = b
    for i, c in enumerate(SPECIAL):
        roles[c] = 1
        rows[c] = 3 * i
    return me, chip, core, pick(chip, roles), pick(chip, rows)


def slot_place(s, core, special, row):
    k = s % 2
    blk = jnp.where(special == 1, 2 * k + (k + core) % 2, 4 + 2 * s + (s + core) % 2)
    b = jnp.where(special == 1, row + s // 2, row)
    return b, blk


def home_of(b, blk):
    core = ((blk + 1) // 2) % 2
    half = blk // 2
    chip = jnp.where(blk < 4, SPECIAL[b // 3], ROW_CHIP[b])
    slot = jnp.where(blk < 4, (b % 3) * 2 + half, half - 2)
    return chip * 2 + core, slot


def group_barrier(n_dev):
    me = lax.axis_index("cp")
    barrier = pltpu.get_barrier_semaphore()
    for d in range(1, n_dev):
        dev = lax.rem(me + d, n_dev)
        pl.semaphore_signal(barrier, inc=1, device_id={"cp": dev}, device_id_type=pl.DeviceIdType.MESH)
    pl.semaphore_wait(barrier, n_dev - 1)


def remote(src, dst, send, recv, dev):
    return pltpu.make_async_remote_copy(
        src_ref=src, dst_ref=dst, send_sem=send, recv_sem=recv, device_id={"cp": dev},
        device_id_type=pl.DeviceIdType.MESH,
    )


def exchange_kernel(to_home, n_dev, x_ref, o_ref, buf, send, recv, sem):
    me, _, core, special, row = placement()
    n = x_ref.shape[0]
    homes = [home_of(b, me) for b in range(n)]
    places = [slot_place(s, core, special, row) for s in range(n)]
    places = [(blk, b) for b, blk in places]
    dest, origin = (homes, places) if to_home else (places, homes)
    for i, (dev, dst) in enumerate(dest):

        @pl.when(dev == me)
        def _():
            pltpu.make_async_copy(x_ref.at[i], buf.at[i], sem.at[i]).start()

    group_barrier(n_dev)
    for i, (dev, dst) in enumerate(dest):

        @pl.when(dev != me)
        def _():
            remote(x_ref.at[i], o_ref.at[dst], send.at[i], recv.at[dst], dev).start()

    for i, (dev, dst) in enumerate(dest):

        @pl.when(dev == me)
        def _():
            pltpu.make_async_copy(x_ref.at[i], buf.at[i], sem.at[i]).wait()
            pltpu.make_async_copy(buf.at[i], o_ref.at[dst], sem.at[i]).start()
            pltpu.make_async_copy(buf.at[i], o_ref.at[dst], sem.at[i]).wait()

    for i, (dev, _) in enumerate(origin):

        @pl.when(dev != me)
        def _():
            remote(x_ref.at[i], o_ref.at[i], send.at[i], recv.at[i], dev).wait_recv()

    for i, (dev, dst) in enumerate(dest):

        @pl.when(dev != me)
        def _():
            remote(x_ref.at[i], o_ref.at[dst], send.at[i], recv.at[dst], dev).wait_send()


def exchange(to_home, n_dev, x, cid):
    n = x.shape[0]
    dma = pltpu.SemaphoreType.DMA
    return pl.pallas_call(
        functools.partial(exchange_kernel, to_home, n_dev),
        out_shape=jax.ShapeDtypeStruct(x.shape, x.dtype),
        in_specs=[pl.BlockSpec(memory_space=pl.ANY)],
        out_specs=pl.BlockSpec(memory_space=pl.ANY),
        scratch_shapes=[pltpu.VMEM(x.shape, x.dtype), dma((n,)), dma((n,)), dma((n,))],
        compiler_params=pltpu.CompilerParams(collective_id=cid, has_side_effects=True),
    )(x)


def norm_rows(vals, gain):
    inv = lax.rsqrt(jnp.mean(vals * vals, axis=-1, keepdims=True) + NORM_EPS)
    return vals * inv * (1.0 + gain)


def qkv_kernel(layer, nq, nk, slots, x_ref, ln_ref, qk_ref, cos_ref, sin_ref, wq_ref, wk_ref, wv_ref, q_ref, k_ref, v_ref, a_ref, raw_ref):
    i = pl.program_id(0)
    rows = x_ref.shape[0] // slots
    hd = wq_ref.shape[-1]
    half = hd // 2

    @pl.when(i == 0)
    def _():
        gain = ln_ref[layer, 0:1, :].astype(jnp.float32)
        for s in range(slots):
            r = pl.ds(s * rows, rows)
            a_ref[r, :] = norm_rows(x_ref[r, :].astype(jnp.float32), gain).astype(jnp.bfloat16)

    def product(w_ref):
        raw_ref[...] = jnp.dot(a_ref[...], w_ref[0], preferred_element_type=jnp.float32)

    def turned(s, which):
        r = pl.ds(s * rows, rows)
        raw = raw_ref[r, :].astype(jnp.bfloat16).astype(jnp.float32)
        vals = norm_rows(raw, qk_ref[layer, which : which + 1, :].astype(jnp.float32))
        first, second = vals[:, :half], vals[:, half:]
        cos, sin = cos_ref[r, :], sin_ref[r, :]
        return jnp.concatenate([first * cos - second * sin, second * cos + first * sin], axis=-1).astype(jnp.bfloat16)

    @pl.when(i < nq)
    def _():
        product(wq_ref)
        for s in range(slots):
            q_ref[s, 0] = turned(s, 0) * jnp.bfloat16(hd**-0.5)

    @pl.when((i >= nq) & (i < nq + nk))
    def _():
        product(wk_ref)
        for s in range(slots):
            k_ref[s] = turned(s, 1)

    @pl.when(i >= nq + nk)
    def _():
        product(wv_ref)
        for s in range(slots):
            v_ref[s] = raw_ref[pl.ds(s * rows, rows), :].astype(jnp.bfloat16)


def qkv(layer, x, ln_w, qk_w, cos, sin, w_q, w_k, w_v):
    slots, rows, dim = x.shape
    hd = qk_w.shape[-1]
    nq, nk = w_q.shape[-1] // hd, w_k.shape[-1] // hd
    x2 = x.reshape(slots * rows, dim)
    whole = lambda a: pl.BlockSpec(a.shape, lambda i: (0,) * a.ndim)
    at = lambda lo, n: (lambda i: jnp.clip(i - lo, 0, n - 1))
    iq, ik, iv = at(0, nq), at(nq, nk), at(nq + nk, nk)
    wspec = lambda f: pl.BlockSpec((1, dim, hd), lambda i: (layer, 0, f(i)))
    return pl.pallas_call(
        functools.partial(qkv_kernel, layer, nq, nk, slots),
        grid=(nq + 2 * nk,),
        in_specs=[whole(x2), whole(ln_w), whole(qk_w), whole(cos), whole(sin), wspec(iq), wspec(ik), wspec(iv)],
        out_specs=[
            pl.BlockSpec((slots, 1, rows, hd), lambda i: (0, iq(i), 0, 0)),
            pl.BlockSpec((slots, rows, hd), lambda i: (0, 0, ik(i))),
            pl.BlockSpec((slots, rows, hd), lambda i: (0, 0, iv(i))),
        ],
        out_shape=[
            jax.ShapeDtypeStruct((slots, nq, rows, hd), jnp.bfloat16),
            jax.ShapeDtypeStruct((slots, rows, nk * hd), jnp.bfloat16),
            jax.ShapeDtypeStruct((slots, rows, nk * hd), jnp.bfloat16),
        ],
        scratch_shapes=[pltpu.VMEM(x2.shape, jnp.bfloat16), pltpu.VMEM((slots * rows, hd), jnp.float32)],
        compiler_params=pltpu.CompilerParams(dimension_semantics=("arbitrary",), vmem_limit_bytes=VMEM_LIMIT),
    )(x2, ln_w, qk_w, cos, sin, w_q, w_k, w_v)


def attn_kernel(window_blocks, q_ref, k_ref, v_ref, o_ref, kbuf, vbuf, qbuf, obuf, acc, mx, sm, sbuf, wacc, wm, wl, bias,
                qsem, ksem, vsem, ksend, vsend, fsend, krecv, vrecv, osem):
    me, chip, core, special, row = placement()
    mate = chip * 2 + (1 - core)
    slots, nq, rows, hd = q_ref.shape
    nk = k_ref.shape[-1] // hd
    rep = nq // nk
    per = 4
    tile = per * rows
    barrier = pltpu.get_barrier_semaphore()

    def tell(dev):
        pl.semaphore_signal(barrier, inc=1, device_id={"cp": dev}, device_id_type=pl.DeviceIdType.MESH)

    def buf_index(s, c):
        b, blk = slot_place(s, c, special, row)
        return jnp.where(special == 1, (s // 2) * 4 + blk, blk)

    serve_chip = [jnp.where(row == 0, ROW_CHIP[r], ROW_CHIP[r + 3]) for r in range(3)]
    my_special = jnp.where(row < 3, SPECIAL[0], SPECIAL[1]) * 2 + core

    for s in range(slots):
        idx = buf_index(s, core)
        pltpu.make_async_copy(k_ref.at[s], kbuf.at[idx], ksem.at[s]).start()
        pltpu.make_async_copy(v_ref.at[s], vbuf.at[idx], vsem.at[s]).start()
        pltpu.make_async_copy(q_ref.at[s], qbuf.at[s], qsem.at[s]).start()

    tell(mate)

    @pl.when(special == 1)
    def _():
        for r in range(3):
            tell(serve_chip[r] * 2 + core)
        pl.semaphore_wait(barrier, 4)

    @pl.when(special == 0)
    def _():
        tell(my_special)
        pl.semaphore_wait(barrier, 2)

    @pl.when(special == 1)
    def _():
        for k in range(2):
            for r in range(3):
                s = 2 * r + k
                blk = 2 * k + (k + core) % 2
                dev = serve_chip[r] * 2 + core
                remote(k_ref.at[s], kbuf.at[blk], ksend.at[1, s], krecv.at[blk], dev).start()
                remote(v_ref.at[s], vbuf.at[blk], vsend.at[1, s], vrecv.at[blk], dev).start()

    for s in range(slots):
        idx = buf_index(s, core)
        remote(k_ref.at[s], kbuf.at[idx], ksend.at[0, s], krecv.at[idx], mate).start()
        remote(v_ref.at[s], vbuf.at[idx], vsend.at[0, s], vrecv.at[idx], mate).start()

    qi = lax.broadcasted_iota(jnp.int32, (rows, tile), 0)
    ki = lax.broadcasted_iota(jnp.int32, (rows, tile), 1)
    bias[0] = jnp.zeros((rows, tile), jnp.float32)
    for j in range(per):
        bias[1 + j] = jnp.where(ki <= qi + j * rows, 0.0, NEG)
        if window_blocks is not None:
            bias[1 + per + j] = jnp.where(ki > qi + j * rows, 0.0, NEG)

    def start_tile(blk):
        if window_blocks is None:
            return jnp.int32(0)
        return jnp.maximum(blk - window_blocks, 0) // per

    def scores(s, t, base, blk):
        edge = jnp.where(t == blk // per, 1 + blk % per, 0)
        if window_blocks is not None:
            old = blk - window_blocks
            edge = jnp.where((old >= 0) & (t == old // per), 1 + per + old % per, edge)
        off = bias[edge][None]
        kt = kbuf.at[pl.ds(base + per * t, per)]
        out = []
        for g in range(nk):
            q2 = qbuf[s, g * rep : (g + 1) * rep].reshape(rep * rows, hd)
            kk = kt[:, :, g * hd : (g + 1) * hd].reshape(tile, hd)
            sc = lax.dot_general(q2, kk, (((1,), (1,)), ((), ())), preferred_element_type=jnp.float32)
            out.append((sc.reshape(rep, rows, tile) + off).reshape(rep * rows, tile))
        return out

    lanes = 128

    def columns(val, op):
        parts = [val[:, j * lanes : (j + 1) * lanes] for j in range(tile // lanes)]
        return functools.reduce(op, parts)

    def spread(val):
        return jnp.concatenate([val] * (tile // lanes), axis=1)

    def row_max(val):
        return jnp.broadcast_to(jnp.max(val, axis=-1, keepdims=True), val.shape)

    def values(t, base, g):
        return vbuf.at[pl.ds(base + per * t, per)][:, :, g * hd : (g + 1) * hd].reshape(tile, hd)

    def finish(s, total, weight):
        for g in range(nk):
            out = (total[g] / jnp.sum(weight[g], axis=-1, keepdims=True)).astype(jnp.bfloat16)
            for h in range(rep):
                lo = (g * rep + h) * hd
                obuf[s, :, lo : lo + hd] = out[h * rows : (h + 1) * rows]
        pltpu.make_async_copy(obuf.at[s], o_ref.at[s], osem.at[s]).start()

    for s in range(slots):
        pltpu.make_async_copy(k_ref.at[s], kbuf.at[buf_index(s, core)], ksem.at[s]).wait()
        pltpu.make_async_copy(v_ref.at[s], vbuf.at[buf_index(s, core)], vsem.at[s]).wait()
        pltpu.make_async_copy(q_ref.at[s], qbuf.at[s], qsem.at[s]).wait()
    for s in range(slots):
        idx = buf_index(s, 1 - core)
        remote(k_ref.at[s], kbuf.at[idx], ksend.at[0, s], krecv.at[idx], mate).wait()
        remote(v_ref.at[s], vbuf.at[idx], vsend.at[0, s], vrecv.at[idx], mate).wait()

    @pl.loop(0, slots)
    def _(s):
        _, blk = slot_place(s, core, special, row)
        base = jnp.where(special == 1, (s // 2) * per, 0)
        first = jnp.where(special == 1, 0, jnp.maximum(start_tile(blk), 1))
        last = blk // per + 1
        for g in range(nk):
            wm[g] = jnp.full(wm.shape[1:], NEG, jnp.float32)
            wl[g] = jnp.zeros(wl.shape[1:], jnp.float32)
            wacc[g] = jnp.zeros(wacc.shape[1:], jnp.float32)

        @pl.loop(first, last)
        def _(t):
            for g, sc in enumerate(scores(s, t, base, blk)):
                sbuf[g, t] = sc
                wm[g] = jnp.maximum(wm[g], columns(sc, jnp.maximum))

        for g in range(nk):
            wm[g] = row_max(wm[g])

        @pl.loop(first, last)
        def _(t):
            for g in range(nk):
                p = jnp.exp(sbuf[g, t] - spread(wm[g]))
                wl[g] += columns(p, jnp.add)
                wacc[g] += jnp.dot(p.astype(jnp.bfloat16), values(t, base, g), preferred_element_type=jnp.float32)

        more = (special == 0) & (start_tile(blk) == 0)

        @pl.when(more)
        def _():
            for g in range(nk):
                mx[s, g] = wm[g]
                sm[s, g] = wl[g]
                acc[s, g] = wacc[g]

        @pl.when(jnp.logical_not(more))
        def _():
            finish(s, [wacc[g] for g in range(nk)], [wl[g] for g in range(nk)])

    @pl.when(special == 0)
    def _():
        mine = [2 * k + (k + core) % 2 for k in range(2)]
        theirs = [2 * k + (k + 1 - core) % 2 for k in range(2)]
        for k in range(2):
            blk = mine[k]
            remote(k_ref.at[k], kbuf.at[blk], fsend.at[0, k], krecv.at[blk], mate).wait_recv()
            remote(kbuf.at[blk], kbuf.at[blk], fsend.at[0, k], krecv.at[blk], mate).start()
            remote(v_ref.at[k], vbuf.at[blk], fsend.at[1, k], vrecv.at[blk], mate).wait_recv()
            remote(vbuf.at[blk], vbuf.at[blk], fsend.at[1, k], vrecv.at[blk], mate).start()
        for k in range(2):
            blk = theirs[k]
            remote(kbuf.at[blk], kbuf.at[blk], fsend.at[0, k], krecv.at[blk], mate).wait()
            remote(vbuf.at[blk], vbuf.at[blk], fsend.at[1, k], vrecv.at[blk], mate).wait()

        @pl.loop(0, slots)
        def _(s):
            _, blk = slot_place(s, core, special, row)

            @pl.when(start_tile(blk) == 0)
            def _():
                total, weight = [], []
                for g, sc in enumerate(scores(s, 0, 0, blk)):
                    old = mx[s, g]
                    new = row_max(jnp.maximum(old, columns(sc, jnp.maximum)))
                    p = jnp.exp(sc - spread(new))
                    alpha = jnp.exp(old - new)
                    weight.append(alpha * sm[s, g] + columns(p, jnp.add))
                    part = jnp.dot(p.astype(jnp.bfloat16), values(0, 0, g), preferred_element_type=jnp.float32)
                    total.append(jnp.concatenate([alpha] * (hd // lanes), axis=1) * acc[s, g] + part)
                finish(s, total, weight)

    @pl.when(special == 1)
    def _():
        for s in range(slots):
            remote(k_ref.at[s], kbuf.at[0], ksend.at[1, s], krecv.at[0], mate).wait_send()
            remote(v_ref.at[s], vbuf.at[0], vsend.at[1, s], vrecv.at[0], mate).wait_send()

    for s in range(slots):
        pltpu.make_async_copy(obuf.at[s], o_ref.at[s], osem.at[s]).wait()


def attention(window, q, k, v, cid):
    slots, nq, rows, hd = q.shape
    nk = k.shape[-1] // hd
    blocks = 16
    wide = nq // nk * rows
    dma = pltpu.SemaphoreType.DMA
    any_spec = pl.BlockSpec(memory_space=pl.ANY)
    body = functools.partial(attn_kernel, None if window is None else window // rows)
    return pl.pallas_call(
        body,
        out_shape=jax.ShapeDtypeStruct((slots, rows, nq * hd), jnp.bfloat16),
        in_specs=[any_spec] * 3,
        out_specs=any_spec,
        scratch_shapes=[
            pltpu.VMEM((blocks, rows, nk * hd), jnp.bfloat16),
            pltpu.VMEM((blocks, rows, nk * hd), jnp.bfloat16),
            pltpu.VMEM(q.shape, jnp.bfloat16),
            pltpu.VMEM((slots, rows, nq * hd), jnp.bfloat16),
            pltpu.VMEM((slots, nk, wide, hd), jnp.float32),
            pltpu.VMEM((slots, nk, wide, 128), jnp.float32),
            pltpu.VMEM((slots, nk, wide, 128), jnp.float32),
            pltpu.VMEM((nk, blocks // 4, wide, 4 * rows), jnp.float32),
            pltpu.VMEM((nk, wide, hd), jnp.float32),
            pltpu.VMEM((nk, wide, 128), jnp.float32),
            pltpu.VMEM((nk, wide, 128), jnp.float32),
            pltpu.VMEM((9, rows, 4 * rows), jnp.float32),
            dma((slots,)), dma((slots,)), dma((slots,)),
            dma((2, slots)), dma((2, slots)), dma((2, 2)),
            dma((blocks,)), dma((blocks,)), dma((slots,)),
        ],
        compiler_params=pltpu.CompilerParams(collective_id=cid, has_side_effects=True, vmem_limit_bytes=VMEM_LIMIT),
    )(q, k, v)


def post_kernel(layer, n_o, n_f, slots, o_ref, x_ref, ln_ref, wo_ref, wg_ref, wu_ref, wd_ref, out_ref, att, y_ref, c_ref, acc, act):
    i = pl.program_id(0)
    rows = x_ref.shape[0] // slots
    tn = wo_ref.shape[-1]
    f32 = jnp.float32

    @pl.when(i < n_o)
    def _():
        part = jnp.dot(o_ref[...], wo_ref[0], preferred_element_type=f32).astype(jnp.bfloat16)
        att[:, pl.ds(pl.multiple_of(i * tn, tn), tn)] = part

    @pl.when(i == n_o - 1)
    def _():
        for s in range(slots):
            r = pl.ds(s * rows, rows)
            y = x_ref[r, :].astype(f32) + norm_rows(att[r, :].astype(f32), ln_ref[layer, 1:2, :].astype(f32))
            y = y.astype(jnp.bfloat16)
            y_ref[r, :] = y
            c_ref[r, :] = norm_rows(y.astype(f32), ln_ref[layer, 2:3, :].astype(f32)).astype(jnp.bfloat16)

    def up(slot):
        gate = jnp.dot(c_ref[...], wg_ref[0], preferred_element_type=f32)
        val = jnp.dot(c_ref[...], wu_ref[0], preferred_element_type=f32)
        act[slot] = (jax.nn.gelu(gate, approximate=True) * val).astype(jnp.bfloat16)

    def down(slot):
        return jnp.dot(act[slot], wd_ref[0], preferred_element_type=f32)

    j = i - n_o

    @pl.when(j == 0)
    def _():
        up(0)

    @pl.when(j == 1)
    def _():
        acc[...] = down(0)
        up(1)

    for parity in range(2):

        @pl.when((j > 1) & (j < n_f) & (j % 2 == parity))
        def _():
            acc[...] += down(1 - parity)
            up(parity)

    @pl.when(j == n_f)
    def _():
        acc[...] += down((n_f - 1) % 2)
        for s in range(slots):
            r = pl.ds(s * rows, rows)
            m = acc[r, :].astype(jnp.bfloat16).astype(f32)
            out = y_ref[r, :].astype(f32) + norm_rows(m, ln_ref[layer, 3:4, :].astype(f32))
            out_ref[r, :] = out.astype(jnp.bfloat16)


def post(layer, o, x, ln_w, w_o, w_gate, w_up, w_down):
    slots, rows, dim = x.shape
    inner, ff = w_o.shape[1], w_gate.shape[-1]
    total = slots * rows
    tn, tf = min(256, dim), min(512, ff)
    n_o, n_f = dim // tn, ff // tf
    o2, x2 = o.reshape(total, inner), x.reshape(total, dim)
    one = lambda a: pl.BlockSpec(a.shape, lambda i: (0,) * a.ndim, pipeline_mode=pl.Buffered(1))
    at_f = lambda i: jnp.clip(i - n_o, 0, n_f - 1)
    return pl.pallas_call(
        functools.partial(post_kernel, layer, n_o, n_f, slots),
        grid=(n_o + n_f + 1,),
        in_specs=[
            one(o2), one(x2), one(ln_w),
            pl.BlockSpec((1, inner, tn), lambda i: (layer, 0, jnp.minimum(i, n_o - 1))),
            pl.BlockSpec((1, dim, tf), lambda i: (layer, 0, at_f(i))),
            pl.BlockSpec((1, dim, tf), lambda i: (layer, 0, at_f(i))),
            pl.BlockSpec((1, tf, dim), lambda i: (layer, at_f(i - 1), 0)),
        ],
        out_specs=pl.BlockSpec((total, dim), lambda i: (0, 0), pipeline_mode=pl.Buffered(1)),
        out_shape=jax.ShapeDtypeStruct((total, dim), jnp.bfloat16),
        scratch_shapes=[
            pltpu.VMEM((total, dim), jnp.bfloat16),
            pltpu.VMEM((total, dim), jnp.bfloat16),
            pltpu.VMEM((total, dim), jnp.bfloat16),
            pltpu.VMEM((total, dim), jnp.float32),
            pltpu.VMEM((2, total, tf), jnp.bfloat16),
        ],
        compiler_params=pltpu.CompilerParams(dimension_semantics=("arbitrary",), vmem_limit_bytes=VMEM_LIMIT),
    )(o2, x2, ln_w, w_o, w_gate, w_up, w_down).reshape(slots, rows, dim)


def rope_tables(pos, hd):
    half = hd // 2
    out = []
    for base, scale in ((LOCAL_BASE, 1.0), (GLOBAL_BASE, GLOBAL_SCALE)):
        freq = base ** (-2.0 * jnp.arange(half, dtype=jnp.float32) / hd)
        ang = (pos.astype(jnp.float32) / scale)[:, None] * freq[None, :]
        out += [jnp.cos(ang), jnp.sin(ang)]
    return out


def solution(mesh):
    n_dev = mesh.shape["cp"]

    def device_fn(x_loc, ln_w, qk_w, w_q, w_k, w_v, w_o, w_gate, w_up, w_down):
        slots, rows, dim = x_loc.shape
        hd = qk_w.shape[-1]
        _, _, core, special, row = placement()
        blk = jnp.stack([slot_place(s, core, special, row)[1] for s in range(slots)])
        pos = (blk[:, None] * rows + jnp.arange(rows)[None, :]).reshape(-1)
        tables = rope_tables(pos, hd)

        def layer(x, l, window):
            q, k, v = qkv(l, x, ln_w, qk_w, tables[2 * l], tables[2 * l + 1], w_q, w_k, w_v)
            o = attention(window, q, k, v, 1 + l)
            return post(l, o, x, ln_w, w_o, w_gate, w_up, w_down)

        x = exchange(True, n_dev, x_loc, 0)
        x = layer(x, 0, WINDOW)
        x = layer(x, 1, None)
        return exchange(False, n_dev, x, 3)

    act_part = P("dp", "cp", None)
    return jax.shard_map(device_fn, mesh=mesh, in_specs=(act_part,) + (P(),) * 9, out_specs=act_part, check_vma=False)
```

```python
import functools

import jax
import jax.numpy as jnp
from jax import lax
from jax.experimental import pallas as pl
from jax.experimental.pallas import tpu as pltpu
from jax.sharding import PartitionSpec as P

WINDOW = 1024
NORM_EPS = 1e-6
LOCAL_BASE = 10000.0
GLOBAL_BASE = 1000000.0
GLOBAL_SCALE = 8.0
NEG = -1e30

ROW_CHIP = (0, 3, 4, 1, 5, 6)
SPECIAL = (2, 7)
VMEM_LIMIT = 64 * 1024 * 1024 - 128 * 1024
MESH = pl.DeviceIdType.MESH
BF16, F32 = jnp.bfloat16, jnp.float32
ANY = pl.BlockSpec(memory_space=pl.ANY)
WHOLE = pl.BlockSpec(memory_space=pltpu.VMEM)
DMA = pltpu.SemaphoreType.DMA


def pick(idx, table):
    out = jnp.int32(table[-1])
    for i in range(len(table) - 2, -1, -1):
        out = jnp.where(idx == i, jnp.int32(table[i]), out)
    return out


def placement():
    me = lax.axis_index("cp")
    chip, core = me // 2, me % 2
    roles = [0] * 8
    rows = [0] * 8
    for b, c in enumerate(ROW_CHIP):
        rows[c] = b
    for i, c in enumerate(SPECIAL):
        roles[c] = 1
        rows[c] = 3 * i
    return me, chip, core, pick(chip, roles), pick(chip, rows)


def slot_place(s, core, special, row):
    k = s % 2
    blk = jnp.where(special == 1, 2 * k + (k + core) % 2, 4 + 2 * s + (s + core) % 2)
    b = jnp.where(special == 1, row + s // 2, row)
    return b, blk


def ring(a, b):
    return min((a - b) % 8, (b - a) % 8)


ARRIVAL = [sorted(range(6), key=lambda s: (ring(2 + s, c), s)) for c in range(8)]
for c in SPECIAL:
    ARRIVAL[c] = [4, 5, 0, 2, 1, 3]


def home_of(b, blk):
    core = ((blk + 1) // 2) % 2
    half = blk // 2
    chip = jnp.where(blk < 4, pick(b // 3, SPECIAL), pick(b, ROW_CHIP))
    slot = jnp.where(blk < 4, (b % 3) * 2 + half, half - 2)
    return chip * 2 + core, slot


def chunk_slot(ch, i, special, row):
    b = jnp.where(special == 1, row + i, row)
    return 2 * i + (b % 2 if ch == 0 else 1 - b % 2)


def kv_index(s, core, special, row):
    _, blk = slot_place(s, core, special, row)
    return jnp.where(special == 1, (s // 2) * 4 + blk, blk)


def served(row, r):
    return jnp.where(row == 0, ROW_CHIP[r], ROW_CHIP[r + 3])


def signal_group(n_dev):
    me = lax.axis_index("cp")
    barrier = pltpu.get_barrier_semaphore()
    for d in range(1, n_dev):
        pl.semaphore_signal(barrier, inc=1, device_id={"cp": lax.rem(me + d, n_dev)}, device_id_type=MESH)


def wait_group(n_dev):
    pl.semaphore_wait(pltpu.get_barrier_semaphore(), n_dev - 1)


def remote(src, dst, send, recv, dev):
    return pltpu.make_async_remote_copy(
        src_ref=src, dst_ref=dst, send_sem=send, recv_sem=recv, device_id={"cp": dev}, device_id_type=MESH
    )


def local(src, dst, sem):
    return pltpu.make_async_copy(src, dst, sem)


def norm_rows(vals, gain):
    inv = lax.rsqrt(jnp.mean(vals * vals, axis=-1, keepdims=True) + NORM_EPS)
    return vals * inv * (1.0 + gain)


def norm_turn(raw, gain, cos, sin):
    half = raw.shape[-1] // 2
    vals = norm_rows(raw.astype(BF16).astype(F32), gain)
    first, second = vals[:, :half], vals[:, half:]
    return jnp.concatenate([first * cos - second * sin, second * cos + first * sin], axis=-1).astype(BF16)


class KeyValues:
    def __init__(self, k_all, v_all, send, recv, fwd):
        self.me, chip, self.core, self.special, self.row = placement()
        self.mate = chip * 2 + 1 - self.core
        self.both = ((0, k_all), (1, v_all))
        self.send, self.recv, self.fwd = send, recv, fwd

    def _copies(self, s, stage):
        idx = kv_index(s, self.core, self.special, self.row)
        _, blk = slot_place(s, self.core, self.special, self.row)
        dev = served(self.row, 0) * 2 + self.core
        for r in (1, 2):
            dev = jnp.where(s // 2 == r, served(self.row, r) * 2 + self.core, dev)
        out = []
        for x, full in self.both:
            out.append((
                local(stage[x], full.at[idx], self.send.at[x, 0, s]),
                remote(stage[x], full.at[idx], self.send.at[x, 1, s], self.recv.at[x, idx], self.mate),
                remote(stage[x], full.at[blk], self.send.at[x, 2, s], self.recv.at[x, blk], dev),
            ))
        return out

    def start(self, s, stage):
        for own, mate, row in self._copies(s, stage):

            @pl.when(self.special == 1)
            def _():
                row.start()

            mate.start()
            own.start()

    def wait_sent(self, s, stage):
        for own, mate, row in self._copies(s, stage):
            own.wait()
            mate.wait_send()

            @pl.when(self.special == 1)
            def _():
                row.wait_send()

    def wait_all(self, slots):
        for x, full in self.both:

            @pl.when(self.special == 0)
            def _():
                for k in range(2):
                    blk = 2 * k + (k + self.core) % 2
                    remote(full.at[blk], full.at[blk], self.fwd.at[x, k], self.recv.at[x, blk], self.mate).wait_recv()
                    remote(full.at[blk], full.at[blk], self.fwd.at[x, k], self.recv.at[x, blk], self.mate).start()

            for s in range(slots):
                idx = kv_index(s, 1 - self.core, self.special, self.row)
                remote(full.at[idx], full.at[idx], self.fwd.at[x, 0], self.recv.at[x, idx], self.mate).wait_recv()

        @pl.when(self.special == 0)
        def _():
            for x, full in self.both:
                for k in range(2):
                    blk = 2 * k + (k + 1 - self.core) % 2
                    remote(full.at[blk], full.at[blk], self.fwd.at[x, k], self.recv.at[x, blk], self.mate).wait()


def first_kernel(n_dev, nq, nk, x_ref, ln_ref, qk_ref, cos_ref, sin_ref, wq_ref, wk_ref, wv_ref,
                 h_ref, q_ref, k_all, v_all, xbuf, abuf, wq, wk, wv, qst, kst, vst,
                 wsem, xsend, xrecv, hsem, qsem, ksend, krecv, fsem):
    me, chip, core, special, row = placement()
    n, rows, dim = x_ref.shape
    hd = qk_ref.shape[-1]
    homes = [home_of(jnp.int32(b), me) for b in range(n)]
    keys = KeyValues(k_all, v_all, ksend, krecv, fsem)

    signal_group(n_dev)
    for b, (dev, slot) in enumerate(homes):

        @pl.when(dev == me)
        def _():
            local(x_ref.at[b], xbuf.at[slot], xrecv.at[slot]).start()

    weights = ((wk_ref, wk), (wv_ref, wv), (wq_ref, wq))
    for j, (src, dst) in enumerate(weights):
        local(src.at[0], dst, wsem.at[j]).start()
    wait_group(n_dev)
    for b in SEND_ORDER:
        dev, slot = homes[b]

        @pl.when(dev != me)
        def _():
            remote(x_ref.at[b], xbuf.at[slot], xsend.at[b], xrecv.at[slot], dev).start()

    gain = ln_ref[0, 0:1, :].astype(F32)

    def take(pair):
        places = [pick(chip, [ARRIVAL[c][2 * pair + j] for c in range(8)]) for j in range(2)]
        for j, s in enumerate(places):
            local(xbuf.at[s], xbuf.at[s], xrecv.at[s]).wait()
            local(xbuf.at[s], h_ref.at[s], hsem.at[s]).start()
            abuf[j * rows : (j + 1) * rows, :] = norm_rows(xbuf[s].astype(F32), gain).astype(BF16)
        return places

    def tables(s):
        r = pl.ds(pl.multiple_of(s * rows, rows), rows)
        return cos_ref[r, :], sin_ref[r, :]

    def product(w, h):
        return jnp.dot(abuf[...], w[:, pl.ds(pl.multiple_of(h * hd, hd), hd)], preferred_element_type=F32)

    for pair in range(n // 2):
        places = take(pair)
        if pair == 0:
            local(wk_ref.at[0], wk, wsem.at[0]).wait()
            local(wv_ref.at[0], wv, wsem.at[1]).wait()
        turn = [tables(s) for s in places]
        k_gain = qk_ref[0, 1:2, :].astype(F32)
        q_gain = qk_ref[0, 0:1, :].astype(F32)

        @pl.loop(0, nk)
        def _(h):
            col = pl.ds(pl.multiple_of(h * hd, hd), hd)
            k_raw, v_raw = product(wk, h), product(wv, h)
            for j, s in enumerate(places):
                part = slice(j * rows, (j + 1) * rows)
                kst[s, :, col] = norm_turn(k_raw[part], k_gain, *turn[j])
                vst[s, :, col] = v_raw[part].astype(BF16)

        if pair == 0:
            local(wq_ref.at[0], wq, wsem.at[2]).wait()

        @pl.loop(0, nq)
        def _(h):
            raw = product(wq, h)
            for j, s in enumerate(places):
                part = slice(j * rows, (j + 1) * rows)
                qst[s, h] = norm_turn(raw[part], q_gain, *turn[j]) * BF16(hd**-0.5)

        for s in places:
            keys.start(s, (kst.at[s], vst.at[s]))
            local(qst.at[s], q_ref.at[s], qsem.at[s]).start()

    for s in range(n):
        keys.wait_sent(s, (kst.at[s], vst.at[s]))
        local(qst.at[s], q_ref.at[s], qsem.at[s]).wait()
        local(xbuf.at[s], h_ref.at[s], hsem.at[s]).wait()
    for b, (dev, slot) in enumerate(homes):

        @pl.when(dev != me)
        def _():
            remote(x_ref.at[b], xbuf.at[slot], xsend.at[b], xrecv.at[slot], dev).wait_send()

    keys.wait_all(n)


SEND_ORDER = (2, 5, 0, 3, 1, 4)


def first(n_dev, x, ln_w, qk_w, cos, sin, w_q, w_k, w_v):
    n, rows, dim = x.shape
    hd = qk_w.shape[-1]
    nq, nk = w_q.shape[-1] // hd, w_k.shape[-1] // hd
    blocks = 16
    q_shape, s_shape, kv_shape = (n, nq, rows, hd), (n, rows, nk * hd), (blocks, rows, nk * hd)
    return pl.pallas_call(
        functools.partial(first_kernel, n_dev, nq, nk),
        out_shape=[jax.ShapeDtypeStruct(a, BF16) for a in (x.shape, q_shape, kv_shape, kv_shape)],
        in_specs=[ANY, WHOLE, WHOLE, WHOLE, WHOLE, ANY, ANY, ANY],
        out_specs=[ANY] * 4,
        scratch_shapes=[
            pltpu.VMEM(x.shape, BF16), pltpu.VMEM((2 * rows, dim), BF16),
            pltpu.VMEM(w_q.shape[1:], BF16), pltpu.VMEM(w_k.shape[1:], BF16), pltpu.VMEM(w_v.shape[1:], BF16),
            pltpu.VMEM(q_shape, BF16), pltpu.VMEM(s_shape, BF16), pltpu.VMEM(s_shape, BF16),
            DMA((3,)), DMA((n,)), DMA((n,)), DMA((n,)), DMA((n,)), DMA((2, 3, n)), DMA((2, blocks)), DMA((2, 2)),
        ],
        compiler_params=pltpu.CompilerParams(collective_id=0, has_side_effects=True, vmem_limit_bytes=VMEM_LIMIT),
    )(x, ln_w, qk_w, cos, sin, w_q, w_k, w_v)


def attn_kernel(window_blocks, q_ref, k_ref, v_ref, o_ref, kbuf, vbuf, qbuf, obuf, sbuf, wacc, wm, wl, bias, qsem, ksem, osem):
    _, _, core, special, row = placement()
    slots, nq, rows, hd = q_ref.shape
    nk = k_ref.shape[-1] // hd
    rep = nq // nk
    per = 4
    tile = per * rows
    tiles = k_ref.shape[0] // per

    def loads(t):
        part = pl.ds(t * per, per)
        return [local(k_ref.at[part], kbuf.at[part], ksem.at[0, t]), local(v_ref.at[part], vbuf.at[part], ksem.at[1, t])]

    for s in range(slots):
        local(q_ref.at[s], qbuf.at[s], qsem.at[s]).start()
    for t in range(tiles):
        for c in loads(t):
            c.start()

    qi = lax.broadcasted_iota(jnp.int32, (rows, tile), 0)
    ki = lax.broadcasted_iota(jnp.int32, (rows, tile), 1)
    bias[0] = jnp.zeros((rows, tile), jnp.float32)
    for j in range(per):
        bias[1 + j] = jnp.where(ki <= qi + j * rows, 0.0, NEG)
        if window_blocks is not None:
            bias[1 + per + j] = jnp.where(ki > qi + j * rows, 0.0, NEG)

    def start_tile(blk):
        if window_blocks is None:
            return jnp.int32(0)
        return jnp.maximum(blk - window_blocks, 0) // per

    def scores(s, t, base, blk):
        edge = jnp.where(t == blk // per, 1 + blk % per, 0)
        if window_blocks is not None:
            old = blk - window_blocks
            edge = jnp.where((old >= 0) & (t == old // per), 1 + per + old % per, edge)
        off = bias[edge][None]
        kt = kbuf.at[pl.ds(base + per * t, per)]
        out = []
        for g in range(nk):
            q2 = qbuf[s, g * rep : (g + 1) * rep].reshape(rep * rows, hd)
            kk = kt[:, :, g * hd : (g + 1) * hd].reshape(tile, hd)
            sc = lax.dot_general(q2, kk, (((1,), (1,)), ((), ())), preferred_element_type=jnp.float32)
            out.append((sc.reshape(rep, rows, tile) + off).reshape(rep * rows, tile))
        return out

    lanes = 128

    def columns(val, op):
        parts = [val[:, j * lanes : (j + 1) * lanes] for j in range(tile // lanes)]
        return functools.reduce(op, parts)

    def spread(val):
        return jnp.concatenate([val] * (tile // lanes), axis=1)

    def row_max(val):
        return jnp.broadcast_to(jnp.max(val, axis=-1, keepdims=True), val.shape)

    def values(t, base, g):
        return vbuf.at[pl.ds(base + per * t, per)][:, :, g * hd : (g + 1) * hd].reshape(tile, hd)

    def finish(s, total, weight):
        for g in range(nk):
            out = (total[g] / jnp.sum(weight[g], axis=-1, keepdims=True)).astype(jnp.bfloat16)
            for h in range(rep):
                lo = (g * rep + h) * hd
                obuf[s, :, lo : lo + hd] = out[h * rows : (h + 1) * rows]
        local(obuf.at[s], o_ref.at[s], osem.at[s]).start()

    for t in range(tiles):
        for c in loads(t):
            c.wait()

    @pl.loop(0, slots)
    def _(s):
        _, blk = slot_place(s, core, special, row)
        base = jnp.where(special == 1, (s // 2) * per, 0)
        first = start_tile(blk)
        last = blk // per + 1
        local(q_ref.at[s], qbuf.at[s], qsem.at[s]).wait()
        for g in range(nk):
            wm[g] = jnp.full(wm.shape[1:], NEG, F32)
            wl[g] = jnp.zeros(wl.shape[1:], F32)
            wacc[g] = jnp.zeros(wacc.shape[1:], F32)

        @pl.loop(first, last)
        def _(t):
            for g, sc in enumerate(scores(s, t, base, blk)):
                sbuf[g, t] = sc
                wm[g] = jnp.maximum(wm[g], columns(sc, jnp.maximum))

        for g in range(nk):
            wm[g] = row_max(wm[g])

        @pl.loop(first, last)
        def _(t):
            for g in range(nk):
                p = jnp.exp(sbuf[g, t] - spread(wm[g]))
                wl[g] += columns(p, jnp.add)
                wacc[g] += jnp.dot(p.astype(BF16), values(t, base, g), preferred_element_type=F32)

        finish(s, [wacc[g] for g in range(nk)], [wl[g] for g in range(nk)])

    for s in range(slots):
        local(obuf.at[s], o_ref.at[s], osem.at[s]).wait()


def attention(window, q, k, v):
    slots, nq, rows, hd = q.shape
    blocks = k.shape[0]
    nk = k.shape[-1] // hd
    wide = nq // nk * rows
    return pl.pallas_call(
        functools.partial(attn_kernel, None if window is None else window // rows),
        out_shape=jax.ShapeDtypeStruct((slots, rows, nq * hd), BF16),
        in_specs=[ANY] * 3,
        out_specs=ANY,
        scratch_shapes=[
            pltpu.VMEM(k.shape, BF16), pltpu.VMEM(v.shape, BF16), pltpu.VMEM(q.shape, BF16),
            pltpu.VMEM((slots, rows, nq * hd), BF16),
            pltpu.VMEM((nk, blocks // 4, wide, 4 * rows), F32),
            pltpu.VMEM((nk, wide, hd), F32), pltpu.VMEM((nk, wide, 128), F32), pltpu.VMEM((nk, wide, 128), F32),
            pltpu.VMEM((9, rows, 4 * rows), F32),
            DMA((slots,)), DMA((2, blocks // 4)), DMA((slots,)),
        ],
        compiler_params=pltpu.CompilerParams(vmem_limit_bytes=VMEM_LIMIT),
    )(q, k, v)


def layer_kernel(layer, last, n_dev, n_o, n_f, n_k, n_q, *refs):
    if last:
        (o_ref, x_ref, ln_ref, wo_ref, wg_ref, wu_ref, wd_ref, out_ref,
         att, y_ref, c_ref, acc, act, ybuf, ysend, yrecv, osend, orecv) = refs
    else:
        (o_ref, x_ref, ln_ref, qk_ref, cos_ref, sin_ref, wo_ref, wg_ref, wu_ref, wd_ref, wk_ref, wv_ref, wq_ref,
         h_ref, q_ref, k_all, v_all,
         att, y_ref, c_ref, acc, act, qst, kst, vst, hsem, qsem, ksend, krecv, fsem) = refs
        keys = KeyValues(k_all, v_all, ksend, krecv, fsem)
        hd = qk_ref.shape[-1]
    me, chip, core, special, row = placement()
    i = pl.program_id(0)
    half = y_ref.shape[1]
    rows = half // 3
    tn = wo_ref.shape[-1]
    span = n_f + 1 + n_k + n_k + n_q

    def slot_rows(s):
        return pl.ds(pl.multiple_of(s * rows, rows), rows)

    def own_rows(m):
        return pl.ds(m * rows, rows)

    def gain(which, l=layer):
        return ln_ref[l, which : which + 1, :].astype(F32)

    def c_of(y):
        return norm_rows(y.astype(F32), gain(2)).astype(BF16)

    @pl.when(i == 0)
    def _():
        signal_group(n_dev)

    @pl.when(i < n_o)
    def _():
        part = jnp.dot(o_ref[...], wo_ref[0], preferred_element_type=F32).astype(BF16)
        att[:, pl.ds(pl.multiple_of(i * tn, tn), tn)] = part

    @pl.when(i == n_o - 1)
    def _():
        for ch in range(2):
            for m in range(3):
                r = slot_rows(chunk_slot(ch, m, special, row))
                y = x_ref[r, :].astype(F32) + norm_rows(att[r, :].astype(F32), gain(1))
                y = y.astype(BF16)
                y_ref[ch, own_rows(m), :] = y
                if ch == 0:
                    c_ref[own_rows(m), :] = c_of(y)

    t = i - n_o

    def up(slot):
        gate = jnp.dot(c_ref[...], wg_ref[0], preferred_element_type=F32)
        val = jnp.dot(c_ref[...], wu_ref[0], preferred_element_type=F32)
        act[slot] = (jax.nn.gelu(gate, approximate=True) * val).astype(BF16)

    def down(slot):
        return jnp.dot(act[slot], wd_ref[0], preferred_element_type=F32)

    j = t % span

    @pl.when((t >= 0) & (j == 0))
    def _():
        up(0)

    @pl.when((t >= 0) & (j == 1))
    def _():
        acc[...] = down(0)
        up(1)

    for parity in range(2):

        @pl.when((t >= 0) & (j > 1) & (j < n_f) & (j % 2 == parity))
        def _():
            acc[...] += down(1 - parity)
            up(parity)

    @pl.when((t >= 0) & (j == n_f))
    def _():
        acc[...] += down((n_f - 1) % 2)

    def result(m, y):
        val = acc[own_rows(m), :].astype(BF16).astype(F32)
        return (y.astype(F32) + norm_rows(val, gain(3))).astype(BF16)

    if last:
        def sent(ch, m):
            b, blk = slot_place(chunk_slot(ch, m, special, row), core, special, row)
            src = y_ref.at[ch, own_rows(m)]
            if ch == 0:
                far = lambda: remote(src, out_ref.at[b], osend.at[m], orecv.at[b], blk)
                return blk, far, lambda: local(src, out_ref.at[b], orecv.at[b])
            return blk, lambda: remote(src, ybuf.at[b // 2], ysend.at[m], yrecv.at[b // 2], blk), None

        def owned(ch, m):
            turn = (me // 2) % 2
            b = 2 * m + (turn if ch == 0 else 1 - turn)
            return b, home_of(b, me)[0]

        @pl.when(t == 1)
        def _():
            wait_group(n_dev)
            for m in range(3):
                dev, far, _ = sent(1, m)

                @pl.when(dev != me)
                def _():
                    far().start()

        @pl.when(t == n_f)
        def _():
            for m in range(3):
                y_ref[0, own_rows(m), :] = result(m, y_ref[0, own_rows(m), :])
            for m in range(3):
                b, dev = owned(1, m)

                @pl.when(dev != me)
                def _():
                    remote(ybuf.at[m], ybuf.at[m], ysend.at[m], yrecv.at[m], me).wait_recv()

            for m in range(3):
                b, blk = slot_place(chunk_slot(1, m, special, row), core, special, row)

                @pl.when(blk == me)
                def _():
                    ybuf[b // 2] = y_ref[1, own_rows(m), :]

            for m in range(3):
                c_ref[own_rows(m), :] = c_of(ybuf[m])

        @pl.when(t == span + 1)
        def _():
            for m in range(3):
                dev, far, near = sent(0, m)

                @pl.when(dev != me)
                def _():
                    far().start()

                @pl.when(dev == me)
                def _():
                    near().start()

        @pl.when(t == span + n_f)
        def _():
            for m in range(3):
                ybuf[m] = result(m, ybuf[m])
            for m in range(3):
                b, _ = owned(1, m)
                local(ybuf.at[m], out_ref.at[b], orecv.at[b]).start()
            for ch in range(2):
                for m in range(3):
                    dev, far, _ = sent(ch, m)

                    @pl.when(dev != me)
                    def _():
                        far().wait_send()

            for b in range(6):
                local(out_ref.at[b], out_ref.at[b], orecv.at[b]).wait()

        return

    for ch in range(2):

        @pl.when(t == ch * span + n_f)
        def _():
            for m in range(3):
                h = result(m, y_ref[ch, own_rows(m), :])
                y_ref[ch, own_rows(m), :] = h
                c_ref[own_rows(m), :] = norm_rows(h.astype(F32), gain(0, layer + 1)).astype(BF16)

        if ch == 1:
            @pl.when(t == span + n_f)
            def _():
                for m in range(3):
                    s = chunk_slot(0, m, special, row)
                    keys.wait_sent(s, (kst.at[m], vst.at[m]))
                    local(qst.at[m], q_ref.at[s], qsem.at[s]).wait()

        if ch == 0:
            @pl.when(t == 1)
            def _():
                wait_group(n_dev)

        def turn(m):
            r = slot_rows(chunk_slot(ch, m, special, row))
            return cos_ref[r, :], sin_ref[r, :]

        def heads(w_ref, put):
            for h in range(w_ref.shape[-1] // hd):
                raw = jnp.dot(c_ref[...], w_ref[0, :, h * hd : (h + 1) * hd], preferred_element_type=F32)
                for m in range(3):
                    put(h, m, raw[m * rows : (m + 1) * rows])

        u = t - (ch * span + n_f + 1)
        per = wk_ref.shape[-1] // hd

        @pl.when((u >= 0) & (u < n_k))
        def _():
            def put(h, m, raw):
                col = pl.ds(pl.multiple_of((u * per + h) * hd, hd), hd)
                kst[m, :, col] = norm_turn(raw, qk_ref[layer + 1, 1:2, :].astype(F32), *turn(m))

            heads(wk_ref, put)

        @pl.when((u >= n_k) & (u < 2 * n_k))
        def _():
            def put(h, m, raw):
                col = pl.ds(pl.multiple_of(((u - n_k) * per + h) * hd, hd), hd)
                vst[m, :, col] = raw.astype(BF16)

            heads(wv_ref, put)

        @pl.when((u >= 2 * n_k) & (u < 2 * n_k + n_q))
        def _():
            def put(h, m, raw):
                out = norm_turn(raw, qk_ref[layer + 1, 0:1, :].astype(F32), *turn(m))
                qst[m, (u - 2 * n_k) * per + h] = out * BF16(hd**-0.5)

            heads(wq_ref, put)

        @pl.when(u == 2 * n_k)
        def _():
            for m in range(3):
                s = chunk_slot(ch, m, special, row)
                keys.start(s, (kst.at[m], vst.at[m]))
                local(y_ref.at[ch, own_rows(m)], h_ref.at[s], hsem.at[s]).start()

        @pl.when(u == 2 * n_k + n_q - 1)
        def _():
            for m in range(3):
                s = chunk_slot(ch, m, special, row)
                local(qst.at[m], q_ref.at[s], qsem.at[s]).start()

    @pl.when(t == span - 1)
    def _():
        for m in range(3):
            c_ref[own_rows(m), :] = c_of(y_ref[1, own_rows(m), :])

    @pl.when(i == pl.num_programs(0) - 1)
    def _():
        for m in range(3):
            s = chunk_slot(1, m, special, row)
            keys.wait_sent(s, (kst.at[m], vst.at[m]))
            local(qst.at[m], q_ref.at[s], qsem.at[s]).wait()
        for s in range(6):
            local(y_ref.at[0, own_rows(0)], h_ref.at[s], hsem.at[s]).wait()
        keys.wait_all(6)


def after_attention(layer, last, n_dev, cid, o, x, ln_w, w_o, w_gate, w_up, w_down, more=()):
    slots, rows, dim = x.shape
    inner, ff = w_o.shape[1], w_gate.shape[-1]
    total = slots * rows
    half = total // 2
    blocks = 16
    tn, tf = min(256, dim), min(512, ff)
    n_o, n_f = dim // tn, ff // tf
    o2, x2 = o.reshape(total, inner), x.reshape(total, dim)
    n_k = n_q = 0
    if not last:
        qk_w, cos, sin, w_q, w_k, w_v = more
        hd = qk_w.shape[-1]
        wide = 2 * hd
        n_k, n_q = w_k.shape[-1] // wide, w_q.shape[-1] // wide
    span = n_f + 1 + 2 * n_k + n_q
    one = lambda a: pl.BlockSpec(a.shape, lambda i: (0,) * a.ndim, pipeline_mode=pl.Buffered(1))

    def at_f(i):
        t = jnp.clip(i - n_o, 0, 2 * span - 1)
        return jnp.minimum(t % span, n_f - 1)

    def next_w(lo, n):
        return lambda i: (layer + 1, 0, jnp.clip(jnp.clip(i - n_o, 0, 2 * span - 1) % span - (n_f + 1 + lo), 0, n - 1))

    mlp_specs = [
        pl.BlockSpec((1, inner, tn), lambda i: (layer, 0, jnp.minimum(i, n_o - 1))),
        pl.BlockSpec((1, dim, tf), lambda i: (layer, 0, at_f(i))),
        pl.BlockSpec((1, dim, tf), lambda i: (layer, 0, at_f(i))),
        pl.BlockSpec((1, tf, dim), lambda i: (layer, at_f(i - 1), 0)),
    ]
    work = [
        pltpu.VMEM((total, dim), BF16), pltpu.VMEM((2, half, dim), BF16), pltpu.VMEM((half, dim), BF16),
        pltpu.VMEM((half, dim), F32), pltpu.VMEM((2, half, tf), BF16),
    ]
    params = pltpu.CompilerParams(
        dimension_semantics=("arbitrary",), collective_id=cid, has_side_effects=True, vmem_limit_bytes=VMEM_LIMIT
    )
    body = functools.partial(layer_kernel, layer, last, n_dev, n_o, n_f, n_k, n_q)
    if last:
        return pl.pallas_call(
            body, grid=(n_o + 2 * span,),
            in_specs=[one(o2), one(x2), one(ln_w)] + mlp_specs,
            out_specs=ANY,
            out_shape=jax.ShapeDtypeStruct(x.shape, BF16),
            scratch_shapes=work + [pltpu.VMEM((3, rows, dim), BF16), DMA((3,)), DMA((3,)), DMA((3,)), DMA((slots,))],
            compiler_params=params,
        )(o2, x2, ln_w, w_o, w_gate, w_up, w_down)
    nq, nk = w_q.shape[-1] // hd, w_k.shape[-1] // hd
    q_shape, kv_shape = (slots, nq, rows, hd), (blocks, rows, nk * hd)
    return pl.pallas_call(
        body, grid=(n_o + 2 * span,),
        in_specs=[one(o2), one(x2), one(ln_w), one(qk_w), one(cos), one(sin)] + mlp_specs + [
            pl.BlockSpec((1, dim, wide), next_w(0, n_k)),
            pl.BlockSpec((1, dim, wide), next_w(n_k, n_k)),
            pl.BlockSpec((1, dim, wide), next_w(2 * n_k, n_q)),
        ],
        out_specs=[ANY] * 4,
        out_shape=[jax.ShapeDtypeStruct(a, BF16) for a in (x.shape, q_shape, kv_shape, kv_shape)],
        scratch_shapes=work + [
            pltpu.VMEM((3, nq, rows, hd), BF16), pltpu.VMEM((3, rows, nk * hd), BF16), pltpu.VMEM((3, rows, nk * hd), BF16),
            DMA((slots,)), DMA((slots,)), DMA((2, 3, slots)), DMA((2, blocks)), DMA((2, 2)),
        ],
        compiler_params=params,
    )(o2, x2, ln_w, qk_w, cos, sin, w_o, w_gate, w_up, w_down, w_k, w_v, w_q)


def rope_tables(pos, hd):
    half = hd // 2
    out = []
    for base, scale in ((LOCAL_BASE, 1.0), (GLOBAL_BASE, GLOBAL_SCALE)):
        freq = base ** (-2.0 * jnp.arange(half, dtype=jnp.float32) / hd)
        ang = (pos.astype(jnp.float32) / scale)[:, None] * freq[None, :]
        out += [jnp.cos(ang), jnp.sin(ang)]
    return out


def solution(mesh):
    n_dev = mesh.shape["cp"]

    def device_fn(x_loc, ln_w, qk_w, w_q, w_k, w_v, w_o, w_gate, w_up, w_down):
        slots, rows, dim = x_loc.shape
        _, _, core, special, row = placement()
        blk = jnp.stack([slot_place(s, core, special, row)[1] for s in range(slots)])
        pos = (blk[:, None] * rows + jnp.arange(rows)[None, :]).reshape(-1)
        cos0, sin0, cos1, sin1 = rope_tables(pos, qk_w.shape[-1])
        x, q, k, v = first(n_dev, x_loc, ln_w, qk_w, cos0, sin0, w_q, w_k, w_v)
        o = attention(WINDOW, q, k, v)
        mlp = (w_o, w_gate, w_up, w_down)
        x, q, k, v = after_attention(0, False, n_dev, 1, o, x, ln_w, *mlp, more=(qk_w, cos1, sin1, w_q, w_k, w_v))
        o = attention(None, q, k, v)
        return after_attention(1, True, n_dev, 2, o, x, ln_w, *mlp)

    act_part = P("dp", "cp", None)
    return jax.shard_map(device_fn, mesh=mesh, in_specs=(act_part,) + (P(),) * 9, out_specs=act_part, check_vma=False)
```

```python
import functools

import jax
import jax.numpy as jnp
from jax import lax
from jax.experimental import pallas as pl
from jax.experimental.pallas import tpu as pltpu
from jax.sharding import PartitionSpec as P

WINDOW = 1024
NORM_EPS = 1e-6
LOCAL_BASE = 10000.0
GLOBAL_BASE = 1000000.0
GLOBAL_SCALE = 8.0
NEG = -1e30

ROW_CHIP = (0, 3, 4, 1, 5, 6)
SPECIAL = (2, 7)
VMEM_LIMIT = 64 * 1024 * 1024 - 128 * 1024
MESH = pl.DeviceIdType.MESH
BF16, F32 = jnp.bfloat16, jnp.float32
ANY = pl.BlockSpec(memory_space=pl.ANY)
WHOLE = pl.BlockSpec(memory_space=pltpu.VMEM)
DMA = pltpu.SemaphoreType.DMA


def pick(idx, table):
    out = jnp.int32(table[-1])
    for i in range(len(table) - 2, -1, -1):
        out = jnp.where(idx == i, jnp.int32(table[i]), out)
    return out


def placement():
    me = lax.axis_index("cp")
    chip, core = me // 2, me % 2
    roles = [0] * 8
    rows = [0] * 8
    for b, c in enumerate(ROW_CHIP):
        rows[c] = b
    for i, c in enumerate(SPECIAL):
        roles[c] = 1
        rows[c] = 3 * i
    return me, chip, core, pick(chip, roles), pick(chip, rows)


def slot_place(s, core, special, row):
    k = s % 2
    blk = jnp.where(special == 1, 2 * k + (k + core) % 2, 4 + 2 * s + (s + core) % 2)
    b = jnp.where(special == 1, row + s // 2, row)
    return b, blk


def ring(a, b):
    return min((a - b) % 8, (b - a) % 8)


ARRIVAL = [sorted(range(6), key=lambda s: (ring(2 + s, c), s)) for c in range(8)]
for c in SPECIAL:
    ARRIVAL[c] = [4, 5, 0, 2, 1, 3]


def home_of(b, blk):
    core = ((blk + 1) // 2) % 2
    half = blk // 2
    chip = jnp.where(blk < 4, pick(b // 3, SPECIAL), pick(b, ROW_CHIP))
    slot = jnp.where(blk < 4, (b % 3) * 2 + half, half - 2)
    return chip * 2 + core, slot


def chunk_slot(ch, i, special, row):
    b = jnp.where(special == 1, row + i, row)
    return 2 * i + (b % 2 if ch == 0 else 1 - b % 2)


def kv_index(s, core, special, row):
    _, blk = slot_place(s, core, special, row)
    return jnp.where(special == 1, (s // 2) * 4 + blk, blk)


def served(row, r):
    return jnp.where(row == 0, ROW_CHIP[r], ROW_CHIP[r + 3])


def signal_group(n_dev):
    me = lax.axis_index("cp")
    barrier = pltpu.get_barrier_semaphore()
    for d in range(1, n_dev):
        pl.semaphore_signal(barrier, inc=1, device_id={"cp": lax.rem(me + d, n_dev)}, device_id_type=MESH)


def wait_group(n_dev):
    pl.semaphore_wait(pltpu.get_barrier_semaphore(), n_dev - 1)


def remote(src, dst, send, recv, dev):
    return pltpu.make_async_remote_copy(
        src_ref=src, dst_ref=dst, send_sem=send, recv_sem=recv, device_id={"cp": dev}, device_id_type=MESH
    )


def local(src, dst, sem):
    return pltpu.make_async_copy(src, dst, sem)


def norm_rows(vals, gain):
    inv = lax.rsqrt(jnp.mean(vals * vals, axis=-1, keepdims=True) + NORM_EPS)
    return vals * inv * (1.0 + gain)


def norm_turn(raw, gain, cos, sin):
    half = raw.shape[-1] // 2
    vals = norm_rows(raw.astype(BF16).astype(F32), gain)
    first, second = vals[:, :half], vals[:, half:]
    return jnp.concatenate([first * cos - second * sin, second * cos + first * sin], axis=-1).astype(BF16)


class KeyValues:
    def __init__(self, k_all, v_all, send, recv, fwd):
        self.both = ((0, k_all), (1, v_all))
        self.send, self.recv, self.fwd = send, recv, fwd

    def here(self):
        _, chip, self.core, self.special, self.row = placement()
        self.mate = chip * 2 + 1 - self.core

    def _copies(self, s, stage):
        idx = kv_index(s, self.core, self.special, self.row)
        _, blk = slot_place(s, self.core, self.special, self.row)
        dev = served(self.row, 0) * 2 + self.core
        for r in (1, 2):
            dev = jnp.where(s // 2 == r, served(self.row, r) * 2 + self.core, dev)
        out = []
        for x, full in self.both:
            out.append((
                local(stage[x], full.at[idx], self.send.at[x, 0, s]),
                remote(stage[x], full.at[idx], self.send.at[x, 1, s], self.recv.at[x, idx], self.mate),
                remote(stage[x], full.at[blk], self.send.at[x, 2, s], self.recv.at[x, blk], dev),
            ))
        return out

    def start(self, s, stage):
        self.here()
        for own, mate, row in self._copies(s, stage):

            @pl.when(self.special == 1)
            def _():
                row.start()

            mate.start()
            own.start()

    def wait_sent(self, s, stage):
        self.here()
        for own, mate, row in self._copies(s, stage):
            own.wait()
            mate.wait_send()

            @pl.when(self.special == 1)
            def _():
                row.wait_send()

    def wait_all(self, slots):
        self.here()
        for x, full in self.both:

            @pl.when(self.special == 0)
            def _():
                for k in range(2):
                    blk = 2 * k + (k + self.core) % 2
                    remote(full.at[blk], full.at[blk], self.fwd.at[x, k], self.recv.at[x, blk], self.mate).wait_recv()
                    remote(full.at[blk], full.at[blk], self.fwd.at[x, k], self.recv.at[x, blk], self.mate).start()

            for s in range(slots):
                idx = kv_index(s, 1 - self.core, self.special, self.row)
                remote(full.at[idx], full.at[idx], self.fwd.at[x, 0], self.recv.at[x, idx], self.mate).wait_recv()

        @pl.when(self.special == 0)
        def _():
            for x, full in self.both:
                for k in range(2):
                    blk = 2 * k + (k + 1 - self.core) % 2
                    remote(full.at[blk], full.at[blk], self.fwd.at[x, k], self.recv.at[x, blk], self.mate).wait()


def first_kernel(n_dev, nq, nk, x_ref, ln_ref, qk_ref, cos_ref, sin_ref, wq_ref, wk_ref, wv_ref,
                 h_ref, q_ref, k_all, v_all, xbuf, abuf, wq, wk, wv, qst, kst, vst,
                 wsem, xsend, xrecv, hsem, qsem, ksend, krecv, fsem):
    me, chip, core, special, row = placement()
    n, rows, dim = x_ref.shape
    hd = qk_ref.shape[-1]
    homes = [home_of(jnp.int32(b), me) for b in range(n)]
    keys = KeyValues(k_all, v_all, ksend, krecv, fsem)

    signal_group(n_dev)
    for b, (dev, slot) in enumerate(homes):

        @pl.when(dev == me)
        def _():
            local(x_ref.at[b], xbuf.at[slot], xrecv.at[slot]).start()

    weights = ((wk_ref, wk), (wv_ref, wv), (wq_ref, wq))
    for j, (src, dst) in enumerate(weights):
        local(src.at[0], dst, wsem.at[j]).start()
    wait_group(n_dev)
    for b in SEND_ORDER:
        dev, slot = homes[b]

        @pl.when(dev != me)
        def _():
            remote(x_ref.at[b], xbuf.at[slot], xsend.at[b], xrecv.at[slot], dev).start()

    gain = ln_ref[0, 0:1, :].astype(F32)

    def take(pair):
        places = [pick(chip, [ARRIVAL[c][2 * pair + j] for c in range(8)]) for j in range(2)]
        for j, s in enumerate(places):
            local(xbuf.at[s], xbuf.at[s], xrecv.at[s]).wait()
            local(xbuf.at[s], h_ref.at[s], hsem.at[s]).start()
            abuf[j * rows : (j + 1) * rows, :] = norm_rows(xbuf[s].astype(F32), gain).astype(BF16)
        return places

    def tables(s):
        r = pl.ds(pl.multiple_of(s * rows, rows), rows)
        return cos_ref[r, :], sin_ref[r, :]

    def product(w, h):
        return jnp.dot(abuf[...], w[:, pl.ds(pl.multiple_of(h * hd, hd), hd)], preferred_element_type=F32)

    for pair in range(n // 2):
        places = take(pair)
        if pair == 0:
            local(wk_ref.at[0], wk, wsem.at[0]).wait()
            local(wv_ref.at[0], wv, wsem.at[1]).wait()
        turn = [tables(s) for s in places]
        k_gain = qk_ref[0, 1:2, :].astype(F32)
        q_gain = qk_ref[0, 0:1, :].astype(F32)

        @pl.loop(0, nk)
        def _(h):
            col = pl.ds(pl.multiple_of(h * hd, hd), hd)
            k_raw, v_raw = product(wk, h), product(wv, h)
            for j, s in enumerate(places):
                part = slice(j * rows, (j + 1) * rows)
                kst[s, :, col] = norm_turn(k_raw[part], k_gain, *turn[j])
                vst[s, :, col] = v_raw[part].astype(BF16)

        if pair == 0:
            local(wq_ref.at[0], wq, wsem.at[2]).wait()

        def query(h):
            raw = product(wq, h)
            for j, s in enumerate(places):
                part = slice(j * rows, (j + 1) * rows)
                qst[s, h] = norm_turn(raw[part], q_gain, *turn[j]) * BF16(hd**-0.5)

        query(0)
        for s in places:
            keys.start(s, (kst.at[s], vst.at[s]))
        pl.loop(1, nq)(query)
        for s in places:
            local(qst.at[s], q_ref.at[s], qsem.at[s]).start()

    for s in range(n):
        keys.wait_sent(s, (kst.at[s], vst.at[s]))
        local(qst.at[s], q_ref.at[s], qsem.at[s]).wait()
        local(xbuf.at[s], h_ref.at[s], hsem.at[s]).wait()
    for b, (dev, slot) in enumerate(homes):

        @pl.when(dev != me)
        def _():
            remote(x_ref.at[b], xbuf.at[slot], xsend.at[b], xrecv.at[slot], dev).wait_send()

    keys.wait_all(n)


SEND_ORDER = (2, 5, 0, 3, 1, 4)


def first(n_dev, x, ln_w, qk_w, cos, sin, w_q, w_k, w_v):
    n, rows, dim = x.shape
    hd = qk_w.shape[-1]
    nq, nk = w_q.shape[-1] // hd, w_k.shape[-1] // hd
    blocks = 16
    q_shape, s_shape, kv_shape = (n, nq, rows, hd), (n, rows, nk * hd), (blocks, rows, nk * hd)
    return pl.pallas_call(
        functools.partial(first_kernel, n_dev, nq, nk),
        out_shape=[jax.ShapeDtypeStruct(a, BF16) for a in (x.shape, q_shape, kv_shape, kv_shape)],
        in_specs=[ANY, WHOLE, WHOLE, WHOLE, WHOLE, ANY, ANY, ANY],
        out_specs=[ANY] * 4,
        scratch_shapes=[
            pltpu.VMEM(x.shape, BF16), pltpu.VMEM((2 * rows, dim), BF16),
            pltpu.VMEM(w_q.shape[1:], BF16), pltpu.VMEM(w_k.shape[1:], BF16), pltpu.VMEM(w_v.shape[1:], BF16),
            pltpu.VMEM(q_shape, BF16), pltpu.VMEM(s_shape, BF16), pltpu.VMEM(s_shape, BF16),
            DMA((3,)), DMA((n,)), DMA((n,)), DMA((n,)), DMA((n,)), DMA((2, 3, n)), DMA((2, blocks)), DMA((2, 2)),
        ],
        compiler_params=pltpu.CompilerParams(collective_id=0, has_side_effects=True, vmem_limit_bytes=VMEM_LIMIT),
    )(x, ln_w, qk_w, cos, sin, w_q, w_k, w_v)


def attn_kernel(window_blocks, q_ref, k_ref, v_ref, o_ref, kbuf, vbuf, qbuf, obuf, sbuf, wacc, wm, wl, bias, qsem, ksem, osem):
    _, _, core, special, row = placement()
    slots, nq, rows, hd = q_ref.shape
    nk = k_ref.shape[-1] // hd
    rep = nq // nk
    per = 4
    tile = per * rows
    tiles = k_ref.shape[0] // per

    def loads(t):
        part = pl.ds(t * per, per)
        return [local(k_ref.at[part], kbuf.at[part], ksem.at[0, t]), local(v_ref.at[part], vbuf.at[part], ksem.at[1, t])]

    for s in range(slots):
        local(q_ref.at[s], qbuf.at[s], qsem.at[s]).start()
    for t in range(tiles):
        for c in loads(t):
            c.start()

    qi = lax.broadcasted_iota(jnp.int32, (rows, tile), 0)
    ki = lax.broadcasted_iota(jnp.int32, (rows, tile), 1)
    bias[0] = jnp.zeros((rows, tile), jnp.float32)
    for j in range(per):
        bias[1 + j] = jnp.where(ki <= qi + j * rows, 0.0, NEG)
        if window_blocks is not None:
            bias[1 + per + j] = jnp.where(ki > qi + j * rows, 0.0, NEG)

    def start_tile(blk):
        if window_blocks is None:
            return jnp.int32(0)
        return jnp.maximum(blk - window_blocks, 0) // per

    def scores(s, t, base, blk):
        edge = jnp.where(t == blk // per, 1 + blk % per, 0)
        if window_blocks is not None:
            old = blk - window_blocks
            edge = jnp.where((old >= 0) & (t == old // per), 1 + per + old % per, edge)
        off = bias[edge][None]
        kt = kbuf.at[pl.ds(base + per * t, per)]
        out = []
        for g in range(nk):
            q2 = qbuf[s, g * rep : (g + 1) * rep].reshape(rep * rows, hd)
            kk = kt[:, :, g * hd : (g + 1) * hd].reshape(tile, hd)
            sc = lax.dot_general(q2, kk, (((1,), (1,)), ((), ())), preferred_element_type=jnp.float32)
            out.append((sc.reshape(rep, rows, tile) + off).reshape(rep * rows, tile))
        return out

    lanes = 128

    def columns(val, op):
        parts = [val[:, j * lanes : (j + 1) * lanes] for j in range(tile // lanes)]
        return functools.reduce(op, parts)

    def spread(val):
        return jnp.concatenate([val] * (tile // lanes), axis=1)

    def row_max(val):
        return jnp.broadcast_to(jnp.max(val, axis=-1, keepdims=True), val.shape)

    def values(t, base, g):
        return vbuf.at[pl.ds(base + per * t, per)][:, :, g * hd : (g + 1) * hd].reshape(tile, hd)

    def finish(s, total, weight):
        for g in range(nk):
            out = (total[g] / jnp.sum(weight[g], axis=-1, keepdims=True)).astype(jnp.bfloat16)
            for h in range(rep):
                lo = (g * rep + h) * hd
                obuf[s, :, lo : lo + hd] = out[h * rows : (h + 1) * rows]
        local(obuf.at[s], o_ref.at[s], osem.at[s]).start()

    for t in range(tiles):
        for c in loads(t):
            c.wait()

    @pl.loop(0, slots)
    def _(s):
        _, blk = slot_place(s, core, special, row)
        base = jnp.where(special == 1, (s // 2) * per, 0)
        first = start_tile(blk)
        last = blk // per + 1
        local(q_ref.at[s], qbuf.at[s], qsem.at[s]).wait()
        for g in range(nk):
            wm[g] = jnp.full(wm.shape[1:], NEG, F32)
            wl[g] = jnp.zeros(wl.shape[1:], F32)
            wacc[g] = jnp.zeros(wacc.shape[1:], F32)

        @pl.loop(first, last)
        def _(t):
            for g, sc in enumerate(scores(s, t, base, blk)):
                sbuf[g, t] = sc
                wm[g] = jnp.maximum(wm[g], columns(sc, jnp.maximum))

        for g in range(nk):
            wm[g] = row_max(wm[g])

        @pl.loop(first, last)
        def _(t):
            for g in range(nk):
                p = jnp.exp(sbuf[g, t] - spread(wm[g]))
                wl[g] += columns(p, jnp.add)
                wacc[g] += jnp.dot(p.astype(BF16), values(t, base, g), preferred_element_type=F32)

        finish(s, [wacc[g] for g in range(nk)], [wl[g] for g in range(nk)])

    for s in range(slots):
        local(obuf.at[s], o_ref.at[s], osem.at[s]).wait()


def attention(window, q, k, v):
    slots, nq, rows, hd = q.shape
    blocks = k.shape[0]
    nk = k.shape[-1] // hd
    wide = nq // nk * rows
    return pl.pallas_call(
        functools.partial(attn_kernel, None if window is None else window // rows),
        out_shape=jax.ShapeDtypeStruct((slots, rows, nq * hd), BF16),
        in_specs=[ANY] * 3,
        out_specs=ANY,
        scratch_shapes=[
            pltpu.VMEM(k.shape, BF16), pltpu.VMEM(v.shape, BF16), pltpu.VMEM(q.shape, BF16),
            pltpu.VMEM((slots, rows, nq * hd), BF16),
            pltpu.VMEM((nk, blocks // 4, wide, 4 * rows), F32),
            pltpu.VMEM((nk, wide, hd), F32), pltpu.VMEM((nk, wide, 128), F32), pltpu.VMEM((nk, wide, 128), F32),
            pltpu.VMEM((9, rows, 4 * rows), F32),
            DMA((slots,)), DMA((2, blocks // 4)), DMA((slots,)),
        ],
        compiler_params=pltpu.CompilerParams(vmem_limit_bytes=VMEM_LIMIT),
    )(q, k, v)


def layer_kernel(layer, last, n_dev, n_o, n_f, n_k, n_q, *refs):
    if last:
        (o_ref, x_ref, ln_ref, wo_ref, wg_ref, wu_ref, wd_ref, out_ref,
         att, y_ref, c_ref, acc, act, ybuf, ysend, yrecv, osend, orecv) = refs
    else:
        (o_ref, x_ref, ln_ref, qk_ref, cos_ref, sin_ref, wo_ref, wg_ref, wu_ref, wd_ref, wk_ref, wv_ref, wq_ref,
         h_ref, q_ref, k_all, v_all,
         att, y_ref, c_ref, acc, act, qst, kst, vst, hsem, qsem, ksend, krecv, fsem) = refs
        keys = KeyValues(k_all, v_all, ksend, krecv, fsem)
        hd = qk_ref.shape[-1]
    i = pl.program_id(0)
    half = y_ref.shape[1]
    rows = half // 3
    tn = wo_ref.shape[-1]
    span = n_f + 1 + n_k + n_k + n_q

    def slot_of(ch, m):
        _, _, _, special, row = placement()
        return chunk_slot(ch, m, special, row)

    def place_of(ch, m):
        _, _, core, special, row = placement()
        return slot_place(chunk_slot(ch, m, special, row), core, special, row)

    def slot_rows(s):
        return pl.ds(pl.multiple_of(s * rows, rows), rows)

    def own_rows(m):
        return pl.ds(m * rows, rows)

    def gain(which, l=layer):
        return ln_ref[l, which : which + 1, :].astype(F32)

    def c_of(y):
        return norm_rows(y.astype(F32), gain(2)).astype(BF16)

    @pl.when(i == 0)
    def _():
        signal_group(n_dev)

    @pl.when(i < n_o)
    def _():
        part = jnp.dot(o_ref[...], wo_ref[0], preferred_element_type=F32).astype(BF16)
        att[:, pl.ds(pl.multiple_of(i * tn, tn), tn)] = part

    @pl.when(i == n_o - 1)
    def _():
        for ch in range(2):
            for m in range(3):
                r = slot_rows(slot_of(ch, m))
                y = x_ref[r, :].astype(F32) + norm_rows(att[r, :].astype(F32), gain(1))
                y = y.astype(BF16)
                y_ref[ch, own_rows(m), :] = y
                if ch == 0:
                    c_ref[own_rows(m), :] = c_of(y)

    t = i - n_o

    def up(slot):
        gate = jnp.dot(c_ref[...], wg_ref[0], preferred_element_type=F32)
        val = jnp.dot(c_ref[...], wu_ref[0], preferred_element_type=F32)
        act[slot] = (jax.nn.gelu(gate, approximate=True) * val).astype(BF16)

    def down(slot):
        return jnp.dot(act[slot], wd_ref[0], preferred_element_type=F32)

    j = jnp.where(t >= span, t - span, t)

    @pl.when((t >= 0) & (j == 0))
    def _():
        up(0)

    @pl.when((t >= 0) & (j == 1))
    def _():
        acc[...] = down(0)
        up(1)

    for parity in range(2):

        @pl.when((t >= 0) & (j > 1) & (j < n_f) & ((j & 1) == parity))
        def _():
            acc[...] += down(1 - parity)
            up(parity)

    @pl.when((t >= 0) & (j == n_f))
    def _():
        acc[...] += down((n_f - 1) % 2)

    def result(m, y):
        val = acc[own_rows(m), :].astype(BF16).astype(F32)
        return (y.astype(F32) + norm_rows(val, gain(3))).astype(BF16)

    if last:
        def sent(ch, m):
            b, blk = place_of(ch, m)
            src = y_ref.at[ch, own_rows(m)]
            if ch == 0:
                far = lambda: remote(src, out_ref.at[b], osend.at[m], orecv.at[b], blk)
                return blk, far, lambda: local(src, out_ref.at[b], orecv.at[b])
            return blk, lambda: remote(src, ybuf.at[b // 2], ysend.at[m], yrecv.at[b // 2], blk), None

        def owned(ch, m):
            me = lax.axis_index("cp")
            turn = (me // 2) % 2
            b = 2 * m + (turn if ch == 0 else 1 - turn)
            return b, home_of(b, me)[0]

        @pl.when(t == 1)
        def _():
            wait_group(n_dev)
            me = lax.axis_index("cp")
            for m in range(3):
                dev, far, _ = sent(1, m)

                @pl.when(dev != me)
                def _():
                    far().start()

        @pl.when(t == n_f)
        def _():
            me = lax.axis_index("cp")
            for m in range(3):
                y_ref[0, own_rows(m), :] = result(m, y_ref[0, own_rows(m), :])
            for m in range(3):
                b, dev = owned(1, m)

                @pl.when(dev != me)
                def _():
                    remote(ybuf.at[m], ybuf.at[m], ysend.at[m], yrecv.at[m], me).wait_recv()

            for m in range(3):
                b, blk = place_of(1, m)

                @pl.when(blk == me)
                def _():
                    ybuf[b // 2] = y_ref[1, own_rows(m), :]

            for m in range(3):
                c_ref[own_rows(m), :] = c_of(ybuf[m])

        @pl.when(t == span + 1)
        def _():
            me = lax.axis_index("cp")
            for m in range(3):
                dev, far, near = sent(0, m)

                @pl.when(dev != me)
                def _():
                    far().start()

                @pl.when(dev == me)
                def _():
                    near().start()

        @pl.when(t == span + n_f)
        def _():
            me = lax.axis_index("cp")
            for m in range(3):
                ybuf[m] = result(m, ybuf[m])
            for m in range(3):
                b, _ = owned(1, m)
                local(ybuf.at[m], out_ref.at[b], orecv.at[b]).start()
            for ch in range(2):
                for m in range(3):
                    dev, far, _ = sent(ch, m)

                    @pl.when(dev != me)
                    def _():
                        far().wait_send()

            for b in range(6):
                local(out_ref.at[b], out_ref.at[b], orecv.at[b]).wait()

        return

    for ch in range(2):

        @pl.when(t == ch * span + n_f)
        def _():
            for m in range(3):
                h = result(m, y_ref[ch, own_rows(m), :])
                y_ref[ch, own_rows(m), :] = h
                c_ref[own_rows(m), :] = norm_rows(h.astype(F32), gain(0, layer + 1)).astype(BF16)

        if ch == 1:
            @pl.when(t == span + n_f)
            def _():
                for m in range(3):
                    s = slot_of(0, m)
                    keys.wait_sent(s, (kst.at[m], vst.at[m]))
                    local(qst.at[m], q_ref.at[s], qsem.at[s]).wait()

        def turn(m):
            r = slot_rows(slot_of(ch, m))
            return cos_ref[r, :], sin_ref[r, :]

        def heads(w_ref, put):
            for h in range(w_ref.shape[-1] // hd):
                raw = jnp.dot(c_ref[...], w_ref[0, :, h * hd : (h + 1) * hd], preferred_element_type=F32)
                for m in range(3):
                    put(h, m, raw[m * rows : (m + 1) * rows])

        u = t - (ch * span + n_f + 1)
        per = wk_ref.shape[-1] // hd

        @pl.when((u >= 0) & (u < n_k))
        def _():
            def put(h, m, raw):
                col = pl.ds(pl.multiple_of((u * per + h) * hd, hd), hd)
                kst[m, :, col] = norm_turn(raw, qk_ref[layer + 1, 1:2, :].astype(F32), *turn(m))

            heads(wk_ref, put)

        @pl.when((u >= n_k) & (u < 2 * n_k))
        def _():
            def put(h, m, raw):
                col = pl.ds(pl.multiple_of(((u - n_k) * per + h) * hd, hd), hd)
                vst[m, :, col] = raw.astype(BF16)

            heads(wv_ref, put)

        @pl.when((u >= 2 * n_k) & (u < 2 * n_k + n_q))
        def _():
            def put(h, m, raw):
                out = norm_turn(raw, qk_ref[layer + 1, 0:1, :].astype(F32), *turn(m))
                qst[m, (u - 2 * n_k) * per + h] = out * BF16(hd**-0.5)

            heads(wq_ref, put)

        @pl.when(u == 2 * n_k)
        def _():
            if ch == 0:
                wait_group(n_dev)
            for m in range(3):
                s = slot_of(ch, m)
                keys.start(s, (kst.at[m], vst.at[m]))
                local(y_ref.at[ch, own_rows(m)], h_ref.at[s], hsem.at[s]).start()

        @pl.when(u == 2 * n_k + n_q - 1)
        def _():
            for m in range(3):
                s = slot_of(ch, m)
                local(qst.at[m], q_ref.at[s], qsem.at[s]).start()

    @pl.when(t == span - 1)
    def _():
        for m in range(3):
            c_ref[own_rows(m), :] = c_of(y_ref[1, own_rows(m), :])

    @pl.when(i == pl.num_programs(0) - 1)
    def _():
        for m in range(3):
            s = slot_of(1, m)
            keys.wait_sent(s, (kst.at[m], vst.at[m]))
            local(qst.at[m], q_ref.at[s], qsem.at[s]).wait()
        for s in range(6):
            local(y_ref.at[0, own_rows(0)], h_ref.at[s], hsem.at[s]).wait()
        keys.wait_all(6)


def after_attention(layer, last, n_dev, cid, o, x, ln_w, w_o, w_gate, w_up, w_down, more=()):
    slots, rows, dim = x.shape
    inner, ff = w_o.shape[1], w_gate.shape[-1]
    total = slots * rows
    half = total // 2
    blocks = 16
    tn, tf = min(256, dim), min(768 if last and ff % 768 == 0 else 512, ff)
    n_o, n_f = dim // tn, ff // tf
    o2, x2 = o.reshape(total, inner), x.reshape(total, dim)
    n_k = n_q = 0
    if not last:
        qk_w, cos, sin, w_q, w_k, w_v = more
        hd = qk_w.shape[-1]
        wide = 2 * hd
        n_k, n_q = w_k.shape[-1] // wide, w_q.shape[-1] // wide
    span = n_f + 1 + 2 * n_k + n_q
    one = lambda a: pl.BlockSpec(a.shape, lambda i: (0,) * a.ndim, pipeline_mode=pl.Buffered(1))

    def at_step(i):
        t = i - n_o
        return jnp.where(t >= span, t - span, t)

    def at_f(i):
        return jnp.clip(at_step(i), 0, n_f - 1)

    def next_w(lo, n):
        return lambda i: (layer + 1, 0, jnp.clip(at_step(i) - (n_f + 1 + lo), 0, n - 1))

    mlp_specs = [
        pl.BlockSpec((1, inner, tn), lambda i: (layer, 0, jnp.minimum(i, n_o - 1))),
        pl.BlockSpec((1, dim, tf), lambda i: (layer, 0, at_f(i))),
        pl.BlockSpec((1, dim, tf), lambda i: (layer, 0, at_f(i))),
        pl.BlockSpec((1, tf, dim), lambda i: (layer, at_f(i - 1), 0)),
    ]
    work = [
        pltpu.VMEM((total, dim), BF16), pltpu.VMEM((2, half, dim), BF16), pltpu.VMEM((half, dim), BF16),
        pltpu.VMEM((half, dim), F32), pltpu.VMEM((2, half, tf), BF16),
    ]
    params = pltpu.CompilerParams(
        dimension_semantics=("arbitrary",), collective_id=cid, has_side_effects=True, vmem_limit_bytes=VMEM_LIMIT
    )
    body = functools.partial(layer_kernel, layer, last, n_dev, n_o, n_f, n_k, n_q)
    if last:
        return pl.pallas_call(
            body, grid=(n_o + 2 * span,),
            in_specs=[one(o2), one(x2), one(ln_w)] + mlp_specs,
            out_specs=ANY,
            out_shape=jax.ShapeDtypeStruct(x.shape, BF16),
            scratch_shapes=work + [pltpu.VMEM((3, rows, dim), BF16), DMA((3,)), DMA((3,)), DMA((3,)), DMA((slots,))],
            compiler_params=params,
        )(o2, x2, ln_w, w_o, w_gate, w_up, w_down)
    nq, nk = w_q.shape[-1] // hd, w_k.shape[-1] // hd
    q_shape, kv_shape = (slots, nq, rows, hd), (blocks, rows, nk * hd)
    return pl.pallas_call(
        body, grid=(n_o + 2 * span,),
        in_specs=[one(o2), one(x2), one(ln_w), one(qk_w), one(cos), one(sin)] + mlp_specs + [
            pl.BlockSpec((1, dim, wide), next_w(0, n_k)),
            pl.BlockSpec((1, dim, wide), next_w(n_k, n_k)),
            pl.BlockSpec((1, dim, wide), next_w(2 * n_k, n_q)),
        ],
        out_specs=[ANY] * 4,
        out_shape=[jax.ShapeDtypeStruct(a, BF16) for a in (x.shape, q_shape, kv_shape, kv_shape)],
        scratch_shapes=work + [
            pltpu.VMEM((3, nq, rows, hd), BF16), pltpu.VMEM((3, rows, nk * hd), BF16), pltpu.VMEM((3, rows, nk * hd), BF16),
            DMA((slots,)), DMA((slots,)), DMA((2, 3, slots)), DMA((2, blocks)), DMA((2, 2)),
        ],
        compiler_params=params,
    )(o2, x2, ln_w, qk_w, cos, sin, w_o, w_gate, w_up, w_down, w_k, w_v, w_q)


def rope_tables(pos, hd):
    half = hd // 2
    out = []
    for base, scale in ((LOCAL_BASE, 1.0), (GLOBAL_BASE, GLOBAL_SCALE)):
        freq = base ** (-2.0 * jnp.arange(half, dtype=jnp.float32) / hd)
        ang = (pos.astype(jnp.float32) / scale)[:, None] * freq[None, :]
        out += [jnp.cos(ang), jnp.sin(ang)]
    return out


def solution(mesh):
    n_dev = mesh.shape["cp"]

    def device_fn(x_loc, ln_w, qk_w, w_q, w_k, w_v, w_o, w_gate, w_up, w_down):
        slots, rows, dim = x_loc.shape
        _, _, core, special, row = placement()
        blk = jnp.stack([slot_place(s, core, special, row)[1] for s in range(slots)])
        pos = (blk[:, None] * rows + jnp.arange(rows)[None, :]).reshape(-1)
        cos0, sin0, cos1, sin1 = rope_tables(pos, qk_w.shape[-1])
        x, q, k, v = first(n_dev, x_loc, ln_w, qk_w, cos0, sin0, w_q, w_k, w_v)
        o = attention(WINDOW, q, k, v)
        mlp = (w_o, w_gate, w_up, w_down)
        x, q, k, v = after_attention(0, False, n_dev, 1, o, x, ln_w, *mlp, more=(qk_w, cos1, sin1, w_q, w_k, w_v))
        o = attention(None, q, k, v)
        return after_attention(1, True, n_dev, 2, o, x, ln_w, *mlp)

    act_part = P("dp", "cp", None)
    return jax.shard_map(device_fn, mesh=mesh, in_specs=(act_part,) + (P(),) * 9, out_specs=act_part, check_vma=False)
```

```python
import functools

import jax
import jax.numpy as jnp
from jax import lax
from jax.experimental import pallas as pl
from jax.experimental.pallas import tpu as pltpu
from jax.sharding import PartitionSpec as P

WINDOW = 1024
NORM_EPS = 1e-6
LOCAL_BASE = 10000.0
GLOBAL_BASE = 1000000.0
GLOBAL_SCALE = 8.0
NEG = -1e30

ROW_CHIP = (0, 3, 4, 1, 5, 6)
SPECIAL = (2, 7)
VMEM_LIMIT = 64 * 1024 * 1024 - 128 * 1024
MESH = pl.DeviceIdType.MESH
BF16, F32 = jnp.bfloat16, jnp.float32
ANY = pl.BlockSpec(memory_space=pl.ANY)
WHOLE = pl.BlockSpec(memory_space=pltpu.VMEM)
DMA = pltpu.SemaphoreType.DMA


def pick(idx, table):
    out = jnp.int32(table[-1])
    for i in range(len(table) - 2, -1, -1):
        out = jnp.where(idx == i, jnp.int32(table[i]), out)
    return out


def placement():
    me = lax.axis_index("cp")
    chip, core = me // 2, me % 2
    roles = [0] * 8
    rows = [0] * 8
    for b, c in enumerate(ROW_CHIP):
        rows[c] = b
    for i, c in enumerate(SPECIAL):
        roles[c] = 1
        rows[c] = 3 * i
    return me, chip, core, pick(chip, roles), pick(chip, rows)


def slot_place(s, core, special, row):
    k = s % 2
    blk = jnp.where(special == 1, 2 * k + (k + core) % 2, 4 + 2 * s + (s + core) % 2)
    b = jnp.where(special == 1, row + s // 2, row)
    return b, blk


def ring(a, b):
    return min((a - b) % 8, (b - a) % 8)


ARRIVAL = [sorted(range(6), key=lambda s: (ring(2 + s, c), s)) for c in range(8)]
for c in SPECIAL:
    ARRIVAL[c] = [4, 5, 0, 2, 1, 3]


def home_of(b, blk):
    core = ((blk + 1) // 2) % 2
    half = blk // 2
    chip = jnp.where(blk < 4, pick(b // 3, SPECIAL), pick(b, ROW_CHIP))
    slot = jnp.where(blk < 4, (b % 3) * 2 + half, half - 2)
    return chip * 2 + core, slot


def chunk_slot(ch, i, special, row):
    b = jnp.where(special == 1, row + i, row)
    return 2 * i + (b % 2 if ch == 0 else 1 - b % 2)


def kv_index(s, core, special, row):
    _, blk = slot_place(s, core, special, row)
    return jnp.where(special == 1, (s // 2) * 4 + blk, blk)


def served(row, r):
    return jnp.where(row == 0, ROW_CHIP[r], ROW_CHIP[r + 3])


def signal_group(n_dev):
    me = lax.axis_index("cp")
    barrier = pltpu.get_barrier_semaphore()
    for d in range(1, n_dev):
        pl.semaphore_signal(barrier, inc=1, device_id={"cp": lax.rem(me + d, n_dev)}, device_id_type=MESH)


def wait_group(n_dev):
    pl.semaphore_wait(pltpu.get_barrier_semaphore(), n_dev - 1)


def remote(src, dst, send, recv, dev):
    return pltpu.make_async_remote_copy(
        src_ref=src, dst_ref=dst, send_sem=send, recv_sem=recv, device_id={"cp": dev}, device_id_type=MESH
    )


def local(src, dst, sem):
    return pltpu.make_async_copy(src, dst, sem)


def norm_rows(vals, gain):
    inv = lax.rsqrt(jnp.mean(vals * vals, axis=-1, keepdims=True) + NORM_EPS)
    return vals * inv * (1.0 + gain)


def norm_turn(raw, gain, cos, sin):
    half = raw.shape[-1] // 2
    vals = norm_rows(raw.astype(BF16).astype(F32), gain)
    first, second = vals[:, :half], vals[:, half:]
    return jnp.concatenate([first * cos - second * sin, second * cos + first * sin], axis=-1).astype(BF16)


class KeyValues:
    def __init__(self, k_all, v_all, send, recv, fwd):
        self.both = ((0, k_all), (1, v_all))
        self.send, self.recv, self.fwd = send, recv, fwd

    def here(self):
        _, chip, self.core, self.special, self.row = placement()
        self.mate = chip * 2 + 1 - self.core

    def _copies(self, s, stage):
        idx = kv_index(s, self.core, self.special, self.row)
        _, blk = slot_place(s, self.core, self.special, self.row)
        dev = served(self.row, 0) * 2 + self.core
        for r in (1, 2):
            dev = jnp.where(s // 2 == r, served(self.row, r) * 2 + self.core, dev)
        out = []
        for x, full in self.both:
            out.append((
                local(stage[x], full.at[idx], self.send.at[x, 0, s]),
                remote(stage[x], full.at[idx], self.send.at[x, 1, s], self.recv.at[x, idx], self.mate),
                remote(stage[x], full.at[blk], self.send.at[x, 2, s], self.recv.at[x, blk], dev),
            ))
        return out

    def start(self, s, stage):
        self.here()
        for own, mate, row in self._copies(s, stage):

            @pl.when(self.special == 1)
            def _():
                row.start()

            mate.start()
            own.start()

    def wait_sent(self, s, stage):
        self.here()
        for own, mate, row in self._copies(s, stage):
            own.wait()
            mate.wait_send()

            @pl.when(self.special == 1)
            def _():
                row.wait_send()

    def wait_all(self, slots):
        self.here()
        for x, full in self.both:

            @pl.when(self.special == 0)
            def _():
                for k in range(2):
                    blk = 2 * k + (k + self.core) % 2
                    remote(full.at[blk], full.at[blk], self.fwd.at[x, k], self.recv.at[x, blk], self.mate).wait_recv()
                    remote(full.at[blk], full.at[blk], self.fwd.at[x, k], self.recv.at[x, blk], self.mate).start()

            for s in range(slots):
                idx = kv_index(s, 1 - self.core, self.special, self.row)
                remote(full.at[idx], full.at[idx], self.fwd.at[x, 0], self.recv.at[x, idx], self.mate).wait_recv()

        @pl.when(self.special == 0)
        def _():
            for x, full in self.both:
                for k in range(2):
                    blk = 2 * k + (k + 1 - self.core) % 2
                    remote(full.at[blk], full.at[blk], self.fwd.at[x, k], self.recv.at[x, blk], self.mate).wait()


def first_kernel(n_dev, nq, nk, x_ref, ln_ref, qk_ref, cos_ref, sin_ref, wq_ref, wk_ref, wv_ref,
                 h_ref, q_ref, k_all, v_all, xbuf, abuf, wq, wk, wv, qst, kst, vst,
                 wsem, xsend, xrecv, hsem, qsem, ksend, krecv, fsem):
    me, chip, core, special, row = placement()
    n, rows, dim = x_ref.shape
    hd = qk_ref.shape[-1]
    homes = [home_of(jnp.int32(b), me) for b in range(n)]
    keys = KeyValues(k_all, v_all, ksend, krecv, fsem)

    signal_group(n_dev)
    for b, (dev, slot) in enumerate(homes):

        @pl.when(dev == me)
        def _():
            local(x_ref.at[b], xbuf.at[slot], xrecv.at[slot]).start()

    weights = ((wk_ref, wk), (wv_ref, wv), (wq_ref, wq))
    for j, (src, dst) in enumerate(weights):
        local(src.at[0], dst, wsem.at[j]).start()
    wait_group(n_dev)
    for b in SEND_ORDER:
        dev, slot = homes[b]

        @pl.when(dev != me)
        def _():
            remote(x_ref.at[b], xbuf.at[slot], xsend.at[b], xrecv.at[slot], dev).start()

    gain = ln_ref[0, 0:1, :].astype(F32)

    def take(pair):
        places = [pick(chip, [ARRIVAL[c][2 * pair + j] for c in range(8)]) for j in range(2)]
        for j, s in enumerate(places):
            local(xbuf.at[s], xbuf.at[s], xrecv.at[s]).wait()
            local(xbuf.at[s], h_ref.at[s], hsem.at[s]).start()
            abuf[j * rows : (j + 1) * rows, :] = norm_rows(xbuf[s].astype(F32), gain).astype(BF16)
        return places

    def tables(s):
        r = pl.ds(pl.multiple_of(s * rows, rows), rows)
        return cos_ref[r, :], sin_ref[r, :]

    def product(w, h):
        return jnp.dot(abuf[...], w[:, pl.ds(pl.multiple_of(h * hd, hd), hd)], preferred_element_type=F32)

    for pair in range(n // 2):
        places = take(pair)
        if pair == 0:
            local(wk_ref.at[0], wk, wsem.at[0]).wait()
            local(wv_ref.at[0], wv, wsem.at[1]).wait()
        turn = [tables(s) for s in places]
        k_gain = qk_ref[0, 1:2, :].astype(F32)
        q_gain = qk_ref[0, 0:1, :].astype(F32)

        @pl.loop(0, nk)
        def _(h):
            col = pl.ds(pl.multiple_of(h * hd, hd), hd)
            k_raw, v_raw = product(wk, h), product(wv, h)
            for j, s in enumerate(places):
                part = slice(j * rows, (j + 1) * rows)
                kst[s, :, col] = norm_turn(k_raw[part], k_gain, *turn[j])
                vst[s, :, col] = v_raw[part].astype(BF16)

        if pair == 0:
            local(wq_ref.at[0], wq, wsem.at[2]).wait()

        def query(h):
            raw = product(wq, h)
            for j, s in enumerate(places):
                part = slice(j * rows, (j + 1) * rows)
                qst[s, h] = norm_turn(raw[part], q_gain, *turn[j]) * BF16(hd**-0.5)

        query(0)
        for s in places:
            keys.start(s, (kst.at[s], vst.at[s]))
        pl.loop(1, nq)(query)
        for s in places:
            local(qst.at[s], q_ref.at[s], qsem.at[s]).start()

    for s in range(n):
        keys.wait_sent(s, (kst.at[s], vst.at[s]))
        local(qst.at[s], q_ref.at[s], qsem.at[s]).wait()
        local(xbuf.at[s], h_ref.at[s], hsem.at[s]).wait()
    for b, (dev, slot) in enumerate(homes):

        @pl.when(dev != me)
        def _():
            remote(x_ref.at[b], xbuf.at[slot], xsend.at[b], xrecv.at[slot], dev).wait_send()

    keys.wait_all(n)


SEND_ORDER = (2, 5, 0, 3, 1, 4)


def first(n_dev, x, ln_w, qk_w, cos, sin, w_q, w_k, w_v):
    n, rows, dim = x.shape
    hd = qk_w.shape[-1]
    nq, nk = w_q.shape[-1] // hd, w_k.shape[-1] // hd
    blocks = 16
    q_shape, s_shape, kv_shape = (n, nq, rows, hd), (n, rows, nk * hd), (blocks, rows, nk * hd)
    return pl.pallas_call(
        functools.partial(first_kernel, n_dev, nq, nk),
        out_shape=[jax.ShapeDtypeStruct(a, BF16) for a in (x.shape, q_shape, kv_shape, kv_shape)],
        in_specs=[ANY, WHOLE, WHOLE, WHOLE, WHOLE, ANY, ANY, ANY],
        out_specs=[ANY] * 4,
        scratch_shapes=[
            pltpu.VMEM(x.shape, BF16), pltpu.VMEM((2 * rows, dim), BF16),
            pltpu.VMEM(w_q.shape[1:], BF16), pltpu.VMEM(w_k.shape[1:], BF16), pltpu.VMEM(w_v.shape[1:], BF16),
            pltpu.VMEM(q_shape, BF16), pltpu.VMEM(s_shape, BF16), pltpu.VMEM(s_shape, BF16),
            DMA((3,)), DMA((n,)), DMA((n,)), DMA((n,)), DMA((n,)), DMA((2, 3, n)), DMA((2, blocks)), DMA((2, 2)),
        ],
        compiler_params=pltpu.CompilerParams(collective_id=0, has_side_effects=True, vmem_limit_bytes=VMEM_LIMIT),
    )(x, ln_w, qk_w, cos, sin, w_q, w_k, w_v)


def attn_kernel(window_blocks, q_ref, k_ref, v_ref, o_ref, kbuf, vbuf, qbuf, obuf, sbuf, wacc, wm, wl, bias, qsem, ksem, osem):
    _, _, core, special, row = placement()
    slots, nq, rows, hd = q_ref.shape
    nk = k_ref.shape[-1] // hd
    rep = nq // nk
    per = 4
    tile = per * rows
    tiles = k_ref.shape[0] // per

    def loads(t):
        part = pl.ds(t * per, per)
        return [local(k_ref.at[part], kbuf.at[part], ksem.at[0, t]), local(v_ref.at[part], vbuf.at[part], ksem.at[1, t])]

    for s in range(slots):
        local(q_ref.at[s], qbuf.at[s], qsem.at[s]).start()
    for t in range(tiles):
        for c in loads(t):
            c.start()

    qi = lax.broadcasted_iota(jnp.int32, (rows, tile), 0)
    ki = lax.broadcasted_iota(jnp.int32, (rows, tile), 1)
    bias[0] = jnp.zeros((rows, tile), jnp.float32)
    for j in range(per):
        bias[1 + j] = jnp.where(ki <= qi + j * rows, 0.0, NEG)
        if window_blocks is not None:
            bias[1 + per + j] = jnp.where(ki > qi + j * rows, 0.0, NEG)

    def start_tile(blk):
        if window_blocks is None:
            return jnp.int32(0)
        return jnp.maximum(blk - window_blocks, 0) // per

    def scores(s, t, base, blk):
        edge = jnp.where(t == blk // per, 1 + blk % per, 0)
        if window_blocks is not None:
            old = blk - window_blocks
            edge = jnp.where((old >= 0) & (t == old // per), 1 + per + old % per, edge)
        off = bias[edge][None]
        kt = kbuf.at[pl.ds(base + per * t, per)]
        out = []
        for g in range(nk):
            q2 = qbuf[s, g * rep : (g + 1) * rep].reshape(rep * rows, hd)
            kk = kt[:, :, g * hd : (g + 1) * hd].reshape(tile, hd)
            sc = lax.dot_general(q2, kk, (((1,), (1,)), ((), ())), preferred_element_type=jnp.float32)
            out.append((sc.reshape(rep, rows, tile) + off).reshape(rep * rows, tile))
        return out

    lanes = 128

    def columns(val, op):
        parts = [val[:, j * lanes : (j + 1) * lanes] for j in range(tile // lanes)]
        return functools.reduce(op, parts)

    def spread(val):
        return jnp.concatenate([val] * (tile // lanes), axis=1)

    def row_max(val):
        return jnp.broadcast_to(jnp.max(val, axis=-1, keepdims=True), val.shape)

    def values(t, base, g):
        return vbuf.at[pl.ds(base + per * t, per)][:, :, g * hd : (g + 1) * hd].reshape(tile, hd)

    def finish(s, total, weight):
        for g in range(nk):
            out = (total[g] / jnp.sum(weight[g], axis=-1, keepdims=True)).astype(jnp.bfloat16)
            for h in range(rep):
                lo = (g * rep + h) * hd
                obuf[s, :, lo : lo + hd] = out[h * rows : (h + 1) * rows]
        local(obuf.at[s], o_ref.at[s], osem.at[s]).start()

    for t in range(tiles):
        for c in loads(t):
            c.wait()

    @pl.loop(0, slots)
    def _(s):
        _, blk = slot_place(s, core, special, row)
        base = jnp.where(special == 1, (s // 2) * per, 0)
        first = start_tile(blk)
        last = blk // per + 1
        local(q_ref.at[s], qbuf.at[s], qsem.at[s]).wait()
        for g in range(nk):
            wm[g] = jnp.full(wm.shape[1:], NEG, F32)
            wl[g] = jnp.zeros(wl.shape[1:], F32)
            wacc[g] = jnp.zeros(wacc.shape[1:], F32)

        @pl.loop(first, last)
        def _(t):
            for g, sc in enumerate(scores(s, t, base, blk)):
                sbuf[g, t] = sc
                wm[g] = jnp.maximum(wm[g], columns(sc, jnp.maximum))

        for g in range(nk):
            wm[g] = row_max(wm[g])

        @pl.loop(first, last)
        def _(t):
            for g in range(nk):
                p = jnp.exp(sbuf[g, t] - spread(wm[g]))
                wl[g] += columns(p, jnp.add)
                wacc[g] += jnp.dot(p.astype(BF16), values(t, base, g), preferred_element_type=F32)

        finish(s, [wacc[g] for g in range(nk)], [wl[g] for g in range(nk)])

    for s in range(slots):
        local(obuf.at[s], o_ref.at[s], osem.at[s]).wait()


def attention(window, q, k, v):
    slots, nq, rows, hd = q.shape
    blocks = k.shape[0]
    nk = k.shape[-1] // hd
    wide = nq // nk * rows
    return pl.pallas_call(
        functools.partial(attn_kernel, None if window is None else window // rows),
        out_shape=jax.ShapeDtypeStruct((slots, rows, nq * hd), BF16),
        in_specs=[ANY] * 3,
        out_specs=ANY,
        scratch_shapes=[
            pltpu.VMEM(k.shape, BF16), pltpu.VMEM(v.shape, BF16), pltpu.VMEM(q.shape, BF16),
            pltpu.VMEM((slots, rows, nq * hd), BF16),
            pltpu.VMEM((nk, blocks // 4, wide, 4 * rows), F32),
            pltpu.VMEM((nk, wide, hd), F32), pltpu.VMEM((nk, wide, 128), F32), pltpu.VMEM((nk, wide, 128), F32),
            pltpu.VMEM((9, rows, 4 * rows), F32),
            DMA((slots,)), DMA((2, blocks // 4)), DMA((slots,)),
        ],
        compiler_params=pltpu.CompilerParams(vmem_limit_bytes=VMEM_LIMIT),
    )(q, k, v)


class Ring:
    def __init__(self, buf, sem, count, source):
        self.buf, self.sem, self.count, self.source = buf, sem, count, source
        self.depth = buf.shape[0]

    def begin(self):
        for t in range(min(self.depth, self.count)):
            self.start(t, t)

    def start(self, t, slot):
        self.source(t, lambda ref: local(ref, self.buf.at[slot], self.sem.at[slot]).start())

    def get(self, t):
        slot = lax.rem(t, self.depth) if not isinstance(t, int) else t % self.depth
        local(self.buf.at[slot], self.buf.at[slot], self.sem.at[slot]).wait()
        return self.buf.at[slot]

    def free(self, t):
        new = t + self.depth
        if isinstance(t, int):
            if new < self.count:
                self.start(new, t % self.depth)
            return

        @pl.when(new < self.count)
        def _():
            self.start(new, lax.rem(t, self.depth))


def layer_kernel(layer, last, n_dev, *refs):
    if last:
        (o_ref, x_ref, ln_ref, wo_ref, wg_ref, wu_ref, wd_ref, out_ref,
         obuf, y_ref, att, c_ref, acc, act, wo, wg, wu, wd, isem, osem, gsem, usem, dsem,
         ybuf, ysend, yrecv, osend, orecv) = refs
    else:
        (o_ref, x_ref, ln_ref, qk_ref, cos_ref, sin_ref, wo_ref, wg_ref, wu_ref, wd_ref, wk_ref, wv_ref, wq_ref,
         h_ref, q_ref, k_all, v_all,
         obuf, y_ref, att, c_ref, acc, act, wo, wg, wu, wd, isem, osem, gsem, usem, dsem,
         wn, nsem, qst, kst, vst, hsem, qsem, ksend, krecv, fsem) = refs
        keys = KeyValues(k_all, v_all, ksend, krecv, fsem)
        hd = qk_ref.shape[-1]
        nk, nq = wk_ref.shape[-1] // hd, wq_ref.shape[-1] // hd
    rows = acc.shape[0] // 3
    tn, tf = wo.shape[-1], wg.shape[-1]
    n_o, n_f = wo_ref.shape[-1] // tn, wg_ref.shape[-1] // tf

    def cols(t, width):
        start = t * width
        return pl.ds(start if isinstance(t, int) else pl.multiple_of(start, width), width)

    def tile_f(t):
        return (t % n_f) if isinstance(t, int) else lax.rem(t, n_f)

    o_ring = Ring(wo, osem, n_o, lambda t, put: put(wo_ref.at[layer, :, cols(t, tn)]))
    g_ring = Ring(wg, gsem, 2 * n_f, lambda t, put: put(wg_ref.at[layer, :, cols(tile_f(t), tf)]))
    u_ring = Ring(wu, usem, 2 * n_f, lambda t, put: put(wu_ref.at[layer, :, cols(tile_f(t), tf)]))
    d_ring = Ring(wd, dsem, 2 * n_f, lambda t, put: put(wd_ref.at[layer, cols(tile_f(t), tf), :]))

    in_o = local(o_ref, obuf, isem.at[0])
    in_x = local(x_ref, y_ref, isem.at[1])
    in_o.start()
    o_ring.begin()
    in_x.start()
    for r in (g_ring, u_ring, d_ring):
        r.begin()
    signal_group(n_dev)

    def slot_of(ch, m):
        _, _, _, special, row = placement()
        return chunk_slot(ch, m, special, row)

    def place_of(ch, m):
        _, _, core, special, row = placement()
        return slot_place(chunk_slot(ch, m, special, row), core, special, row)

    def slot_rows(s):
        return pl.ds(pl.multiple_of(s * rows, rows), rows)

    def own_rows(m):
        return pl.ds(m * rows, rows)

    def y_at(ch, m):
        return y_ref.at[slot_rows(slot_of(ch, m))]

    def gain(which, l=layer):
        return ln_ref[l, which : which + 1, :].astype(F32)

    def c_of(y):
        return norm_rows(y.astype(F32), gain(2)).astype(BF16)

    in_o.wait()

    @pl.loop(0, n_o)
    def _(t):
        tile = o_ring.get(t)
        att[:, cols(t, tn)] = jnp.dot(obuf[...], tile[...], preferred_element_type=F32).astype(BF16)
        o_ring.free(t)

    in_x.wait()
    for ch in range(2):
        for m in range(3):
            r = slot_rows(slot_of(ch, m))
            y = y_ref[r, :].astype(F32) + norm_rows(att[r, :].astype(F32), gain(1))
            y = y.astype(BF16)
            y_ref[r, :] = y
            if ch == 0 or not last:
                c_ref[ch, own_rows(m), :] = c_of(y)

    def up(ch, t, to):
        gate = jnp.dot(c_ref[ch], g_ring.get(t)[...], preferred_element_type=F32)
        val = jnp.dot(c_ref[ch], u_ring.get(t)[...], preferred_element_type=F32)
        act[to] = (jax.nn.gelu(gate, approximate=True) * val).astype(BF16)
        g_ring.free(t)
        u_ring.free(t)

    def down(t, at):
        acc[...] += jnp.dot(act[at], d_ring.get(t)[...], preferred_element_type=F32)
        d_ring.free(t)

    def mlp(ch, after_first):
        base = ch * n_f
        acc[...] = jnp.zeros(acc.shape, F32)
        up(ch, base, 0)
        after_first()

        @pl.loop(1, n_f)
        def _(t):
            even = lax.rem(t, 2)
            down(base + t - 1, 1 - even)
            up(ch, base + t, even)

        down(base + n_f - 1, (n_f - 1) % 2)

    def result(m, y):
        val = acc[own_rows(m), :].astype(BF16).astype(F32)
        return (y.astype(F32) + norm_rows(val, gain(3))).astype(BF16)

    if last:
        me = lax.axis_index("cp")

        def sent(ch, m):
            b, blk = place_of(ch, m)
            src = y_at(ch, m)
            if ch == 0:
                far = lambda: remote(src, out_ref.at[b], osend.at[m], orecv.at[b], blk)
                return blk, far, lambda: local(src, out_ref.at[b], orecv.at[b])
            return blk, lambda: remote(src, ybuf.at[b // 2], ysend.at[m], yrecv.at[b // 2], blk), None

        def owned(ch, m):
            turn = (me // 2) % 2
            b = 2 * m + (turn if ch == 0 else 1 - turn)
            return b, home_of(b, me)[0]

        def send_streams():
            wait_group(n_dev)
            for m in range(3):
                dev, far, _ = sent(1, m)

                @pl.when(dev != me)
                def _():
                    far().start()

        def send_results():
            for m in range(3):
                dev, far, near = sent(0, m)

                @pl.when(dev != me)
                def _():
                    far().start()

                @pl.when(dev == me)
                def _():
                    near().start()

        mlp(0, send_streams)
        for m in range(3):
            y_at(0, m)[...] = result(m, y_at(0, m)[...])
        for m in range(3):
            b, dev = owned(1, m)

            @pl.when(dev != me)
            def _():
                remote(ybuf.at[m], ybuf.at[m], ysend.at[m], yrecv.at[m], me).wait_recv()

        for m in range(3):
            b, blk = place_of(1, m)

            @pl.when(blk == me)
            def _():
                ybuf[b // 2] = y_at(1, m)[...]

        for m in range(3):
            c_ref[1, own_rows(m), :] = c_of(ybuf[m])
        mlp(1, send_results)
        for m in range(3):
            ybuf[m] = result(m, ybuf[m])
        for m in range(3):
            b, _ = owned(1, m)
            local(ybuf.at[m], out_ref.at[b], orecv.at[b]).start()
        for ch in range(2):
            for m in range(3):
                dev, far, _ = sent(ch, m)

                @pl.when(dev != me)
                def _():
                    far().wait_send()

        for b in range(6):
            local(out_ref.at[b], out_ref.at[b], orecv.at[b]).wait()
        return

    def source(t, put):
        kind = lax.rem(t, 2 * nk) if not isinstance(t, int) else t % (2 * nk)
        cases = (
            (jnp.logical_and(t < 4 * nk, kind < nk), lambda: put(wk_ref.at[layer + 1, :, cols(kind, hd)])),
            (jnp.logical_and(t < 4 * nk, kind >= nk), lambda: put(wv_ref.at[layer + 1, :, cols(kind - nk, hd)])),
            (t >= 4 * nk, lambda: put(wq_ref.at[layer + 1, :, cols(t - 4 * nk, hd)])),
        )
        for cond, do in cases:
            pl.when(cond)(do)

    n_ring = Ring(wn, nsem, 4 * nk + nq, source)
    n_ring.begin()
    k_gain, q_gain = (qk_ref[layer + 1, j : j + 1, :].astype(F32) for j in (1, 0))

    def turn(ch, m):
        r = slot_rows(slot_of(ch, m))
        return cos_ref[r, :], sin_ref[r, :]

    def send_keys(ch):
        for m in range(3):
            keys.start(slot_of(ch, m), (kst.at[ch, m], vst.at[ch, m]))

    def keys_and_values(ch):
        for m in range(3):
            h = result(m, y_at(ch, m)[...])
            y_at(ch, m)[...] = h
            c_ref[ch, own_rows(m), :] = norm_rows(h.astype(F32), gain(0, layer + 1)).astype(BF16)

        @pl.loop(0, nk)
        def _(h):
            t = ch * 2 * nk + h
            raw = jnp.dot(c_ref[ch], n_ring.get(t)[...], preferred_element_type=F32)
            n_ring.free(t)
            for m in range(3):
                kst[ch, m, :, cols(h, hd)] = norm_turn(raw[m * rows : (m + 1) * rows], k_gain, *turn(ch, m))

        @pl.loop(0, nk)
        def _(h):
            t = (ch * 2 + 1) * nk + h
            raw = jnp.dot(c_ref[ch], n_ring.get(t)[...], preferred_element_type=F32)
            n_ring.free(t)
            for m in range(3):
                vst[ch, m, :, cols(h, hd)] = raw[m * rows : (m + 1) * rows].astype(BF16)

        for m in range(3):
            s = slot_of(ch, m)
            local(y_at(ch, m), h_ref.at[s], hsem.at[s]).start()

    def query(h):
        t = 4 * nk + h
        tile = n_ring.get(t)
        for ch in range(2):
            raw = jnp.dot(c_ref[ch], tile[...], preferred_element_type=F32)
            for m in range(3):
                out = norm_turn(raw[m * rows : (m + 1) * rows], q_gain, *turn(ch, m))
                qst[ch, m, h] = out * BF16(hd**-0.5)
        n_ring.free(t)

    def first_keys():
        wait_group(n_dev)
        send_keys(0)

    mlp(0, lambda: None)
    keys_and_values(0)
    mlp(1, first_keys)
    keys_and_values(1)
    query(0)
    send_keys(1)
    pl.loop(1, nq)(query)
    for ch in range(2):
        for m in range(3):
            s = slot_of(ch, m)
            local(qst.at[ch, m], q_ref.at[s], qsem.at[s]).start()
    for ch in range(2):
        for m in range(3):
            s = slot_of(ch, m)
            keys.wait_sent(s, (kst.at[ch, m], vst.at[ch, m]))
            local(qst.at[ch, m], q_ref.at[s], qsem.at[s]).wait()
            local(y_at(ch, m), h_ref.at[s], hsem.at[s]).wait()
    keys.wait_all(6)


def after_attention(layer, last, n_dev, cid, o, x, ln_w, w_o, w_gate, w_up, w_down, more=()):
    slots, rows, dim = x.shape
    inner, ff = w_o.shape[1], w_gate.shape[-1]
    total = slots * rows
    half = total // 2
    blocks = 16
    tn, tf = min(256, dim), min(512, ff)
    deep = 3
    o2, x2 = o.reshape(total, inner), x.reshape(total, dim)
    work = [
        pltpu.VMEM((total, inner), BF16), pltpu.VMEM((total, dim), BF16),
        pltpu.VMEM((total, dim), BF16), pltpu.VMEM((2, half, dim), BF16),
        pltpu.VMEM((half, dim), F32), pltpu.VMEM((2, half, tf), BF16),
        pltpu.VMEM((deep, inner, tn), BF16), pltpu.VMEM((deep, dim, tf), BF16), pltpu.VMEM((deep, dim, tf), BF16),
        pltpu.VMEM((deep, tf, dim), BF16),
        DMA((2,)), DMA((deep,)), DMA((deep,)), DMA((deep,)), DMA((deep,)),
    ]
    params = pltpu.CompilerParams(collective_id=cid, has_side_effects=True, vmem_limit_bytes=VMEM_LIMIT)
    body = functools.partial(layer_kernel, layer, last, n_dev)
    if last:
        return pl.pallas_call(
            body,
            in_specs=[ANY, ANY, WHOLE] + [ANY] * 4,
            out_specs=ANY,
            out_shape=jax.ShapeDtypeStruct(x.shape, BF16),
            scratch_shapes=work + [pltpu.VMEM((3, rows, dim), BF16), DMA((3,)), DMA((3,)), DMA((3,)), DMA((slots,))],
            compiler_params=params,
        )(o2, x2, ln_w, w_o, w_gate, w_up, w_down)
    qk_w, cos, sin, w_q, w_k, w_v = more
    hd = qk_w.shape[-1]
    nq, nk = w_q.shape[-1] // hd, w_k.shape[-1] // hd
    q_shape, kv_shape = (slots, nq, rows, hd), (blocks, rows, nk * hd)
    return pl.pallas_call(
        body,
        in_specs=[ANY, ANY, WHOLE, WHOLE, WHOLE, WHOLE] + [ANY] * 7,
        out_specs=[ANY] * 4,
        out_shape=[jax.ShapeDtypeStruct(a, BF16) for a in (x.shape, q_shape, kv_shape, kv_shape)],
        scratch_shapes=work + [
            pltpu.VMEM((deep, dim, hd), BF16), DMA((deep,)),
            pltpu.VMEM((2, 3, nq, rows, hd), BF16), pltpu.VMEM((2, 3, rows, nk * hd), BF16), pltpu.VMEM((2, 3, rows, nk * hd), BF16),
            DMA((slots,)), DMA((slots,)), DMA((2, 3, slots)), DMA((2, blocks)), DMA((2, 2)),
        ],
        compiler_params=params,
    )(o2, x2, ln_w, qk_w, cos, sin, w_o, w_gate, w_up, w_down, w_k, w_v, w_q)


def rope_tables(pos, hd):
    half = hd // 2
    out = []
    for base, scale in ((LOCAL_BASE, 1.0), (GLOBAL_BASE, GLOBAL_SCALE)):
        freq = base ** (-2.0 * jnp.arange(half, dtype=jnp.float32) / hd)
        ang = (pos.astype(jnp.float32) / scale)[:, None] * freq[None, :]
        out += [jnp.cos(ang), jnp.sin(ang)]
    return out


def solution(mesh):
    n_dev = mesh.shape["cp"]

    def device_fn(x_loc, ln_w, qk_w, w_q, w_k, w_v, w_o, w_gate, w_up, w_down):
        slots, rows, dim = x_loc.shape
        _, _, core, special, row = placement()
        blk = jnp.stack([slot_place(s, core, special, row)[1] for s in range(slots)])
        pos = (blk[:, None] * rows + jnp.arange(rows)[None, :]).reshape(-1)
        cos0, sin0, cos1, sin1 = rope_tables(pos, qk_w.shape[-1])
        x, q, k, v = first(n_dev, x_loc, ln_w, qk_w, cos0, sin0, w_q, w_k, w_v)
        o = attention(WINDOW, q, k, v)
        mlp = (w_o, w_gate, w_up, w_down)
        x, q, k, v = after_attention(0, False, n_dev, 1, o, x, ln_w, *mlp, more=(qk_w, cos1, sin1, w_q, w_k, w_v))
        o = attention(None, q, k, v)
        return after_attention(1, True, n_dev, 2, o, x, ln_w, *mlp)

    act_part = P("dp", "cp", None)
    return jax.shard_map(device_fn, mesh=mesh, in_specs=(act_part,) + (P(),) * 9, out_specs=act_part, check_vma=False)
```

```python
import functools

import jax
import jax.numpy as jnp
from jax import lax
from jax.experimental import pallas as pl
from jax.experimental.pallas import tpu as pltpu
from jax.sharding import PartitionSpec as P

WINDOW = 1024
NORM_EPS = 1e-6
LOCAL_BASE = 10000.0
GLOBAL_BASE = 1000000.0
GLOBAL_SCALE = 8.0
NEG = -1e30

ROW_CHIP = (0, 3, 4, 1, 5, 6)
SPECIAL = (2, 7)
VMEM_LIMIT = 64 * 1024 * 1024 - 128 * 1024
MESH = pl.DeviceIdType.MESH
BF16, F32 = jnp.bfloat16, jnp.float32
ANY = pl.BlockSpec(memory_space=pl.ANY)
WHOLE = pl.BlockSpec(memory_space=pltpu.VMEM)
DMA = pltpu.SemaphoreType.DMA


def pick(idx, table):
    out = jnp.int32(table[-1])
    for i in range(len(table) - 2, -1, -1):
        out = jnp.where(idx == i, jnp.int32(table[i]), out)
    return out


def placement():
    me = lax.axis_index("cp")
    chip, core = me // 2, me % 2
    roles = [0] * 8
    rows = [0] * 8
    for b, c in enumerate(ROW_CHIP):
        rows[c] = b
    for i, c in enumerate(SPECIAL):
        roles[c] = 1
        rows[c] = 3 * i
    return me, chip, core, pick(chip, roles), pick(chip, rows)


def slot_place(s, core, special, row):
    k = s % 2
    blk = jnp.where(special == 1, 2 * k + (k + core) % 2, 4 + 2 * s + (s + core) % 2)
    b = jnp.where(special == 1, row + s // 2, row)
    return b, blk


def ring(a, b):
    return min((a - b) % 8, (b - a) % 8)


ARRIVAL = [sorted(range(6), key=lambda s: (ring(2 + s, c), s)) for c in range(8)]
for c in SPECIAL:
    ARRIVAL[c] = [4, 5, 0, 2, 1, 3]


def home_of(b, blk):
    core = ((blk + 1) // 2) % 2
    half = blk // 2
    chip = jnp.where(blk < 4, pick(b // 3, SPECIAL), pick(b, ROW_CHIP))
    slot = jnp.where(blk < 4, (b % 3) * 2 + half, half - 2)
    return chip * 2 + core, slot


def chunk_slot(ch, i, special, row):
    b = jnp.where(special == 1, row + i, row)
    return 2 * i + (b % 2 if ch == 0 else 1 - b % 2)


def kv_index(s, core, special, row):
    _, blk = slot_place(s, core, special, row)
    return jnp.where(special == 1, (s // 2) * 4 + blk, blk)


def served(row, r):
    return jnp.where(row == 0, ROW_CHIP[r], ROW_CHIP[r + 3])


def signal_group(n_dev):
    me = lax.axis_index("cp")
    barrier = pltpu.get_barrier_semaphore()
    for d in range(1, n_dev):
        pl.semaphore_signal(barrier, inc=1, device_id={"cp": lax.rem(me + d, n_dev)}, device_id_type=MESH)


def wait_group(n_dev):
    pl.semaphore_wait(pltpu.get_barrier_semaphore(), n_dev - 1)


def remote(src, dst, send, recv, dev):
    return pltpu.make_async_remote_copy(
        src_ref=src, dst_ref=dst, send_sem=send, recv_sem=recv, device_id={"cp": dev}, device_id_type=MESH
    )


def local(src, dst, sem):
    return pltpu.make_async_copy(src, dst, sem)


def norm_rows(vals, gain):
    inv = lax.rsqrt(jnp.mean(vals * vals, axis=-1, keepdims=True) + NORM_EPS)
    return vals * inv * (1.0 + gain)


def norm_turn(raw, gain, cos, sin):
    half = raw.shape[-1] // 2
    vals = norm_rows(raw.astype(BF16).astype(F32), gain)
    first, second = vals[:, :half], vals[:, half:]
    return jnp.concatenate([first * cos - second * sin, second * cos + first * sin], axis=-1).astype(BF16)


class KeyValues:
    def __init__(self, k_all, v_all, send, recv, fwd):
        self.both = ((0, k_all), (1, v_all))
        self.send, self.recv, self.fwd = send, recv, fwd

    def here(self):
        _, chip, self.core, self.special, self.row = placement()
        self.mate = chip * 2 + 1 - self.core

    def _copies(self, s, stage):
        idx = kv_index(s, self.core, self.special, self.row)
        _, blk = slot_place(s, self.core, self.special, self.row)
        dev = served(self.row, 0) * 2 + self.core
        for r in (1, 2):
            dev = jnp.where(s // 2 == r, served(self.row, r) * 2 + self.core, dev)
        out = []
        for x, full in self.both:
            out.append((
                local(stage[x], full.at[idx], self.send.at[x, 0, s]),
                remote(stage[x], full.at[idx], self.send.at[x, 1, s], self.recv.at[x, idx], self.mate),
                remote(stage[x], full.at[blk], self.send.at[x, 2, s], self.recv.at[x, blk], dev),
            ))
        return out

    def start(self, s, stage):
        self.here()
        for own, mate, row in self._copies(s, stage):

            @pl.when(self.special == 1)
            def _():
                row.start()

            mate.start()
            own.start()

    def wait_sent(self, s, stage):
        self.here()
        for own, mate, row in self._copies(s, stage):
            own.wait()
            mate.wait_send()

            @pl.when(self.special == 1)
            def _():
                row.wait_send()

    def wait_all(self, slots):
        self.here()
        for x, full in self.both:

            @pl.when(self.special == 0)
            def _():
                for k in range(2):
                    blk = 2 * k + (k + self.core) % 2
                    remote(full.at[blk], full.at[blk], self.fwd.at[x, k], self.recv.at[x, blk], self.mate).wait_recv()
                    remote(full.at[blk], full.at[blk], self.fwd.at[x, k], self.recv.at[x, blk], self.mate).start()

            for s in range(slots):
                idx = kv_index(s, 1 - self.core, self.special, self.row)
                remote(full.at[idx], full.at[idx], self.fwd.at[x, 0], self.recv.at[x, idx], self.mate).wait_recv()

        @pl.when(self.special == 0)
        def _():
            for x, full in self.both:
                for k in range(2):
                    blk = 2 * k + (k + 1 - self.core) % 2
                    remote(full.at[blk], full.at[blk], self.fwd.at[x, k], self.recv.at[x, blk], self.mate).wait()


def first_kernel(n_dev, nq, nk, x_ref, ln_ref, qk_ref, cos_ref, sin_ref, wq_ref, wk_ref, wv_ref,
                 h_ref, q_ref, k_all, v_all, xbuf, abuf, wq, wk, wv, qst, kst, vst,
                 wsem, xsend, xrecv, hsem, qsem, ksend, krecv, fsem):
    me, chip, core, special, row = placement()
    n, rows, dim = x_ref.shape
    hd = qk_ref.shape[-1]
    homes = [home_of(jnp.int32(b), me) for b in range(n)]
    keys = KeyValues(k_all, v_all, ksend, krecv, fsem)

    signal_group(n_dev)
    for b, (dev, slot) in enumerate(homes):

        @pl.when(dev == me)
        def _():
            local(x_ref.at[b], xbuf.at[slot], xrecv.at[slot]).start()

    weights = ((wk_ref, wk), (wv_ref, wv), (wq_ref, wq))
    for j, (src, dst) in enumerate(weights):
        start_parts(src.at[0], dst, wsem.at[j])
    wait_group(n_dev)
    for b in SEND_ORDER:
        dev, slot = homes[b]

        @pl.when(dev != me)
        def _():
            remote(x_ref.at[b], xbuf.at[slot], xsend.at[b], xrecv.at[slot], dev).start()

    gain = ln_ref[0, 0:1, :].astype(F32)

    def take(pair):
        places = [pick(chip, [ARRIVAL[c][2 * pair + j] for c in range(8)]) for j in range(2)]
        for j, s in enumerate(places):
            local(xbuf.at[s], xbuf.at[s], xrecv.at[s]).wait()
            local(xbuf.at[s], h_ref.at[s], hsem.at[s]).start()
            abuf[j * rows : (j + 1) * rows, :] = norm_rows(xbuf[s].astype(F32), gain).astype(BF16)
        return places

    def tables(s):
        r = pl.ds(pl.multiple_of(s * rows, rows), rows)
        return cos_ref[r, :], sin_ref[r, :]

    def product(w, h):
        return jnp.dot(abuf[...], w[:, pl.ds(pl.multiple_of(h * hd, hd), hd)], preferred_element_type=F32)

    for pair in range(n // 2):
        places = take(pair)
        if pair == 0:
            local(wk_ref.at[0], wk, wsem.at[0]).wait()
            local(wv_ref.at[0], wv, wsem.at[1]).wait()
        turn = [tables(s) for s in places]
        k_gain = qk_ref[0, 1:2, :].astype(F32)
        q_gain = qk_ref[0, 0:1, :].astype(F32)

        @pl.loop(0, nk)
        def _(h):
            col = pl.ds(pl.multiple_of(h * hd, hd), hd)
            k_raw, v_raw = product(wk, h), product(wv, h)
            for j, s in enumerate(places):
                part = slice(j * rows, (j + 1) * rows)
                kst[s, :, col] = norm_turn(k_raw[part], k_gain, *turn[j])
                vst[s, :, col] = v_raw[part].astype(BF16)

        if pair == 0:
            local(wq_ref.at[0], wq, wsem.at[2]).wait()

        def query(h):
            raw = product(wq, h)
            for j, s in enumerate(places):
                part = slice(j * rows, (j + 1) * rows)
                qst[s, h] = norm_turn(raw[part], q_gain, *turn[j]) * BF16(hd**-0.5)

        query(0)
        for s in places:
            keys.start(s, (kst.at[s], vst.at[s]))
        pl.loop(1, nq)(query)
        for s in places:
            local(qst.at[s], q_ref.at[s], qsem.at[s]).start()

    for s in range(n):
        keys.wait_sent(s, (kst.at[s], vst.at[s]))
        local(qst.at[s], q_ref.at[s], qsem.at[s]).wait()
        local(xbuf.at[s], h_ref.at[s], hsem.at[s]).wait()
    for b, (dev, slot) in enumerate(homes):

        @pl.when(dev != me)
        def _():
            remote(x_ref.at[b], xbuf.at[slot], xsend.at[b], xrecv.at[slot], dev).wait_send()

    keys.wait_all(n)


SEND_ORDER = (2, 5, 0, 3, 1, 4)


def first(n_dev, x, ln_w, qk_w, cos, sin, w_q, w_k, w_v):
    n, rows, dim = x.shape
    hd = qk_w.shape[-1]
    nq, nk = w_q.shape[-1] // hd, w_k.shape[-1] // hd
    blocks = 16
    q_shape, s_shape, kv_shape = (n, nq, rows, hd), (n, rows, nk * hd), (blocks, rows, nk * hd)
    return pl.pallas_call(
        functools.partial(first_kernel, n_dev, nq, nk),
        out_shape=[jax.ShapeDtypeStruct(a, BF16) for a in (x.shape, q_shape, kv_shape, kv_shape)],
        in_specs=[ANY, WHOLE, WHOLE, WHOLE, WHOLE, ANY, ANY, ANY],
        out_specs=[ANY] * 4,
        scratch_shapes=[
            pltpu.VMEM(x.shape, BF16), pltpu.VMEM((2 * rows, dim), BF16),
            pltpu.VMEM(w_q.shape[1:], BF16), pltpu.VMEM(w_k.shape[1:], BF16), pltpu.VMEM(w_v.shape[1:], BF16),
            pltpu.VMEM(q_shape, BF16), pltpu.VMEM(s_shape, BF16), pltpu.VMEM(s_shape, BF16),
            DMA((3,)), DMA((n,)), DMA((n,)), DMA((n,)), DMA((n,)), DMA((2, 3, n)), DMA((2, blocks)), DMA((2, 2)),
        ],
        compiler_params=pltpu.CompilerParams(collective_id=0, has_side_effects=True, vmem_limit_bytes=VMEM_LIMIT),
    )(x, ln_w, qk_w, cos, sin, w_q, w_k, w_v)


def attn_kernel(window_blocks, q_ref, k_ref, v_ref, o_ref, kbuf, vbuf, qbuf, obuf, sbuf, wacc, wm, wl, bias, qsem, ksem, osem):
    _, _, core, special, row = placement()
    slots, nq, rows, hd = q_ref.shape
    nk = k_ref.shape[-1] // hd
    rep = nq // nk
    per = 4
    tile = per * rows
    tiles = k_ref.shape[0] // per

    def loads(t):
        part = pl.ds(t * per, per)
        return [local(k_ref.at[part], kbuf.at[part], ksem.at[0, t]), local(v_ref.at[part], vbuf.at[part], ksem.at[1, t])]

    for s in range(slots):
        local(q_ref.at[s], qbuf.at[s], qsem.at[s]).start()
    for t in range(tiles):
        for c in loads(t):
            c.start()

    qi = lax.broadcasted_iota(jnp.int32, (rows, tile), 0)
    ki = lax.broadcasted_iota(jnp.int32, (rows, tile), 1)
    bias[0] = jnp.zeros((rows, tile), jnp.float32)
    for j in range(per):
        bias[1 + j] = jnp.where(ki <= qi + j * rows, 0.0, NEG)
        if window_blocks is not None:
            bias[1 + per + j] = jnp.where(ki > qi + j * rows, 0.0, NEG)

    def start_tile(blk):
        if window_blocks is None:
            return jnp.int32(0)
        return jnp.maximum(blk - window_blocks, 0) // per

    def scores(s, t, base, blk):
        edge = jnp.where(t == blk // per, 1 + blk % per, 0)
        if window_blocks is not None:
            old = blk - window_blocks
            edge = jnp.where((old >= 0) & (t == old // per), 1 + per + old % per, edge)
        off = bias[edge][None]
        kt = kbuf.at[pl.ds(base + per * t, per)]
        out = []
        for g in range(nk):
            q2 = qbuf[s, g * rep : (g + 1) * rep].reshape(rep * rows, hd)
            kk = kt[:, :, g * hd : (g + 1) * hd].reshape(tile, hd)
            sc = lax.dot_general(q2, kk, (((1,), (1,)), ((), ())), preferred_element_type=jnp.float32)
            out.append((sc.reshape(rep, rows, tile) + off).reshape(rep * rows, tile))
        return out

    lanes = 128

    def columns(val, op):
        parts = [val[:, j * lanes : (j + 1) * lanes] for j in range(tile // lanes)]
        return functools.reduce(op, parts)

    def spread(val):
        return jnp.concatenate([val] * (tile // lanes), axis=1)

    def row_max(val):
        return jnp.broadcast_to(jnp.max(val, axis=-1, keepdims=True), val.shape)

    def values(t, base, g):
        return vbuf.at[pl.ds(base + per * t, per)][:, :, g * hd : (g + 1) * hd].reshape(tile, hd)

    def finish(s, total, weight):
        for g in range(nk):
            out = (total[g] / jnp.sum(weight[g], axis=-1, keepdims=True)).astype(jnp.bfloat16)
            for h in range(rep):
                lo = (g * rep + h) * hd
                obuf[s, :, lo : lo + hd] = out[h * rows : (h + 1) * rows]
        local(obuf.at[s], o_ref.at[s], osem.at[s]).start()

    for t in range(tiles):
        for c in loads(t):
            c.wait()

    @pl.loop(0, slots)
    def _(s):
        _, blk = slot_place(s, core, special, row)
        base = jnp.where(special == 1, (s // 2) * per, 0)
        first = start_tile(blk)
        last = blk // per + 1
        local(q_ref.at[s], qbuf.at[s], qsem.at[s]).wait()
        for g in range(nk):
            wm[g] = jnp.full(wm.shape[1:], NEG, F32)
            wl[g] = jnp.zeros(wl.shape[1:], F32)
            wacc[g] = jnp.zeros(wacc.shape[1:], F32)

        @pl.loop(first, last)
        def _(t):
            for g, sc in enumerate(scores(s, t, base, blk)):
                sbuf[g, t] = sc
                wm[g] = jnp.maximum(wm[g], columns(sc, jnp.maximum))

        for g in range(nk):
            wm[g] = row_max(wm[g])

        @pl.loop(first, last)
        def _(t):
            for g in range(nk):
                p = jnp.exp(sbuf[g, t] - spread(wm[g]))
                wl[g] += columns(p, jnp.add)
                wacc[g] += jnp.dot(p.astype(BF16), values(t, base, g), preferred_element_type=F32)

        finish(s, [wacc[g] for g in range(nk)], [wl[g] for g in range(nk)])

    for s in range(slots):
        local(obuf.at[s], o_ref.at[s], osem.at[s]).wait()


def attention(window, q, k, v):
    slots, nq, rows, hd = q.shape
    blocks = k.shape[0]
    nk = k.shape[-1] // hd
    wide = nq // nk * rows
    return pl.pallas_call(
        functools.partial(attn_kernel, None if window is None else window // rows),
        out_shape=jax.ShapeDtypeStruct((slots, rows, nq * hd), BF16),
        in_specs=[ANY] * 3,
        out_specs=ANY,
        scratch_shapes=[
            pltpu.VMEM(k.shape, BF16), pltpu.VMEM(v.shape, BF16), pltpu.VMEM(q.shape, BF16),
            pltpu.VMEM((slots, rows, nq * hd), BF16),
            pltpu.VMEM((nk, blocks // 4, wide, 4 * rows), F32),
            pltpu.VMEM((nk, wide, hd), F32), pltpu.VMEM((nk, wide, 128), F32), pltpu.VMEM((nk, wide, 128), F32),
            pltpu.VMEM((9, rows, 4 * rows), F32),
            DMA((slots,)), DMA((2, blocks // 4)), DMA((slots,)),
        ],
        compiler_params=pltpu.CompilerParams(vmem_limit_bytes=VMEM_LIMIT),
    )(q, k, v)


def start_parts(src, dst, sem, parts=4):
    n = src.shape[0]
    if n % (parts * 16):
        local(src, dst, sem).start()
        return
    for j in range(parts):
        part = pl.ds(j * (n // parts), n // parts)
        local(src.at[part], dst.at[part], sem).start()


class Ring:
    def __init__(self, buf, sem, count, source):
        self.buf, self.sem, self.count, self.source = buf, sem, count, source
        self.depth = buf.shape[0]

    def begin(self):
        for t in range(min(self.depth, self.count)):
            self.start(t, t)

    def start(self, t, slot):
        def put(ref):
            start_parts(ref, self.buf.at[slot], self.sem.at[slot])

        self.source(t, put)

    def get(self, t):
        slot = lax.rem(t, self.depth) if not isinstance(t, int) else t % self.depth
        local(self.buf.at[slot], self.buf.at[slot], self.sem.at[slot]).wait()
        return self.buf.at[slot]

    def free(self, t):
        new = t + self.depth
        if isinstance(t, int):
            if new < self.count:
                self.start(new, t % self.depth)
            return

        @pl.when(new < self.count)
        def _():
            self.start(new, lax.rem(t, self.depth))


def layer_kernel(layer, last, n_dev, *refs):
    if last:
        (o_ref, x_ref, ln_ref, wo_ref, wg_ref, wu_ref, wd_ref, out_ref,
         obuf, y_ref, att, c_ref, acc, act, wo, wg, wu, wd, isem, osem, gsem, usem, dsem,
         ybuf, ysend, yrecv, osend, orecv) = refs
    else:
        (o_ref, x_ref, ln_ref, qk_ref, cos_ref, sin_ref, wo_ref, wg_ref, wu_ref, wd_ref, wk_ref, wv_ref, wq_ref,
         h_ref, q_ref, k_all, v_all,
         obuf, y_ref, att, c_ref, acc, act, wo, wg, wu, wd, isem, osem, gsem, usem, dsem,
         wn, nsem, qst, kst, vst, hsem, qsem, ksend, krecv, fsem) = refs
        keys = KeyValues(k_all, v_all, ksend, krecv, fsem)
        hd = qk_ref.shape[-1]
        nk, nq = wk_ref.shape[-1] // hd, wq_ref.shape[-1] // hd
    rows = acc.shape[0] // 3
    tn, tf = wo.shape[-1], wg.shape[-1]
    n_o, n_f = wo_ref.shape[-1] // tn, wg_ref.shape[-1] // tf

    def cols(t, width):
        start = t * width
        return pl.ds(start if isinstance(t, int) else pl.multiple_of(start, width), width)

    def tile_f(t):
        return (t % n_f) if isinstance(t, int) else lax.rem(t, n_f)

    o_ring = Ring(wo, osem, n_o, lambda t, put: put(wo_ref.at[layer, :, cols(t, tn)]))
    g_ring = Ring(wg, gsem, 2 * n_f, lambda t, put: put(wg_ref.at[layer, :, cols(tile_f(t), tf)]))
    u_ring = Ring(wu, usem, 2 * n_f, lambda t, put: put(wu_ref.at[layer, :, cols(tile_f(t), tf)]))
    d_ring = Ring(wd, dsem, 2 * n_f, lambda t, put: put(wd_ref.at[layer, cols(tile_f(t), tf), :]))

    in_o = local(o_ref, obuf, isem.at[0])
    in_x = local(x_ref, y_ref, isem.at[1])
    start_parts(o_ref, obuf, isem.at[0], 6)
    o_ring.begin()
    start_parts(x_ref, y_ref, isem.at[1], 6)
    for r in (g_ring, u_ring, d_ring):
        r.begin()
    signal_group(n_dev)

    def slot_of(ch, m):
        _, _, _, special, row = placement()
        return chunk_slot(ch, m, special, row)

    def place_of(ch, m):
        _, _, core, special, row = placement()
        return slot_place(chunk_slot(ch, m, special, row), core, special, row)

    def slot_rows(s):
        return pl.ds(pl.multiple_of(s * rows, rows), rows)

    def own_rows(m):
        return pl.ds(m * rows, rows)

    def y_at(ch, m):
        return y_ref.at[slot_rows(slot_of(ch, m))]

    def gain(which, l=layer):
        return ln_ref[l, which : which + 1, :].astype(F32)

    def c_of(y):
        return norm_rows(y.astype(F32), gain(2)).astype(BF16)

    in_o.wait()

    @pl.loop(0, n_o)
    def _(t):
        tile = o_ring.get(t)
        att[:, cols(t, tn)] = jnp.dot(obuf[...], tile[...], preferred_element_type=F32).astype(BF16)
        o_ring.free(t)

    in_x.wait()
    for ch in range(2):
        for m in range(3):
            r = slot_rows(slot_of(ch, m))
            y = y_ref[r, :].astype(F32) + norm_rows(att[r, :].astype(F32), gain(1))
            y = y.astype(BF16)
            y_ref[r, :] = y
            if ch == 0 or not last:
                c_ref[ch, own_rows(m), :] = c_of(y)

    def up(ch, g_tile, u_tile):
        gate = jnp.dot(c_ref[ch], g_tile[...], preferred_element_type=F32)
        val = jnp.dot(c_ref[ch], u_tile[...], preferred_element_type=F32)
        return (jax.nn.gelu(gate, approximate=True) * val).astype(BF16)

    def mlp(ch, after_first):
        base = ch * n_f
        act[0] = up(ch, g_ring.get(base), u_ring.get(base))
        acc[...] = jnp.zeros(acc.shape, F32)
        g_ring.free(base)
        u_ring.free(base)
        after_first()

        @pl.loop(1, n_f)
        def _(t):
            new = lax.rem(t, 2)
            g_tile, u_tile, d_tile = g_ring.get(base + t), u_ring.get(base + t), d_ring.get(base + t - 1)
            acc[...] += jnp.dot(act[1 - new], d_tile[...], preferred_element_type=F32)
            act[new] = up(ch, g_tile, u_tile)
            g_ring.free(base + t)
            u_ring.free(base + t)
            d_ring.free(base + t - 1)

        t = base + n_f - 1
        acc[...] += jnp.dot(act[(n_f - 1) % 2], d_ring.get(t)[...], preferred_element_type=F32)
        d_ring.free(t)

    def result(m, y):
        val = acc[own_rows(m), :].astype(BF16).astype(F32)
        return (y.astype(F32) + norm_rows(val, gain(3))).astype(BF16)

    if last:
        me = lax.axis_index("cp")

        def sent(ch, m):
            b, blk = place_of(ch, m)
            src = y_at(ch, m)
            if ch == 0:
                far = lambda: remote(src, out_ref.at[b], osend.at[m], orecv.at[b], blk)
                return blk, far, lambda: local(src, out_ref.at[b], orecv.at[b])
            return blk, lambda: remote(src, ybuf.at[b // 2], ysend.at[m], yrecv.at[b // 2], blk), None

        def owned(ch, m):
            turn = (me // 2) % 2
            b = 2 * m + (turn if ch == 0 else 1 - turn)
            return b, home_of(b, me)[0]

        def send_streams():
            wait_group(n_dev)
            for m in range(3):
                dev, far, _ = sent(1, m)

                @pl.when(dev != me)
                def _():
                    far().start()

        def send_results():
            for m in range(3):
                dev, far, near = sent(0, m)

                @pl.when(dev != me)
                def _():
                    far().start()

                @pl.when(dev == me)
                def _():
                    near().start()

        mlp(0, send_streams)
        for m in range(3):
            y_at(0, m)[...] = result(m, y_at(0, m)[...])
        for m in range(3):
            b, dev = owned(1, m)

            @pl.when(dev != me)
            def _():
                remote(ybuf.at[m], ybuf.at[m], ysend.at[m], yrecv.at[m], me).wait_recv()

        for m in range(3):
            b, blk = place_of(1, m)

            @pl.when(blk == me)
            def _():
                ybuf[b // 2] = y_at(1, m)[...]

        for m in range(3):
            c_ref[1, own_rows(m), :] = c_of(ybuf[m])
        mlp(1, send_results)
        for m in range(3):
            ybuf[m] = result(m, ybuf[m])
        for m in range(3):
            b, _ = owned(1, m)
            local(ybuf.at[m], out_ref.at[b], orecv.at[b]).start()
        for ch in range(2):
            for m in range(3):
                dev, far, _ = sent(ch, m)

                @pl.when(dev != me)
                def _():
                    far().wait_send()

        for b in range(6):
            local(out_ref.at[b], out_ref.at[b], orecv.at[b]).wait()
        return

    def source(t, put):
        kind = lax.rem(t, 2 * nk) if not isinstance(t, int) else t % (2 * nk)
        cases = (
            (jnp.logical_and(t < 4 * nk, kind < nk), lambda: put(wk_ref.at[layer + 1, :, cols(kind, hd)])),
            (jnp.logical_and(t < 4 * nk, kind >= nk), lambda: put(wv_ref.at[layer + 1, :, cols(kind - nk, hd)])),
            (t >= 4 * nk, lambda: put(wq_ref.at[layer + 1, :, cols(t - 4 * nk, hd)])),
        )
        for cond, do in cases:
            pl.when(cond)(do)

    n_ring = Ring(wn, nsem, 4 * nk + nq, source)
    n_ring.begin()
    k_gain, q_gain = (qk_ref[layer + 1, j : j + 1, :].astype(F32) for j in (1, 0))

    def turn(ch, m):
        r = slot_rows(slot_of(ch, m))
        return cos_ref[r, :], sin_ref[r, :]

    def send_keys(ch):
        for m in range(3):
            keys.start(slot_of(ch, m), (kst.at[ch, m], vst.at[ch, m]))

    def keys_and_values(ch):
        for m in range(3):
            h = result(m, y_at(ch, m)[...])
            y_at(ch, m)[...] = h
            c_ref[ch, own_rows(m), :] = norm_rows(h.astype(F32), gain(0, layer + 1)).astype(BF16)

        @pl.loop(0, nk)
        def _(h):
            t = ch * 2 * nk + h
            raw = jnp.dot(c_ref[ch], n_ring.get(t)[...], preferred_element_type=F32)
            n_ring.free(t)
            for m in range(3):
                kst[ch, m, :, cols(h, hd)] = norm_turn(raw[m * rows : (m + 1) * rows], k_gain, *turn(ch, m))

        @pl.loop(0, nk)
        def _(h):
            t = (ch * 2 + 1) * nk + h
            raw = jnp.dot(c_ref[ch], n_ring.get(t)[...], preferred_element_type=F32)
            n_ring.free(t)
            for m in range(3):
                vst[ch, m, :, cols(h, hd)] = raw[m * rows : (m + 1) * rows].astype(BF16)

        for m in range(3):
            s = slot_of(ch, m)
            local(y_at(ch, m), h_ref.at[s], hsem.at[s]).start()

    def query(h):
        t = 4 * nk + h
        tile = n_ring.get(t)
        for ch in range(2):
            raw = jnp.dot(c_ref[ch], tile[...], preferred_element_type=F32)
            for m in range(3):
                out = norm_turn(raw[m * rows : (m + 1) * rows], q_gain, *turn(ch, m))
                qst[ch, m, h] = out * BF16(hd**-0.5)
        n_ring.free(t)

    def first_keys():
        wait_group(n_dev)
        send_keys(0)

    mlp(0, lambda: None)
    keys_and_values(0)
    mlp(1, first_keys)
    keys_and_values(1)
    query(0)
    send_keys(1)
    pl.loop(1, nq)(query)
    for ch in range(2):
        for m in range(3):
            s = slot_of(ch, m)
            local(qst.at[ch, m], q_ref.at[s], qsem.at[s]).start()
    for ch in range(2):
        for m in range(3):
            s = slot_of(ch, m)
            keys.wait_sent(s, (kst.at[ch, m], vst.at[ch, m]))
            local(qst.at[ch, m], q_ref.at[s], qsem.at[s]).wait()
            local(y_at(ch, m), h_ref.at[s], hsem.at[s]).wait()
    keys.wait_all(6)


def after_attention(layer, last, n_dev, cid, o, x, ln_w, w_o, w_gate, w_up, w_down, more=()):
    slots, rows, dim = x.shape
    inner, ff = w_o.shape[1], w_gate.shape[-1]
    total = slots * rows
    half = total // 2
    blocks = 16
    tn, tf = min(256, dim), min(512, ff)
    deep = 3
    o2, x2 = o.reshape(total, inner), x.reshape(total, dim)
    work = [
        pltpu.VMEM((total, inner), BF16), pltpu.VMEM((total, dim), BF16),
        pltpu.VMEM((total, dim), BF16), pltpu.VMEM((2, half, dim), BF16),
        pltpu.VMEM((half, dim), F32), pltpu.VMEM((2, half, tf), BF16),
        pltpu.VMEM((deep, inner, tn), BF16), pltpu.VMEM((deep, dim, tf), BF16), pltpu.VMEM((deep, dim, tf), BF16),
        pltpu.VMEM((deep, tf, dim), BF16),
        DMA((2,)), DMA((deep,)), DMA((deep,)), DMA((deep,)), DMA((deep,)),
    ]
    params = pltpu.CompilerParams(collective_id=cid, has_side_effects=True, vmem_limit_bytes=VMEM_LIMIT)
    body = functools.partial(layer_kernel, layer, last, n_dev)
    if last:
        return pl.pallas_call(
            body,
            in_specs=[ANY, ANY, WHOLE] + [ANY] * 4,
            out_specs=ANY,
            out_shape=jax.ShapeDtypeStruct(x.shape, BF16),
            scratch_shapes=work + [pltpu.VMEM((3, rows, dim), BF16), DMA((3,)), DMA((3,)), DMA((3,)), DMA((slots,))],
            compiler_params=params,
        )(o2, x2, ln_w, w_o, w_gate, w_up, w_down)
    qk_w, cos, sin, w_q, w_k, w_v = more
    hd = qk_w.shape[-1]
    nq, nk = w_q.shape[-1] // hd, w_k.shape[-1] // hd
    q_shape, kv_shape = (slots, nq, rows, hd), (blocks, rows, nk * hd)
    return pl.pallas_call(
        body,
        in_specs=[ANY, ANY, WHOLE, WHOLE, WHOLE, WHOLE] + [ANY] * 7,
        out_specs=[ANY] * 4,
        out_shape=[jax.ShapeDtypeStruct(a, BF16) for a in (x.shape, q_shape, kv_shape, kv_shape)],
        scratch_shapes=work + [
            pltpu.VMEM((deep, dim, hd), BF16), DMA((deep,)),
            pltpu.VMEM((2, 3, nq, rows, hd), BF16), pltpu.VMEM((2, 3, rows, nk * hd), BF16), pltpu.VMEM((2, 3, rows, nk * hd), BF16),
            DMA((slots,)), DMA((slots,)), DMA((2, 3, slots)), DMA((2, blocks)), DMA((2, 2)),
        ],
        compiler_params=params,
    )(o2, x2, ln_w, qk_w, cos, sin, w_o, w_gate, w_up, w_down, w_k, w_v, w_q)


def rope_tables(pos, hd):
    half = hd // 2
    out = []
    for base, scale in ((LOCAL_BASE, 1.0), (GLOBAL_BASE, GLOBAL_SCALE)):
        freq = base ** (-2.0 * jnp.arange(half, dtype=jnp.float32) / hd)
        ang = (pos.astype(jnp.float32) / scale)[:, None] * freq[None, :]
        out += [jnp.cos(ang), jnp.sin(ang)]
    return out


def solution(mesh):
    n_dev = mesh.shape["cp"]

    def device_fn(x_loc, ln_w, qk_w, w_q, w_k, w_v, w_o, w_gate, w_up, w_down):
        slots, rows, dim = x_loc.shape
        _, _, core, special, row = placement()
        blk = jnp.stack([slot_place(s, core, special, row)[1] for s in range(slots)])
        pos = (blk[:, None] * rows + jnp.arange(rows)[None, :]).reshape(-1)
        cos0, sin0, cos1, sin1 = rope_tables(pos, qk_w.shape[-1])
        x, q, k, v = first(n_dev, x_loc, ln_w, qk_w, cos0, sin0, w_q, w_k, w_v)
        o = attention(WINDOW, q, k, v)
        mlp = (w_o, w_gate, w_up, w_down)
        x, q, k, v = after_attention(0, False, n_dev, 1, o, x, ln_w, *mlp, more=(qk_w, cos1, sin1, w_q, w_k, w_v))
        o = attention(None, q, k, v)
        return after_attention(1, True, n_dev, 2, o, x, ln_w, *mlp)

    act_part = P("dp", "cp", None)
    return jax.shard_map(device_fn, mesh=mesh, in_specs=(act_part,) + (P(),) * 9, out_specs=act_part, check_vma=False)
```

```python
import functools

import jax
import jax.numpy as jnp
from jax import lax
from jax.experimental import pallas as pl
from jax.experimental.pallas import tpu as pltpu
from jax.sharding import PartitionSpec as P

WINDOW = 1024
NORM_EPS = 1e-6
LOCAL_BASE = 10000.0
GLOBAL_BASE = 1000000.0
GLOBAL_SCALE = 8.0
NEG = -1e30

ROW_CHIP = (0, 3, 4, 1, 5, 6)
SPECIAL = (2, 7)
VMEM_LIMIT = 64 * 1024 * 1024 - 128 * 1024
MESH = pl.DeviceIdType.MESH
BF16, F32 = jnp.bfloat16, jnp.float32
ANY = pl.BlockSpec(memory_space=pl.ANY)
WHOLE = pl.BlockSpec(memory_space=pltpu.VMEM)
DMA = pltpu.SemaphoreType.DMA


def pick(idx, table):
    out = jnp.int32(table[-1])
    for i in range(len(table) - 2, -1, -1):
        out = jnp.where(idx == i, jnp.int32(table[i]), out)
    return out


def placement():
    me = lax.axis_index("cp")
    chip, core = me // 2, me % 2
    roles = [0] * 8
    rows = [0] * 8
    for b, c in enumerate(ROW_CHIP):
        rows[c] = b
    for i, c in enumerate(SPECIAL):
        roles[c] = 1
        rows[c] = 3 * i
    return me, chip, core, pick(chip, roles), pick(chip, rows)


def slot_place(s, core, special, row):
    k = s % 2
    blk = jnp.where(special == 1, 2 * k + (k + core) % 2, 4 + 2 * s + (s + core) % 2)
    b = jnp.where(special == 1, row + s // 2, row)
    return b, blk


def ring(a, b):
    return min((a - b) % 8, (b - a) % 8)


ARRIVAL = [sorted(range(6), key=lambda s: (ring(2 + s, c), s)) for c in range(8)]
for c in SPECIAL:
    ARRIVAL[c] = [4, 5, 0, 2, 1, 3]


def home_of(b, blk):
    core = ((blk + 1) // 2) % 2
    half = blk // 2
    chip = jnp.where(blk < 4, pick(b // 3, SPECIAL), pick(b, ROW_CHIP))
    slot = jnp.where(blk < 4, (b % 3) * 2 + half, half - 2)
    return chip * 2 + core, slot


def chunk_slot(ch, i, special, row):
    b = jnp.where(special == 1, row + i, row)
    return 2 * i + (b + ch) % 2


def kv_index(s, core, special, row):
    _, blk = slot_place(s, core, special, row)
    return jnp.where(special == 1, (s // 2) * 4 + blk, blk)


def served(row, r):
    return jnp.where(row == 0, ROW_CHIP[r], ROW_CHIP[r + 3])


def signal_group(n_dev):
    me = lax.axis_index("cp")
    barrier = pltpu.get_barrier_semaphore()
    for d in range(1, n_dev):
        pl.semaphore_signal(barrier, inc=1, device_id={"cp": lax.rem(me + d, n_dev)}, device_id_type=MESH)


def wait_group(n_dev):
    pl.semaphore_wait(pltpu.get_barrier_semaphore(), n_dev - 1)


def remote(src, dst, send, recv, dev):
    return pltpu.make_async_remote_copy(
        src_ref=src, dst_ref=dst, send_sem=send, recv_sem=recv, device_id={"cp": dev}, device_id_type=MESH
    )


def local(src, dst, sem):
    return pltpu.make_async_copy(src, dst, sem)


def norm_rows(vals, gain):
    inv = lax.rsqrt(jnp.mean(vals * vals, axis=-1, keepdims=True) + NORM_EPS)
    return vals * inv * (1.0 + gain)


def norm_turn(raw, gain, cos, sin):
    half = raw.shape[-1] // 2
    vals = norm_rows(raw.astype(BF16).astype(F32), gain)
    first, second = vals[:, :half], vals[:, half:]
    return jnp.concatenate([first * cos - second * sin, second * cos + first * sin], axis=-1).astype(BF16)


class KeyValues:
    def __init__(self, k_all, v_all, send, recv, fwd, in_place=False):
        self.in_place = in_place
        self.both = ((0, k_all), (1, v_all))
        self.send, self.recv, self.fwd = send, recv, fwd

    def here(self):
        _, chip, self.core, self.special, self.row = placement()
        self.mate = chip * 2 + 1 - self.core

    def _copies(self, s, stage):
        idx = kv_index(s, self.core, self.special, self.row)
        _, blk = slot_place(s, self.core, self.special, self.row)
        dev = served(self.row, 0) * 2 + self.core
        for r in (1, 2):
            dev = jnp.where(s // 2 == r, served(self.row, r) * 2 + self.core, dev)
        out = []
        for x, full in self.both:
            src = full.at[idx] if self.in_place else stage[x]
            out.append((
                None if self.in_place else local(src, full.at[idx], self.send.at[x, 0, s]),
                remote(src, full.at[idx], self.send.at[x, 1, s], self.recv.at[x, idx], self.mate),
                remote(src, full.at[blk], self.send.at[x, 2, s], self.recv.at[x, blk], dev),
            ))
        return out

    def start(self, s, stage):
        self.here()
        for own, mate, row in self._copies(s, stage):

            @pl.when(self.special == 1)
            def _():
                row.start()

            mate.start()
            if own is not None:
                own.start()

    def wait_sent(self, s, stage):
        self.here()
        for own, mate, row in self._copies(s, stage):
            if own is not None:
                own.wait()
            mate.wait_send()

            @pl.when(self.special == 1)
            def _():
                row.wait_send()

    def wait_mate(self, slots):
        self.here()
        for x, full in self.both:
            for s in range(slots):
                idx = kv_index(s, 1 - self.core, self.special, self.row)
                remote(full.at[idx], full.at[idx], self.fwd.at[x, 0], self.recv.at[x, idx], self.mate).wait_recv()

    def wait_special(self):
        self.here()

        @pl.when(self.special == 0)
        def _():
            for k in range(2):
                blk = 2 * k + (k + self.core) % 2
                for x, full in self.both:
                    remote(full.at[blk], full.at[blk], self.fwd.at[x, k], self.recv.at[x, blk], self.mate).wait_recv()
                    remote(full.at[blk], full.at[blk], self.fwd.at[x, k], self.recv.at[x, blk], self.mate).start()
            for x, full in self.both:
                for k in range(2):
                    blk = 2 * k + (k + 1 - self.core) % 2
                    remote(full.at[blk], full.at[blk], self.fwd.at[x, k], self.recv.at[x, blk], self.mate).wait()


class Trig:
    def __init__(self, ref, layer, rows):
        self.ref, self.layer, self.rows = ref, layer, rows

    def of(self, blk):
        cu, su = (self.ref[self.layer, j, : self.rows, :] for j in range(2))
        cb, sb = (self.ref[self.layer, j, pl.ds(self.rows + blk, 1), :] for j in range(2))
        return cu * cb - su * sb, su * cb + cu * sb


class Attention:
    per, lanes = 4, 128

    def __init__(self, window_blocks, hd, qbuf, kbuf, vbuf, sbuf, wacc, wm, wl, bias, o_ref, osem):
        self.window_blocks, self.hd = window_blocks, hd
        self.qbuf, self.kbuf, self.vbuf, self.sbuf, self.bias = qbuf, kbuf, vbuf, sbuf, bias
        self.wacc, self.wm, self.wl, self.o_ref, self.osem = wacc, wm, wl, o_ref, osem
        self.slots, self.rows = qbuf.shape[:2]
        self.nk = kbuf.shape[-1] // hd
        self.rep = qbuf.shape[-1] // kbuf.shape[-1]
        self.tile = self.per * self.rows

    def fill_bias(self):
        rows, tile, bias = self.rows, self.tile, self.bias
        qi = lax.broadcasted_iota(jnp.int32, (rows, tile), 0)
        ki = lax.broadcasted_iota(jnp.int32, (rows, tile), 1)
        bias[0] = jnp.zeros((rows, tile), F32)
        for j in range(self.per):
            bias[1 + j] = jnp.where(ki <= qi + j * rows, 0.0, NEG)
            if self.window_blocks is not None:
                bias[1 + self.per + j] = jnp.where(ki > qi + j * rows, 0.0, NEG)

    def start_tile(self, blk):
        if self.window_blocks is None:
            return jnp.int32(0)
        return jnp.maximum(blk - self.window_blocks, 0) // self.per

    def part(self, buf, t, base, g):
        block = buf.at[pl.ds(base + self.per * t, self.per)]
        return block[:, :, g * self.hd : (g + 1) * self.hd].reshape(self.tile, self.hd)

    def scores(self, s, t, base, blk):
        rows, rep, hd, per = self.rows, self.rep, self.hd, self.per
        edge = jnp.where(t == blk // per, 1 + blk % per, 0)
        if self.window_blocks is not None:
            old = blk - self.window_blocks
            edge = jnp.where((old >= 0) & (t == old // per), 1 + per + old % per, edge)
        off = self.bias[edge][None]
        out = []
        for g in range(self.nk):
            heads = [self.qbuf[s, :, h * hd : (h + 1) * hd] for h in range(g * rep, (g + 1) * rep)]
            q2 = jnp.concatenate(heads, axis=0)
            sc = lax.dot_general(q2, self.part(self.kbuf, t, base, g), (((1,), (1,)), ((), ())), preferred_element_type=F32)
            out.append((sc.reshape(rep, rows, self.tile) + off).reshape(rep * rows, self.tile))
        return out

    def columns(self, val, op):
        return functools.reduce(op, [val[:, j * self.lanes : (j + 1) * self.lanes] for j in range(self.tile // self.lanes)])

    def spread(self, val):
        return jnp.concatenate([val] * (self.tile // self.lanes), axis=1)

    def row_max(self, val):
        return jnp.broadcast_to(jnp.max(val, axis=-1, keepdims=True), val.shape)

    def passes(self, s, blk, base, first, last):
        for g in range(self.nk):
            self.wm[g] = jnp.full(self.wm.shape[1:], NEG, F32)
            self.wl[g] = jnp.zeros(self.wl.shape[1:], F32)
            self.wacc[g] = jnp.zeros(self.wacc.shape[1:], F32)

        @pl.loop(first, last)
        def _(t):
            for g, sc in enumerate(self.scores(s, t, base, blk)):
                self.sbuf[g, t - first] = sc
                self.wm[g] = jnp.maximum(self.wm[g], self.columns(sc, jnp.maximum))

        for g in range(self.nk):
            self.wm[g] = self.row_max(self.wm[g])

        @pl.loop(first, last)
        def _(t):
            for g in range(self.nk):
                p = jnp.exp(self.sbuf[g, t - first] - self.spread(self.wm[g]))
                self.wl[g] += self.columns(p, jnp.add)
                self.wacc[g] += jnp.dot(p.astype(BF16), self.part(self.vbuf, t, base, g), preferred_element_type=F32)

    def merge(self, s, blk, old, old_sum, old_acc):
        for g, sc in enumerate(self.scores(s, 0, 0, blk)):
            new = self.row_max(jnp.maximum(old[g], self.columns(sc, jnp.maximum)))
            p = jnp.exp(sc - self.spread(new))
            alpha = jnp.exp(old[g] - new)
            self.wl[g] = alpha * old_sum[g] + self.columns(p, jnp.add)
            part = jnp.dot(p.astype(BF16), self.part(self.vbuf, 0, 0, g), preferred_element_type=F32)
            self.wacc[g] = jnp.concatenate([alpha] * (self.hd // self.lanes), axis=1) * old_acc[g] + part

    def finish(self, s):
        for g in range(self.nk):
            out = (self.wacc[g] / jnp.sum(self.wl[g], axis=-1, keepdims=True)).astype(BF16)
            for h in range(self.rep):
                lo = (g * self.rep + h) * self.hd
                self.qbuf[s, :, lo : lo + self.hd] = out[h * self.rows : (h + 1) * self.rows]
        local(self.qbuf.at[s], self.o_ref.at[s], self.osem.at[s]).start()

    def wait_out(self):
        for s in range(self.slots):
            local(self.qbuf.at[s], self.o_ref.at[s], self.osem.at[s]).wait()


def first_kernel(n_dev, window_blocks, x_ref, ln_ref, qk_ref, trig_ref, wq_ref, wk_ref, wv_ref,
                 h_ref, o_ref, xbuf, abuf, wq, wk, wv, qbuf, kbuf, vbuf, sbuf, wacc, wm, wl, bias, mx, sm, acc,
                 wsem, xsend, xrecv, hsem, osem, ksend, krecv, fsem):
    me, chip, core, special, row = placement()
    n, rows, dim = x_ref.shape
    hd = qk_ref.shape[-1]
    nq, nk = wq.shape[-1] // hd, wk.shape[-1] // hd
    homes = [home_of(jnp.int32(b), me) for b in range(n)]
    keys = KeyValues(kbuf, vbuf, ksend, krecv, fsem, in_place=True)
    att = Attention(window_blocks, hd, qbuf, kbuf, vbuf, sbuf, wacc, wm, wl, bias, o_ref, osem)

    signal_group(n_dev)
    for b, (dev, slot) in enumerate(homes):

        @pl.when(dev == me)
        def _():
            local(x_ref.at[b], xbuf.at[slot], xrecv.at[slot]).start()

    for j, (src, dst) in enumerate(((wk_ref, wk), (wv_ref, wv), (wq_ref, wq))):
        start_parts(src.at[0], dst, wsem.at[j])
    wait_group(n_dev)
    for b in SEND_ORDER:
        dev, slot = homes[b]

        @pl.when(dev != me)
        def _():
            remote(x_ref.at[b], xbuf.at[slot], xsend.at[b], xrecv.at[slot], dev).start()

    att.fill_bias()
    trig = Trig(trig_ref, 0, rows)
    gain = ln_ref[0, 0:1, :].astype(F32)
    k_gain = qk_ref[0, 1:2, :].astype(F32)
    q_gain = qk_ref[0, 0:1, :].astype(F32)
    for j, (src, dst) in enumerate(((wk_ref, wk), (wv_ref, wv), (wq_ref, wq))):
        local(src.at[0], dst, wsem.at[j]).wait()
    order = [s for c in range(8) for s in ARRIVAL[c]]

    def col(h):
        return pl.ds(h * hd if isinstance(h, int) else pl.multiple_of(h * hd, hd), hd)

    def product(w, h):
        return jnp.dot(abuf[...], w[:, col(h)], preferred_element_type=F32)

    @pl.loop(0, n // 2)
    def _(pair):
        places = [pick(chip * n + 2 * pair + j, order) for j in range(2)]
        turn, idx = [], []
        for j, s in enumerate(places):
            local(xbuf.at[s], xbuf.at[s], xrecv.at[s]).wait()
            local(xbuf.at[s], h_ref.at[s], hsem.at[s]).start()
            abuf[j * rows : (j + 1) * rows, :] = norm_rows(xbuf[s].astype(F32), gain).astype(BF16)
            turn.append(trig.of(slot_place(s, core, special, row)[1]))
            idx.append(kv_index(s, core, special, row))

        @pl.loop(0, nk)
        def _(h):
            k_raw, v_raw = product(wk, h), product(wv, h)
            for j in range(2):
                part = slice(j * rows, (j + 1) * rows)
                kbuf[idx[j], :, col(h)] = norm_turn(k_raw[part], k_gain, *turn[j])
                vbuf[idx[j], :, col(h)] = v_raw[part].astype(BF16)

        def query(h):
            raw = product(wq, h)
            for j, s in enumerate(places):
                part = slice(j * rows, (j + 1) * rows)
                qbuf[s, :, col(h)] = norm_turn(raw[part], q_gain, *turn[j]) * BF16(hd**-0.5)

        query(0)
        for s in places:
            keys.start(s, None)
        pl.loop(1, nq)(query)

    keys.wait_mate(n)

    @pl.loop(0, n)
    def _(s):
        _, blk = slot_place(s, core, special, row)
        base = jnp.where(special == 1, (s // 2) * att.per, 0)
        att.passes(s, blk, base, jnp.where(special == 1, 0, jnp.maximum(att.start_tile(blk), 1)), blk // att.per + 1)
        more = (special == 0) & (s < mx.shape[0])

        @pl.when(more)
        def _():
            for g in range(nk):
                mx[s, g] = wm[g]
                sm[s, g] = wl[g]
                acc[s, g] = wacc[g]

        @pl.when(jnp.logical_not(more))
        def _():
            att.finish(s)

    keys.wait_special()

    @pl.when(special == 0)
    def _():
        @pl.loop(0, mx.shape[0])
        def _(s):
            _, blk = slot_place(s, core, special, row)
            att.merge(s, blk, *[[ref[s, g] for g in range(nk)] for ref in (mx, sm, acc)])
            att.finish(s)

    att.wait_out()
    for s in range(n):
        keys.wait_sent(s, None)
        local(xbuf.at[s], h_ref.at[s], hsem.at[s]).wait()
    for b, (dev, slot) in enumerate(homes):

        @pl.when(dev != me)
        def _():
            remote(x_ref.at[b], xbuf.at[slot], xsend.at[b], xrecv.at[slot], dev).wait_send()


SEND_ORDER = (2, 5, 0, 3, 1, 4)


def attention_scratch(tiles, slots, rows, nq, nk, hd):
    wide = nq // nk * rows
    return [
        pltpu.VMEM((nk, tiles, wide, 4 * rows), F32),
        pltpu.VMEM((nk, wide, hd), F32), pltpu.VMEM((nk, wide, 128), F32), pltpu.VMEM((nk, wide, 128), F32),
        pltpu.VMEM((9, rows, 4 * rows), F32),
    ]


def first(n_dev, window, x, ln_w, qk_w, trig, w_q, w_k, w_v):
    n, rows, dim = x.shape
    hd = qk_w.shape[-1]
    nq, nk = w_q.shape[-1] // hd, w_k.shape[-1] // hd
    blocks, late, wide = 16, 4, nq // nk * rows
    q_shape, kv_shape = (n, rows, nq * hd), (blocks, rows, nk * hd)
    return pl.pallas_call(
        functools.partial(first_kernel, n_dev, window // rows),
        out_shape=[jax.ShapeDtypeStruct(a, BF16) for a in (x.shape, q_shape)],
        in_specs=[ANY, WHOLE, WHOLE, WHOLE, ANY, ANY, ANY],
        out_specs=[ANY] * 2,
        scratch_shapes=[
            pltpu.VMEM(x.shape, BF16), pltpu.VMEM((2 * rows, dim), BF16),
            pltpu.VMEM(w_q.shape[1:], BF16), pltpu.VMEM(w_k.shape[1:], BF16), pltpu.VMEM(w_v.shape[1:], BF16),
            pltpu.VMEM(q_shape, BF16), pltpu.VMEM(kv_shape, BF16), pltpu.VMEM(kv_shape, BF16),
            *attention_scratch(3, n, rows, nq, nk, hd),
            pltpu.VMEM((late, nk, wide, 128), F32), pltpu.VMEM((late, nk, wide, 128), F32), pltpu.VMEM((late, nk, wide, hd), F32),
            DMA((3,)), DMA((n,)), DMA((n,)), DMA((n,)), DMA((n,)), DMA((2, 3, n)), DMA((2, blocks)), DMA((2, 2)),
        ],
        compiler_params=pltpu.CompilerParams(collective_id=0, has_side_effects=True, vmem_limit_bytes=VMEM_LIMIT),
    )(x, ln_w, qk_w, trig, w_q, w_k, w_v)


def attn_kernel(window_blocks, hd, q_ref, k_ref, v_ref, o_ref, kbuf, vbuf, qbuf, sbuf, wacc, wm, wl, bias, qsem, ksem, osem):
    _, _, core, special, row = placement()
    att = Attention(window_blocks, hd, qbuf, kbuf, vbuf, sbuf, wacc, wm, wl, bias, o_ref, osem)
    per = att.per
    tiles = k_ref.shape[0] // per

    def loads(t):
        part = pl.ds(t * per, per)
        return [local(k_ref.at[part], kbuf.at[part], ksem.at[0, t]), local(v_ref.at[part], vbuf.at[part], ksem.at[1, t])]

    for s in range(att.slots):
        local(q_ref.at[s], qbuf.at[s], qsem.at[s]).start()
    for t in range(tiles):
        for c in loads(t):
            c.start()
    att.fill_bias()
    for t in range(tiles):
        for c in loads(t):
            c.wait()

    @pl.loop(0, att.slots)
    def _(s):
        _, blk = slot_place(s, core, special, row)
        local(q_ref.at[s], qbuf.at[s], qsem.at[s]).wait()
        base = jnp.where(special == 1, (s // 2) * per, 0)
        att.passes(s, blk, base, att.start_tile(blk), blk // per + 1)
        att.finish(s)

    att.wait_out()


def attention(window, hd, q, k, v):
    slots, rows = q.shape[:2]
    blocks = k.shape[0]
    nq, nk = q.shape[-1] // hd, k.shape[-1] // hd
    return pl.pallas_call(
        functools.partial(attn_kernel, None if window is None else window // rows, hd),
        out_shape=jax.ShapeDtypeStruct(q.shape, BF16),
        in_specs=[ANY] * 3,
        out_specs=ANY,
        scratch_shapes=[
            pltpu.VMEM(k.shape, BF16), pltpu.VMEM(v.shape, BF16), pltpu.VMEM(q.shape, BF16),
            *attention_scratch(blocks // 4, slots, rows, nq, nk, hd),
            DMA((slots,)), DMA((2, blocks // 4)), DMA((slots,)),
        ],
        compiler_params=pltpu.CompilerParams(vmem_limit_bytes=VMEM_LIMIT),
    )(q, k, v)


def start_parts(src, dst, sem, parts=4):
    n = src.shape[0]
    if n % (parts * 16):
        local(src, dst, sem).start()
        return
    for j in range(parts):
        part = pl.ds(j * (n // parts), n // parts)
        local(src.at[part], dst.at[part], sem).start()


class Ring:
    def __init__(self, buf, sem, count, source):
        self.buf, self.sem, self.count, self.source = buf, sem, count, source
        self.depth = buf.shape[0]

    def begin(self):
        for t in range(min(self.depth, self.count)):
            self.start(t, t)

    def start(self, t, slot):
        def put(ref):
            start_parts(ref, self.buf.at[slot], self.sem.at[slot])

        self.source(t, put)

    def get(self, t):
        slot = lax.rem(t, self.depth) if not isinstance(t, int) else t % self.depth
        local(self.buf.at[slot], self.buf.at[slot], self.sem.at[slot]).wait()
        return self.buf.at[slot]

    def free(self, t):
        new = t + self.depth
        if isinstance(t, int):
            if new < self.count:
                self.start(new, t % self.depth)
            return

        @pl.when(new < self.count)
        def _():
            self.start(new, lax.rem(t, self.depth))


def layer_kernel(layer, last, n_dev, *refs):
    if last:
        (o_ref, x_ref, ln_ref, wo_ref, wg_ref, wu_ref, wd_ref, out_ref,
         obuf, y_ref, att, c_ref, acc, act, wo, wg, wu, wd, isem, osem, gsem, usem, dsem,
         ybuf, ysend, yrecv, osend, orecv) = refs
    else:
        (o_ref, x_ref, ln_ref, qk_ref, trig_ref, wo_ref, wg_ref, wu_ref, wd_ref, wk_ref, wv_ref, wq_ref,
         h_ref, q_ref, k_all, v_all,
         obuf, y_ref, att, c_ref, acc, act, wo, wg, wu, wd, isem, osem, gsem, usem, dsem,
         wn, nsem, qst, kst, vst, tbuf, hsem, qsem, ksend, krecv, fsem) = refs
        keys = KeyValues(k_all, v_all, ksend, krecv, fsem)
        hd = qk_ref.shape[-1]
        nk, nq = wk_ref.shape[-1] // hd, wq_ref.shape[-1] // hd
    rows = acc.shape[0] // 3
    tn, tf = wo.shape[-1], wg.shape[-1]
    n_o, n_f = wo_ref.shape[-1] // tn, wg_ref.shape[-1] // tf

    def cols(t, width):
        start = t * width
        return pl.ds(start if isinstance(t, int) else pl.multiple_of(start, width), width)

    def tile_f(t):
        return (t % n_f) if isinstance(t, int) else lax.rem(t, n_f)

    o_ring = Ring(wo, osem, n_o, lambda t, put: put(wo_ref.at[layer, :, cols(t, tn)]))
    g_ring = Ring(wg, gsem, 2 * n_f, lambda t, put: put(wg_ref.at[layer, :, cols(tile_f(t), tf)]))
    u_ring = Ring(wu, usem, 2 * n_f, lambda t, put: put(wu_ref.at[layer, :, cols(tile_f(t), tf)]))
    d_ring = Ring(wd, dsem, 2 * n_f, lambda t, put: put(wd_ref.at[layer, cols(tile_f(t), tf), :]))

    in_o = local(o_ref, obuf, isem.at[0])
    in_x = local(x_ref, y_ref, isem.at[1])
    start_parts(o_ref, obuf, isem.at[0], 6)
    o_ring.begin()
    start_parts(x_ref, y_ref, isem.at[1], 6)
    for r in (g_ring, u_ring, d_ring):
        r.begin()
    signal_group(n_dev)

    def slot_of(ch, m):
        _, _, _, special, row = placement()
        return chunk_slot(ch, m, special, row)

    def place_of(ch, m):
        _, _, core, special, row = placement()
        return slot_place(chunk_slot(ch, m, special, row), core, special, row)

    def slot_rows(s):
        return pl.ds(pl.multiple_of(s * rows, rows), rows)

    def own_rows(m):
        return pl.ds(m * rows if isinstance(m, int) else pl.multiple_of(m * rows, rows), rows)

    def y_at(ch, m):
        return y_ref.at[slot_rows(slot_of(ch, m))]

    def gain(which, l=layer):
        return ln_ref[l, which : which + 1, :].astype(F32)

    def c_of(y):
        return norm_rows(y.astype(F32), gain(2)).astype(BF16)

    in_o.wait()

    @pl.loop(0, n_o)
    def _(t):
        tile = o_ring.get(t)
        att[:, cols(t, tn)] = jnp.dot(obuf[...], tile[...], preferred_element_type=F32).astype(BF16)
        o_ring.free(t)

    in_x.wait()

    @pl.loop(0, 6)
    def _(j):
        ch, m = j // 3, lax.rem(j, 3)
        r = slot_rows(slot_of(ch, m))
        y = y_ref[r, :].astype(F32) + norm_rows(att[r, :].astype(F32), gain(1))
        y = y.astype(BF16)
        y_ref[r, :] = y
        c_ref[ch, own_rows(m), :] = c_of(y)

    def up(ch, g_tile, u_tile):
        gate = jnp.dot(c_ref[ch], g_tile[...], preferred_element_type=F32)
        val = jnp.dot(c_ref[ch], u_tile[...], preferred_element_type=F32)
        return (jax.nn.gelu(gate, approximate=True) * val).astype(BF16)

    def mlp(ch, after_first):
        base = ch * n_f
        act[0] = up(ch, g_ring.get(base), u_ring.get(base))
        acc[...] = jnp.zeros(acc.shape, F32)
        g_ring.free(base)
        u_ring.free(base)
        after_first(ch)

        @pl.loop(1, n_f)
        def _(t):
            new = lax.rem(t, 2)
            g_tile, u_tile, d_tile = g_ring.get(base + t), u_ring.get(base + t), d_ring.get(base + t - 1)
            acc[...] += jnp.dot(act[1 - new], d_tile[...], preferred_element_type=F32)
            act[new] = up(ch, g_tile, u_tile)
            g_ring.free(base + t)
            u_ring.free(base + t)
            d_ring.free(base + t - 1)

        t = base + n_f - 1
        acc[...] += jnp.dot(act[(n_f - 1) % 2], d_ring.get(t)[...], preferred_element_type=F32)
        d_ring.free(t)

    def result(m, y):
        val = acc[own_rows(m), :].astype(BF16).astype(F32)
        return (y.astype(F32) + norm_rows(val, gain(3))).astype(BF16)

    if last:
        me = lax.axis_index("cp")

        def sent(ch, m):
            b, blk = place_of(ch, m)
            src = y_at(ch, m)
            if ch == 0:
                far = lambda: remote(src, out_ref.at[b], osend.at[m], orecv.at[b], blk)
                return blk, far, lambda: local(src, out_ref.at[b], orecv.at[b])
            return blk, lambda: remote(src, ybuf.at[b // 2], ysend.at[m], yrecv.at[b // 2], blk), None

        def owned(ch, m):
            turn = (me // 2) % 2
            b = 2 * m + (turn if ch == 0 else 1 - turn)
            return b, home_of(b, me)[0]

        def send_streams():
            wait_group(n_dev)
            for m in range(3):
                dev, far, _ = sent(1, m)

                @pl.when(dev != me)
                def _():
                    far().start()

        def send_results():
            for m in range(3):
                dev, far, near = sent(0, m)

                @pl.when(dev != me)
                def _():
                    far().start()

                @pl.when(dev == me)
                def _():
                    near().start()

        def after_first(ch):
            pl.when(ch == 0)(send_streams)
            pl.when(ch == 1)(send_results)

        @pl.loop(0, 2)
        def _(ch):
            mlp(ch, after_first)

            @pl.when(ch == 0)
            def _():
                @pl.loop(0, 3)
                def _(m):
                    y_at(0, m)[...] = result(m, y_at(0, m)[...])

                for m in range(3):
                    _, dev = owned(1, m)

                    @pl.when(dev != me)
                    def _():
                        remote(ybuf.at[m], ybuf.at[m], ysend.at[m], yrecv.at[m], me).wait_recv()

                for m in range(3):
                    b, blk = place_of(1, m)

                    @pl.when(blk == me)
                    def _():
                        ybuf[b // 2] = y_at(1, m)[...]

                @pl.loop(0, 3)
                def _(m):
                    c_ref[1, own_rows(m), :] = c_of(ybuf[m])

        @pl.loop(0, 3)
        def _(m):
            ybuf[m] = result(m, ybuf[m])

        for m in range(3):
            b, _ = owned(1, m)
            local(ybuf.at[m], out_ref.at[b], orecv.at[b]).start()
        for ch in range(2):
            for m in range(3):
                dev, far, _ = sent(ch, m)

                @pl.when(dev != me)
                def _():
                    far().wait_send()

        for b in range(6):
            local(out_ref.at[b], out_ref.at[b], orecv.at[b]).wait()
        return

    def source(t, put):
        kind = lax.rem(t, 2 * nk) if not isinstance(t, int) else t % (2 * nk)
        cases = (
            (jnp.logical_and(t < 4 * nk, kind < nk), lambda: put(wk_ref.at[layer + 1, :, cols(kind, hd)])),
            (jnp.logical_and(t < 4 * nk, kind >= nk), lambda: put(wv_ref.at[layer + 1, :, cols(kind - nk, hd)])),
            (t >= 4 * nk, lambda: put(wq_ref.at[layer + 1, :, cols(t - 4 * nk, hd)])),
        )
        for cond, do in cases:
            pl.when(cond)(do)

    n_ring = Ring(wn, nsem, 4 * nk + nq, source)
    n_ring.begin()
    k_gain, q_gain = (qk_ref[layer + 1, j : j + 1, :].astype(F32) for j in (1, 0))

    trig = Trig(trig_ref, layer + 1, rows)

    @pl.loop(0, 6)
    def _(j):
        ch, m = j // 3, lax.rem(j, 3)
        tbuf[ch, m, 0], tbuf[ch, m, 1] = trig.of(place_of(ch, m)[1])

    def turn(ch, m):
        return tbuf[ch, m, 0], tbuf[ch, m, 1]

    def send_keys(ch):
        for m in range(3):
            keys.start(slot_of(ch, m), (kst.at[ch, m], vst.at[ch, m]))

    def keys_and_values(ch):
        @pl.loop(0, 3)
        def _(m):
            h = result(m, y_at(ch, m)[...])
            y_at(ch, m)[...] = h
            c_ref[ch, own_rows(m), :] = norm_rows(h.astype(F32), gain(0, layer + 1)).astype(BF16)

        @pl.loop(0, nk)
        def _(h):
            t = ch * 2 * nk + h
            raw = jnp.dot(c_ref[ch], n_ring.get(t)[...], preferred_element_type=F32)
            n_ring.free(t)
            for m in range(3):
                kst[ch, m, :, cols(h, hd)] = norm_turn(raw[m * rows : (m + 1) * rows], k_gain, *turn(ch, m))

        @pl.loop(0, nk)
        def _(h):
            t = (ch * 2 + 1) * nk + h
            raw = jnp.dot(c_ref[ch], n_ring.get(t)[...], preferred_element_type=F32)
            n_ring.free(t)
            for m in range(3):
                vst[ch, m, :, cols(h, hd)] = raw[m * rows : (m + 1) * rows].astype(BF16)

        for m in range(3):
            s = slot_of(ch, m)
            local(y_at(ch, m), h_ref.at[s], hsem.at[s]).start()

    def query(h):
        t = 4 * nk + h
        tile = n_ring.get(t)
        for ch in range(2):
            raw = jnp.dot(c_ref[ch], tile[...], preferred_element_type=F32)
            for m in range(3):
                out = norm_turn(raw[m * rows : (m + 1) * rows], q_gain, *turn(ch, m))
                qst[ch, m, :, cols(h, hd)] = out * BF16(hd**-0.5)
        n_ring.free(t)

    def first_keys():
        wait_group(n_dev)
        send_keys(0)

    @pl.loop(0, 2)
    def _(ch):
        mlp(ch, lambda ch: pl.when(ch == 1)(first_keys))
        keys_and_values(ch)

    query(0)
    send_keys(1)
    pl.loop(1, nq)(query)
    for ch in range(2):
        for m in range(3):
            s = slot_of(ch, m)
            local(qst.at[ch, m], q_ref.at[s], qsem.at[s]).start()
    for ch in range(2):
        for m in range(3):
            s = slot_of(ch, m)
            keys.wait_sent(s, (kst.at[ch, m], vst.at[ch, m]))
            local(qst.at[ch, m], q_ref.at[s], qsem.at[s]).wait()
            local(y_at(ch, m), h_ref.at[s], hsem.at[s]).wait()
    keys.wait_mate(6)
    keys.wait_special()


def after_attention(layer, last, n_dev, cid, o, x, ln_w, w_o, w_gate, w_up, w_down, more=()):
    slots, rows, dim = x.shape
    inner, ff = w_o.shape[1], w_gate.shape[-1]
    total = slots * rows
    half = total // 2
    blocks = 16
    tn, tf = min(256, dim), min(512, ff)
    deep = 3
    o2, x2 = o.reshape(total, inner), x.reshape(total, dim)
    work = [
        pltpu.VMEM((total, inner), BF16), pltpu.VMEM((total, dim), BF16),
        pltpu.VMEM((total, dim), BF16), pltpu.VMEM((2, half, dim), BF16),
        pltpu.VMEM((half, dim), F32), pltpu.VMEM((2, half, tf), BF16),
        pltpu.VMEM((deep, inner, tn), BF16), pltpu.VMEM((deep, dim, tf), BF16), pltpu.VMEM((deep, dim, tf), BF16),
        pltpu.VMEM((deep, tf, dim), BF16),
        DMA((2,)), DMA((deep,)), DMA((deep,)), DMA((deep,)), DMA((deep,)),
    ]
    params = pltpu.CompilerParams(collective_id=cid, has_side_effects=True, vmem_limit_bytes=VMEM_LIMIT)
    body = functools.partial(layer_kernel, layer, last, n_dev)
    if last:
        return pl.pallas_call(
            body,
            in_specs=[ANY, ANY, WHOLE] + [ANY] * 4,
            out_specs=ANY,
            out_shape=jax.ShapeDtypeStruct(x.shape, BF16),
            scratch_shapes=work + [pltpu.VMEM((3, rows, dim), BF16), DMA((3,)), DMA((3,)), DMA((3,)), DMA((slots,))],
            compiler_params=params,
        )(o2, x2, ln_w, w_o, w_gate, w_up, w_down)
    qk_w, trig, w_q, w_k, w_v = more
    hd = qk_w.shape[-1]
    nq, nk = w_q.shape[-1] // hd, w_k.shape[-1] // hd
    q_shape, kv_shape = (slots, rows, nq * hd), (blocks, rows, nk * hd)
    return pl.pallas_call(
        body,
        in_specs=[ANY, ANY, WHOLE, WHOLE, WHOLE] + [ANY] * 7,
        out_specs=[ANY] * 4,
        out_shape=[jax.ShapeDtypeStruct(a, BF16) for a in (x.shape, q_shape, kv_shape, kv_shape)],
        scratch_shapes=work + [
            pltpu.VMEM((deep, dim, hd), BF16), DMA((deep,)),
            pltpu.VMEM((2, 3, rows, nq * hd), BF16), pltpu.VMEM((2, 3, rows, nk * hd), BF16), pltpu.VMEM((2, 3, rows, nk * hd), BF16),
            pltpu.VMEM((2, 3, 2, rows, hd // 2), F32),
            DMA((slots,)), DMA((slots,)), DMA((2, 3, slots)), DMA((2, blocks)), DMA((2, 2)),
        ],
        compiler_params=params,
    )(o2, x2, ln_w, qk_w, trig, w_o, w_gate, w_up, w_down, w_k, w_v, w_q)


def rope_table(rows, blocks, hd):
    half = hd // 2
    pos = jnp.concatenate([jnp.arange(rows), rows * jnp.arange(blocks)]).astype(F32)
    out = []
    for base, scale in ((LOCAL_BASE, 1.0), (GLOBAL_BASE, GLOBAL_SCALE)):
        freq = base ** (-2.0 * jnp.arange(half, dtype=F32) / hd)
        ang = (pos / scale)[:, None] * freq[None, :]
        out.append(jnp.stack([jnp.cos(ang), jnp.sin(ang)]))
    return jnp.stack(out)


def solution(mesh):
    n_dev = mesh.shape["cp"]

    def device_fn(x_loc, ln_w, qk_w, w_q, w_k, w_v, w_o, w_gate, w_up, w_down):
        rows, hd = x_loc.shape[1], qk_w.shape[-1]
        trig = rope_table(rows, n_dev, hd)
        x, o = first(n_dev, WINDOW, x_loc, ln_w, qk_w, trig, w_q, w_k, w_v)
        mlp = (w_o, w_gate, w_up, w_down)
        x, q, k, v = after_attention(0, False, n_dev, 1, o, x, ln_w, *mlp, more=(qk_w, trig, w_q, w_k, w_v))
        o = attention(None, hd, q, k, v)
        return after_attention(1, True, n_dev, 2, o, x, ln_w, *mlp)

    act_part = P("dp", "cp", None)
    return jax.shard_map(device_fn, mesh=mesh, in_specs=(act_part,) + (P(),) * 9, out_specs=act_part, check_vma=False)
```

```python
import functools

import jax
import jax.numpy as jnp
from jax import lax
from jax.experimental import pallas as pl
from jax.experimental.pallas import tpu as pltpu
from jax.sharding import PartitionSpec as P

WINDOW = 1024
NORM_EPS = 1e-6
LOCAL_BASE = 10000.0
GLOBAL_BASE = 1000000.0
GLOBAL_SCALE = 8.0
NEG = -1e30

ROW_CHIP = (0, 3, 4, 1, 5, 6)
SPECIAL = (2, 7)
VMEM_LIMIT = 64 * 1024 * 1024 - 128 * 1024
MESH = pl.DeviceIdType.MESH
BF16, F32 = jnp.bfloat16, jnp.float32
ANY = pl.BlockSpec(memory_space=pl.ANY)
WHOLE = pl.BlockSpec(memory_space=pltpu.VMEM)
DMA = pltpu.SemaphoreType.DMA


def pick(idx, table):
    out = jnp.int32(table[-1])
    for i in range(len(table) - 2, -1, -1):
        out = jnp.where(idx == i, jnp.int32(table[i]), out)
    return out


def placement():
    me = lax.axis_index("cp")
    chip, core = me // 2, me % 2
    roles = [0] * 8
    rows = [0] * 8
    for b, c in enumerate(ROW_CHIP):
        rows[c] = b
    for i, c in enumerate(SPECIAL):
        roles[c] = 1
        rows[c] = 3 * i
    return me, chip, core, pick(chip, roles), pick(chip, rows)


def slot_place(s, core, special, row):
    k = s % 2
    blk = jnp.where(special == 1, 2 * k + (k + core) % 2, 4 + 2 * s + (s + core) % 2)
    b = jnp.where(special == 1, row + s // 2, row)
    return b, blk


EARLY_ORDER = (2, 5, 1, 4, 0, 3)


def arrival():
    out = []
    for dev in range(16):
        chip, core = dev // 2, dev % 2
        if chip in SPECIAL:
            out += [4, 5, 2, 3, 0, 1]
            continue
        b = ROW_CHIP.index(chip)
        for step in range(6):
            out += [(j - 4) // 2 for j in range(4, 16) if (j + step) % 6 == b and (j + 1) // 2 % 2 == core]
    return out


def home_of(b, blk):
    core = ((blk + 1) // 2) % 2
    half = blk // 2
    chip = jnp.where(blk < 4, pick(b // 3, SPECIAL), pick(b, ROW_CHIP))
    slot = jnp.where(blk < 4, (b % 3) * 2 + half, half - 2)
    return chip * 2 + core, slot


def chunk_slot(ch, i, special, row):
    b = jnp.where(special == 1, row + i, row)
    return 2 * i + (b + ch) % 2


def kv_index(s, core, special, row):
    _, blk = slot_place(s, core, special, row)
    return jnp.where(special == 1, (s // 2) * 4 + blk, blk)


def served(row, r):
    return jnp.where(row == 0, ROW_CHIP[r], ROW_CHIP[r + 3])


def signal_group(n_dev):
    me = lax.axis_index("cp")
    barrier = pltpu.get_barrier_semaphore()
    for d in range(1, n_dev):
        pl.semaphore_signal(barrier, inc=1, device_id={"cp": lax.rem(me + d, n_dev)}, device_id_type=MESH)


def wait_group(n_dev):
    pl.semaphore_wait(pltpu.get_barrier_semaphore(), n_dev - 1)


def remote(src, dst, send, recv, dev):
    return pltpu.make_async_remote_copy(
        src_ref=src, dst_ref=dst, send_sem=send, recv_sem=recv, device_id={"cp": dev}, device_id_type=MESH
    )


def local(src, dst, sem):
    return pltpu.make_async_copy(src, dst, sem)


def norm_rows(vals, gain):
    inv = lax.rsqrt(jnp.mean(vals * vals, axis=-1, keepdims=True) + NORM_EPS)
    return vals * inv * (1.0 + gain)


def norm_turn(raw, gain, cos, sin):
    half = raw.shape[-1] // 2
    vals = norm_rows(raw.astype(BF16).astype(F32), gain)
    first, second = vals[:, :half], vals[:, half:]
    return jnp.concatenate([first * cos - second * sin, second * cos + first * sin], axis=-1).astype(BF16)


class KeyValues:
    def __init__(self, k_all, v_all, send, recv, fwd, in_place=False):
        self.in_place = in_place
        self.both = ((0, k_all), (1, v_all))
        self.send, self.recv, self.fwd = send, recv, fwd

    def here(self):
        _, chip, self.core, self.special, self.row = placement()
        self.mate = chip * 2 + 1 - self.core

    def _copies(self, s, stage):
        idx = kv_index(s, self.core, self.special, self.row)
        _, blk = slot_place(s, self.core, self.special, self.row)
        dev = served(self.row, 0) * 2 + self.core
        for r in (1, 2):
            dev = jnp.where(s // 2 == r, served(self.row, r) * 2 + self.core, dev)
        out = []
        for x, full in self.both:
            src = full.at[idx] if self.in_place else stage[x]
            out.append((
                None if self.in_place else local(src, full.at[idx], self.send.at[x, 0, s]),
                remote(src, full.at[idx], self.send.at[x, 1, s], self.recv.at[x, idx], self.mate),
                remote(src, full.at[blk], self.send.at[x, 2, s], self.recv.at[x, blk], dev),
            ))
        return out

    def start(self, s, stage):
        self.here()
        for own, mate, row in self._copies(s, stage):

            @pl.when(self.special == 1)
            def _():
                row.start()

            mate.start()
            if own is not None:
                own.start()

    def wait_sent(self, s, stage):
        self.here()
        for own, mate, row in self._copies(s, stage):
            if own is not None:
                own.wait()
            mate.wait_send()

            @pl.when(self.special == 1)
            def _():
                row.wait_send()

    def wait_mate(self, slots):
        self.here()
        for x, full in self.both:
            for s in range(slots):
                idx = kv_index(s, 1 - self.core, self.special, self.row)
                remote(full.at[idx], full.at[idx], self.fwd.at[x, 0], self.recv.at[x, idx], self.mate).wait_recv()

    def wait_special(self):
        self.here()

        @pl.when(self.special == 0)
        def _():
            for k in range(2):
                blk = 2 * k + (k + self.core) % 2
                for x, full in self.both:
                    remote(full.at[blk], full.at[blk], self.fwd.at[x, k], self.recv.at[x, blk], self.mate).wait_recv()
                    remote(full.at[blk], full.at[blk], self.fwd.at[x, k], self.recv.at[x, blk], self.mate).start()
            for x, full in self.both:
                for k in range(2):
                    blk = 2 * k + (k + 1 - self.core) % 2
                    remote(full.at[blk], full.at[blk], self.fwd.at[x, k], self.recv.at[x, blk], self.mate).wait()


class Trig:
    def __init__(self, ref, layer, rows):
        self.ref, self.layer, self.rows = ref, layer, rows

    def of(self, blk):
        cu, su = (self.ref[self.layer, j, : self.rows, :] for j in range(2))
        cb, sb = (self.ref[self.layer, j, pl.ds(self.rows + blk, 1), :] for j in range(2))
        return cu * cb - su * sb, su * cb + cu * sb


class Attention:
    per, lanes = 4, 128

    def __init__(self, window_blocks, hd, qbuf, kbuf, vbuf, sbuf, wacc, wm, wl, bias, o_ref, osem):
        self.window_blocks, self.hd = window_blocks, hd
        self.qbuf, self.kbuf, self.vbuf, self.sbuf, self.bias = qbuf, kbuf, vbuf, sbuf, bias
        self.wacc, self.wm, self.wl, self.o_ref, self.osem = wacc, wm, wl, o_ref, osem
        self.slots, self.rows = qbuf.shape[:2]
        self.nk = kbuf.shape[-1] // hd
        self.rep = qbuf.shape[-1] // kbuf.shape[-1]
        self.tile = self.per * self.rows
        self.group = wacc.shape[1] // (self.rep * self.rows)

    def fill_bias(self):
        rows, tile, bias = self.rows, self.tile, self.bias
        qi = lax.broadcasted_iota(jnp.int32, (rows, tile), 0)
        ki = lax.broadcasted_iota(jnp.int32, (rows, tile), 1)
        bias[0] = jnp.zeros((rows, tile), F32)
        for j in range(self.per):
            bias[1 + j] = jnp.where(ki <= qi + j * rows, 0.0, NEG)
            if self.window_blocks is not None:
                bias[1 + self.per + j] = jnp.where(ki > qi + j * rows, 0.0, NEG)

    def start_tile(self, blk):
        if self.window_blocks is None:
            return jnp.int32(0)
        return jnp.maximum(blk - self.window_blocks, 0) // self.per

    def part(self, buf, t, base, g):
        block = buf.at[pl.ds(base + self.per * t, self.per)]
        return block[:, :, g * self.hd : (g + 1) * self.hd].reshape(self.tile, self.hd)

    def edge(self, t, blk):
        per = self.per
        out = jnp.where(t == blk // per, 1 + blk % per, 0)
        if self.window_blocks is not None:
            old = blk - self.window_blocks
            out = jnp.where((old >= 0) & (t == old // per), 1 + per + old % per, out)
        return out

    def scores(self, s, t, base, blks):
        rows, rep, hd, group = self.rows, self.rep, self.hd, self.group
        offs = [self.bias[self.edge(t, blk)][None] for blk in blks]
        out = []
        for g in range(self.nk):
            heads = [self.qbuf[s + j, :, h * hd : (h + 1) * hd] for j in range(group) for h in range(g * rep, (g + 1) * rep)]
            q = jnp.concatenate(heads, axis=0)
            sc = lax.dot_general(q, self.part(self.kbuf, t, base, g), (((1,), (1,)), ((), ())), preferred_element_type=F32)
            sc = sc.reshape(group, rep, rows, self.tile)
            sc = jnp.concatenate([sc[j] + offs[j] for j in range(group)], axis=0)
            out.append(sc.reshape(group * rep * rows, self.tile))
        return out

    def columns(self, val, op):
        return functools.reduce(op, [val[:, j * self.lanes : (j + 1) * self.lanes] for j in range(self.tile // self.lanes)])

    def spread(self, val):
        return jnp.concatenate([val] * (self.tile // self.lanes), axis=1)

    def row_max(self, val):
        return jnp.broadcast_to(jnp.max(val, axis=-1, keepdims=True), val.shape)

    def passes(self, s, blks, base, first, last):
        for g in range(self.nk):
            self.wm[g] = jnp.full(self.wm.shape[1:], NEG, F32)
            self.wl[g] = jnp.zeros(self.wl.shape[1:], F32)
            self.wacc[g] = jnp.zeros(self.wacc.shape[1:], F32)

        @pl.loop(first, last)
        def _(t):
            for g, sc in enumerate(self.scores(s, t, base, blks)):
                self.sbuf[g, t - first] = sc
                self.wm[g] = jnp.maximum(self.wm[g], self.columns(sc, jnp.maximum))

        for g in range(self.nk):
            self.wm[g] = self.row_max(self.wm[g])

        @pl.loop(first, last)
        def _(t):
            for g in range(self.nk):
                p = jnp.exp(self.sbuf[g, t - first] - self.spread(self.wm[g]))
                self.wl[g] += self.columns(p, jnp.add)
                self.wacc[g] += jnp.dot(p.astype(BF16), self.part(self.vbuf, t, base, g), preferred_element_type=F32)

    def merge(self, s, blk, old, old_sum, old_acc):
        for g, sc in enumerate(self.scores(s, 0, 0, [blk])):
            new = self.row_max(jnp.maximum(old[g], self.columns(sc, jnp.maximum)))
            p = jnp.exp(sc - self.spread(new))
            alpha = jnp.exp(old[g] - new)
            self.wl[g] = alpha * old_sum[g] + self.columns(p, jnp.add)
            part = jnp.dot(p.astype(BF16), self.part(self.vbuf, 0, 0, g), preferred_element_type=F32)
            self.wacc[g] = jnp.concatenate([alpha] * (self.hd // self.lanes), axis=1) * old_acc[g] + part

    def finish(self, s):
        for g in range(self.nk):
            out = (self.wacc[g] / jnp.sum(self.wl[g], axis=-1, keepdims=True)).astype(BF16)
            for j in range(self.group):
                for h in range(self.rep):
                    lo, r = (g * self.rep + h) * self.hd, (j * self.rep + h) * self.rows
                    self.qbuf[s + j, :, lo : lo + self.hd] = out[r : r + self.rows]
        for j in range(self.group):
            local(self.qbuf.at[s + j], self.o_ref.at[s + j], self.osem.at[s + j]).start()

    def wait_out(self):
        for s in range(self.slots):
            local(self.qbuf.at[s], self.o_ref.at[s], self.osem.at[s]).wait()


def first_kernel(n_dev, window_blocks, x_ref, ln_ref, qk_ref, trig_ref, wq_ref, wk_ref, wv_ref,
                 h_ref, o_ref, xbuf, abuf, wq, wk, wv, qbuf, kbuf, vbuf, sbuf, wacc, wm, wl, bias, mx, sm, acc,
                 wsem, xsend, xrecv, hsem, osem, ksend, krecv, fsem):
    me, chip, core, special, row = placement()
    n, rows, dim = x_ref.shape
    hd = qk_ref.shape[-1]
    nq, nk = wq.shape[-1] // hd, wk.shape[-1] // hd
    homes = [home_of(jnp.int32(b), me) for b in range(n)]
    keys = KeyValues(kbuf, vbuf, ksend, krecv, fsem, in_place=True)
    att = Attention(window_blocks, hd, qbuf, kbuf, vbuf, sbuf, wacc, wm, wl, bias, o_ref, osem)

    signal_group(n_dev)
    for b, (dev, slot) in enumerate(homes):

        @pl.when(dev == me)
        def _():
            local(x_ref.at[b], xbuf.at[slot], xrecv.at[slot]).start()

    for j, (src, dst) in enumerate(((wk_ref, wk), (wv_ref, wv), (wq_ref, wq))):
        start_parts(src.at[0], dst, wsem.at[j])
    wait_group(n_dev)
    for step in range(n):
        b = jnp.where(me < 4, EARLY_ORDER[step], lax.rem(me + step, n))
        dev, slot = home_of(b, me)

        @pl.when(dev != me)
        def _():
            remote(x_ref.at[b], xbuf.at[slot], xsend.at[b], xrecv.at[slot], dev).start()

    att.fill_bias()
    trig = Trig(trig_ref, 0, rows)
    gain = ln_ref[0, 0:1, :].astype(F32)
    k_gain = qk_ref[0, 1:2, :].astype(F32)
    q_gain = qk_ref[0, 0:1, :].astype(F32)
    for j, (src, dst) in enumerate(((wk_ref, wk), (wv_ref, wv), (wq_ref, wq))):
        local(src.at[0], dst, wsem.at[j]).wait()
    order = arrival()

    def col(h):
        return pl.ds(h * hd if isinstance(h, int) else pl.multiple_of(h * hd, hd), hd)

    def product(w, h):
        return jnp.dot(abuf[...], w[:, col(h)], preferred_element_type=F32)

    @pl.loop(0, n // 2)
    def _(pair):
        places = [pick(me * n + 2 * pair + j, order) for j in range(2)]
        turn, idx = [], []
        for j, s in enumerate(places):
            local(xbuf.at[s], xbuf.at[s], xrecv.at[s]).wait()
            local(xbuf.at[s], h_ref.at[s], hsem.at[s]).start()
            abuf[j * rows : (j + 1) * rows, :] = norm_rows(xbuf[s].astype(F32), gain).astype(BF16)
            turn.append(trig.of(slot_place(s, core, special, row)[1]))
            idx.append(kv_index(s, core, special, row))

        @pl.loop(0, nk)
        def _(h):
            k_raw, v_raw = product(wk, h), product(wv, h)
            for j in range(2):
                part = slice(j * rows, (j + 1) * rows)
                kbuf[idx[j], :, col(h)] = norm_turn(k_raw[part], k_gain, *turn[j])
                vbuf[idx[j], :, col(h)] = v_raw[part].astype(BF16)

        def query(h):
            raw = product(wq, h)
            for j, s in enumerate(places):
                part = slice(j * rows, (j + 1) * rows)
                qbuf[s, :, col(h)] = norm_turn(raw[part], q_gain, *turn[j]) * BF16(hd**-0.5)

        query(0)
        for s in places:
            keys.start(s, None)
        pl.loop(1, nq)(query)

    keys.wait_mate(n)

    @pl.loop(0, n)
    def _(s):
        _, blk = slot_place(s, core, special, row)
        base = jnp.where(special == 1, (s // 2) * att.per, 0)
        att.passes(s, [blk], base, jnp.where(special == 1, 0, jnp.maximum(att.start_tile(blk), 1)), blk // att.per + 1)
        more = (special == 0) & (s < mx.shape[0])

        @pl.when(more)
        def _():
            for g in range(nk):
                mx[s, g] = wm[g]
                sm[s, g] = wl[g]
                acc[s, g] = wacc[g]

        @pl.when(jnp.logical_not(more))
        def _():
            att.finish(s)

    keys.wait_special()

    @pl.when(special == 0)
    def _():
        @pl.loop(0, mx.shape[0])
        def _(s):
            _, blk = slot_place(s, core, special, row)
            att.merge(s, blk, *[[ref[s, g] for g in range(nk)] for ref in (mx, sm, acc)])
            att.finish(s)

    att.wait_out()
    for s in range(n):
        keys.wait_sent(s, None)
        local(xbuf.at[s], h_ref.at[s], hsem.at[s]).wait()
    for b, (dev, slot) in enumerate(homes):

        @pl.when(dev != me)
        def _():
            remote(x_ref.at[b], xbuf.at[slot], xsend.at[b], xrecv.at[slot], dev).wait_send()


def attention_scratch(tiles, group, rows, nq, nk, hd):
    wide = group * nq // nk * rows
    return [
        pltpu.VMEM((nk, tiles, wide, 4 * rows), F32),
        pltpu.VMEM((nk, wide, hd), F32), pltpu.VMEM((nk, wide, 128), F32), pltpu.VMEM((nk, wide, 128), F32),
        pltpu.VMEM((9, rows, 4 * rows), F32),
    ]


def first(n_dev, window, x, ln_w, qk_w, trig, w_q, w_k, w_v):
    n, rows, dim = x.shape
    hd = qk_w.shape[-1]
    nq, nk = w_q.shape[-1] // hd, w_k.shape[-1] // hd
    blocks, late, wide = 16, 4, nq // nk * rows
    q_shape, kv_shape = (n, rows, nq * hd), (blocks, rows, nk * hd)
    return pl.pallas_call(
        functools.partial(first_kernel, n_dev, window // rows),
        out_shape=[jax.ShapeDtypeStruct(a, BF16) for a in (x.shape, q_shape)],
        in_specs=[ANY, WHOLE, WHOLE, WHOLE, ANY, ANY, ANY],
        out_specs=[ANY] * 2,
        scratch_shapes=[
            pltpu.VMEM(x.shape, BF16), pltpu.VMEM((2 * rows, dim), BF16),
            pltpu.VMEM(w_q.shape[1:], BF16), pltpu.VMEM(w_k.shape[1:], BF16), pltpu.VMEM(w_v.shape[1:], BF16),
            pltpu.VMEM(q_shape, BF16), pltpu.VMEM(kv_shape, BF16), pltpu.VMEM(kv_shape, BF16),
            *attention_scratch(3, 1, rows, nq, nk, hd),
            pltpu.VMEM((late, nk, wide, 128), F32), pltpu.VMEM((late, nk, wide, 128), F32), pltpu.VMEM((late, nk, wide, hd), F32),
            DMA((3,)), DMA((n,)), DMA((n,)), DMA((n,)), DMA((n,)), DMA((2, 3, n)), DMA((2, blocks)), DMA((2, 2)),
        ],
        compiler_params=pltpu.CompilerParams(collective_id=0, has_side_effects=True, vmem_limit_bytes=VMEM_LIMIT),
    )(x, ln_w, qk_w, trig, w_q, w_k, w_v)


def attn_kernel(window_blocks, hd, q_ref, k_ref, v_ref, o_ref, kbuf, vbuf, qbuf, sbuf, wacc, wm, wl, bias, qsem, ksem, osem):
    _, _, core, special, row = placement()
    att = Attention(window_blocks, hd, qbuf, kbuf, vbuf, sbuf, wacc, wm, wl, bias, o_ref, osem)
    per = att.per
    tiles = k_ref.shape[0] // per

    def loads(t):
        part = pl.ds(t * per, per)
        return [local(k_ref.at[part], kbuf.at[part], ksem.at[0, t]), local(v_ref.at[part], vbuf.at[part], ksem.at[1, t])]

    for s in range(att.slots):
        local(q_ref.at[s], qbuf.at[s], qsem.at[s]).start()
    for t in range(tiles):
        for c in loads(t):
            c.start()
    att.fill_bias()
    group = att.group

    @pl.loop(0, att.slots // group)
    def _(i):
        for t in range(tiles):

            @pl.when(i == max(t - 1, 0))
            def _():
                for c in loads(t):
                    c.wait()

        s = i * group
        blks = [slot_place(s + j, core, special, row)[1] for j in range(group)]
        for j in range(group):
            local(q_ref.at[s + j], qbuf.at[s + j], qsem.at[s + j]).wait()
        base = jnp.where(special == 1, i * per, 0)
        att.passes(s, blks, base, att.start_tile(blks[0]), blks[0] // per + 1)
        att.finish(s)

    att.wait_out()


def attention(window, hd, q, k, v):
    slots, rows = q.shape[:2]
    blocks = k.shape[0]
    nq, nk = q.shape[-1] // hd, k.shape[-1] // hd
    return pl.pallas_call(
        functools.partial(attn_kernel, None if window is None else window // rows, hd),
        out_shape=jax.ShapeDtypeStruct(q.shape, BF16),
        in_specs=[ANY] * 3,
        out_specs=ANY,
        scratch_shapes=[
            pltpu.VMEM(k.shape, BF16), pltpu.VMEM(v.shape, BF16), pltpu.VMEM(q.shape, BF16),
            *attention_scratch(blocks // 4, 2, rows, nq, nk, hd),
            DMA((slots,)), DMA((2, blocks // 4)), DMA((slots,)),
        ],
        compiler_params=pltpu.CompilerParams(vmem_limit_bytes=VMEM_LIMIT),
    )(q, k, v)


def start_parts(src, dst, sem, parts=4):
    n = src.shape[0]
    if n % (parts * 16):
        local(src, dst, sem).start()
        return
    for j in range(parts):
        part = pl.ds(j * (n // parts), n // parts)
        local(src.at[part], dst.at[part], sem).start()


class Ring:
    def __init__(self, buf, sem, count, source):
        self.buf, self.sem, self.count, self.source = buf, sem, count, source
        self.depth = buf.shape[0]

    def begin(self):
        for t in range(min(self.depth, self.count)):
            self.start(t, t)

    def start(self, t, slot):
        def put(ref):
            start_parts(ref, self.buf.at[slot], self.sem.at[slot])

        self.source(t, put)

    def get(self, t):
        slot = lax.rem(t, self.depth) if not isinstance(t, int) else t % self.depth
        local(self.buf.at[slot], self.buf.at[slot], self.sem.at[slot]).wait()
        return self.buf.at[slot]

    def free(self, t):
        new = t + self.depth
        if isinstance(t, int):
            if new < self.count:
                self.start(new, t % self.depth)
            return

        @pl.when(new < self.count)
        def _():
            self.start(new, lax.rem(t, self.depth))


def layer_kernel(layer, last, n_dev, *refs):
    if last:
        (o_ref, x_ref, ln_ref, wo_ref, wg_ref, wu_ref, wd_ref, out_ref,
         obuf, y_ref, att, c_ref, acc, act, wo, wg, wu, wd, isem, osem, gsem, usem, dsem,
         ybuf, ysend, yrecv, osend, orecv) = refs
    else:
        (o_ref, x_ref, ln_ref, qk_ref, trig_ref, wo_ref, wg_ref, wu_ref, wd_ref, wk_ref, wv_ref, wq_ref,
         h_ref, q_ref, k_all, v_all,
         obuf, y_ref, att, c_ref, acc, act, wo, wg, wu, wd, isem, osem, gsem, usem, dsem,
         wn, nsem, qst, kst, vst, tbuf, hsem, qsem, ksend, krecv, fsem) = refs
        keys = KeyValues(k_all, v_all, ksend, krecv, fsem)
        hd = qk_ref.shape[-1]
        nk, nq = wk_ref.shape[-1] // hd, wq_ref.shape[-1] // hd
    rows = acc.shape[0] // 3
    tn, tf = wo.shape[-1], wg.shape[-1]
    n_o, n_f = wo_ref.shape[-1] // tn, wg_ref.shape[-1] // tf

    def cols(t, width):
        start = t * width
        return pl.ds(start if isinstance(t, int) else pl.multiple_of(start, width), width)

    def tile_f(t):
        return (t % n_f) if isinstance(t, int) else lax.rem(t, n_f)

    o_ring = Ring(wo, osem, n_o, lambda t, put: put(wo_ref.at[layer, :, cols(t, tn)]))
    g_ring = Ring(wg, gsem, 2 * n_f, lambda t, put: put(wg_ref.at[layer, :, cols(tile_f(t), tf)]))
    u_ring = Ring(wu, usem, 2 * n_f, lambda t, put: put(wu_ref.at[layer, :, cols(tile_f(t), tf)]))
    d_ring = Ring(wd, dsem, 2 * n_f, lambda t, put: put(wd_ref.at[layer, cols(tile_f(t), tf), :]))

    in_o = local(o_ref, obuf, isem.at[0])
    in_x = local(x_ref, y_ref, isem.at[1])
    start_parts(o_ref, obuf, isem.at[0], 6)
    o_ring.begin()
    start_parts(x_ref, y_ref, isem.at[1], 6)
    for r in (g_ring, u_ring, d_ring):
        r.begin()
    signal_group(n_dev)

    def slot_of(ch, m):
        _, _, _, special, row = placement()
        return chunk_slot(ch, m, special, row)

    def place_of(ch, m):
        _, _, core, special, row = placement()
        return slot_place(chunk_slot(ch, m, special, row), core, special, row)

    def slot_rows(s):
        return pl.ds(pl.multiple_of(s * rows, rows), rows)

    def own_rows(m):
        return pl.ds(m * rows if isinstance(m, int) else pl.multiple_of(m * rows, rows), rows)

    def y_at(ch, m):
        return y_ref.at[slot_rows(slot_of(ch, m))]

    def gain(which, l=layer):
        return ln_ref[l, which : which + 1, :].astype(F32)

    def c_of(y):
        return norm_rows(y.astype(F32), gain(2)).astype(BF16)

    in_o.wait()

    @pl.loop(0, n_o)
    def _(t):
        tile = o_ring.get(t)
        att[:, cols(t, tn)] = jnp.dot(obuf[...], tile[...], preferred_element_type=F32).astype(BF16)
        o_ring.free(t)

    in_x.wait()

    @pl.loop(0, 6)
    def _(j):
        ch, m = j // 3, lax.rem(j, 3)
        r = slot_rows(slot_of(ch, m))
        y = y_ref[r, :].astype(F32) + norm_rows(att[r, :].astype(F32), gain(1))
        y = y.astype(BF16)
        y_ref[r, :] = y
        c_ref[ch, own_rows(m), :] = c_of(y)

    def up(ch, g_tile, u_tile):
        gate = jnp.dot(c_ref[ch], g_tile[...], preferred_element_type=F32)
        val = jnp.dot(c_ref[ch], u_tile[...], preferred_element_type=F32)
        return (jax.nn.gelu(gate, approximate=True) * val).astype(BF16)

    def mlp(ch, after_first):
        base = ch * n_f
        act[0] = up(ch, g_ring.get(base), u_ring.get(base))
        acc[...] = jnp.zeros(acc.shape, F32)
        g_ring.free(base)
        u_ring.free(base)
        after_first(ch)

        @pl.loop(1, n_f)
        def _(t):
            new = lax.rem(t, 2)
            g_tile, u_tile, d_tile = g_ring.get(base + t), u_ring.get(base + t), d_ring.get(base + t - 1)
            acc[...] += jnp.dot(act[1 - new], d_tile[...], preferred_element_type=F32)
            act[new] = up(ch, g_tile, u_tile)
            g_ring.free(base + t)
            u_ring.free(base + t)
            d_ring.free(base + t - 1)

        t = base + n_f - 1
        acc[...] += jnp.dot(act[(n_f - 1) % 2], d_ring.get(t)[...], preferred_element_type=F32)
        d_ring.free(t)

    def result(m, y):
        val = acc[own_rows(m), :].astype(BF16).astype(F32)
        return (y.astype(F32) + norm_rows(val, gain(3))).astype(BF16)

    if last:
        me = lax.axis_index("cp")

        def sent(ch, m):
            b, blk = place_of(ch, m)
            src = y_at(ch, m)
            if ch == 0:
                far = lambda: remote(src, out_ref.at[b], osend.at[m], orecv.at[b], blk)
                return blk, far, lambda: local(src, out_ref.at[b], orecv.at[b])
            return blk, lambda: remote(src, ybuf.at[b // 2], ysend.at[m], yrecv.at[b // 2], blk), None

        def owned(ch, m):
            turn = (me // 2) % 2
            b = 2 * m + (turn if ch == 0 else 1 - turn)
            return b, home_of(b, me)[0]

        def send_streams():
            wait_group(n_dev)
            for m in range(3):
                dev, far, _ = sent(1, m)

                @pl.when(dev != me)
                def _():
                    far().start()

        def send_results():
            for m in range(3):
                dev, far, near = sent(0, m)

                @pl.when(dev != me)
                def _():
                    far().start()

                @pl.when(dev == me)
                def _():
                    near().start()

        def after_first(ch):
            pl.when(ch == 0)(send_streams)
            pl.when(ch == 1)(send_results)

        @pl.loop(0, 2)
        def _(ch):
            mlp(ch, after_first)

            @pl.when(ch == 0)
            def _():
                @pl.loop(0, 3)
                def _(m):
                    y_at(0, m)[...] = result(m, y_at(0, m)[...])

                for m in range(3):
                    _, dev = owned(1, m)

                    @pl.when(dev != me)
                    def _():
                        remote(ybuf.at[m], ybuf.at[m], ysend.at[m], yrecv.at[m], me).wait_recv()

                for m in range(3):
                    b, blk = place_of(1, m)

                    @pl.when(blk == me)
                    def _():
                        ybuf[b // 2] = y_at(1, m)[...]

                @pl.loop(0, 3)
                def _(m):
                    c_ref[1, own_rows(m), :] = c_of(ybuf[m])

        @pl.loop(0, 3)
        def _(m):
            ybuf[m] = result(m, ybuf[m])

        for m in range(3):
            b, _ = owned(1, m)
            local(ybuf.at[m], out_ref.at[b], orecv.at[b]).start()
        for ch in range(2):
            for m in range(3):
                dev, far, _ = sent(ch, m)

                @pl.when(dev != me)
                def _():
                    far().wait_send()

        for b in range(6):
            local(out_ref.at[b], out_ref.at[b], orecv.at[b]).wait()
        return

    def source(t, put):
        kind = lax.rem(t, 2 * nk) if not isinstance(t, int) else t % (2 * nk)
        cases = (
            (jnp.logical_and(t < 4 * nk, kind < nk), lambda: put(wk_ref.at[layer + 1, :, cols(kind, hd)])),
            (jnp.logical_and(t < 4 * nk, kind >= nk), lambda: put(wv_ref.at[layer + 1, :, cols(kind - nk, hd)])),
            (t >= 4 * nk, lambda: put(wq_ref.at[layer + 1, :, cols(t - 4 * nk, hd)])),
        )
        for cond, do in cases:
            pl.when(cond)(do)

    n_ring = Ring(wn, nsem, 4 * nk + nq, source)
    n_ring.begin()
    k_gain, q_gain = (qk_ref[layer + 1, j : j + 1, :].astype(F32) for j in (1, 0))

    trig = Trig(trig_ref, layer + 1, rows)

    @pl.loop(0, 6)
    def _(j):
        ch, m = j // 3, lax.rem(j, 3)
        tbuf[ch, m, 0], tbuf[ch, m, 1] = trig.of(place_of(ch, m)[1])

    def turn(ch, m):
        return tbuf[ch, m, 0], tbuf[ch, m, 1]

    def send_keys(ch):
        for m in range(3):
            keys.start(slot_of(ch, m), (kst.at[ch, m], vst.at[ch, m]))

    def keys_and_values(ch):
        @pl.loop(0, 3)
        def _(m):
            h = result(m, y_at(ch, m)[...])
            y_at(ch, m)[...] = h
            c_ref[ch, own_rows(m), :] = norm_rows(h.astype(F32), gain(0, layer + 1)).astype(BF16)

        @pl.loop(0, nk)
        def _(h):
            t = ch * 2 * nk + h
            raw = jnp.dot(c_ref[ch], n_ring.get(t)[...], preferred_element_type=F32)
            n_ring.free(t)
            for m in range(3):
                kst[ch, m, :, cols(h, hd)] = norm_turn(raw[m * rows : (m + 1) * rows], k_gain, *turn(ch, m))

        @pl.loop(0, nk)
        def _(h):
            t = (ch * 2 + 1) * nk + h
            raw = jnp.dot(c_ref[ch], n_ring.get(t)[...], preferred_element_type=F32)
            n_ring.free(t)
            for m in range(3):
                vst[ch, m, :, cols(h, hd)] = raw[m * rows : (m + 1) * rows].astype(BF16)

        for m in range(3):
            s = slot_of(ch, m)
            local(y_at(ch, m), h_ref.at[s], hsem.at[s]).start()

    def query(h):
        t = 4 * nk + h
        tile = n_ring.get(t)
        for ch in range(2):
            raw = jnp.dot(c_ref[ch], tile[...], preferred_element_type=F32)
            for m in range(3):
                out = norm_turn(raw[m * rows : (m + 1) * rows], q_gain, *turn(ch, m))
                qst[ch, m, :, cols(h, hd)] = out * BF16(hd**-0.5)
        n_ring.free(t)

    def first_keys():
        wait_group(n_dev)
        send_keys(0)

    @pl.loop(0, 2)
    def _(ch):
        mlp(ch, lambda ch: pl.when(ch == 1)(first_keys))
        keys_and_values(ch)

    query(0)
    send_keys(1)
    pl.loop(1, nq)(query)
    for ch in range(2):
        for m in range(3):
            s = slot_of(ch, m)
            local(qst.at[ch, m], q_ref.at[s], qsem.at[s]).start()
    for ch in range(2):
        for m in range(3):
            s = slot_of(ch, m)
            keys.wait_sent(s, (kst.at[ch, m], vst.at[ch, m]))
            local(qst.at[ch, m], q_ref.at[s], qsem.at[s]).wait()
            local(y_at(ch, m), h_ref.at[s], hsem.at[s]).wait()
    keys.wait_mate(6)
    keys.wait_special()


def after_attention(layer, last, n_dev, cid, o, x, ln_w, w_o, w_gate, w_up, w_down, more=()):
    slots, rows, dim = x.shape
    inner, ff = w_o.shape[1], w_gate.shape[-1]
    total = slots * rows
    half = total // 2
    blocks = 16
    tn, tf = min(256, dim), min(512, ff)
    deep = 3
    o2, x2 = o.reshape(total, inner), x.reshape(total, dim)
    work = [
        pltpu.VMEM((total, inner), BF16), pltpu.VMEM((total, dim), BF16),
        pltpu.VMEM((total, dim), BF16), pltpu.VMEM((2, half, dim), BF16),
        pltpu.VMEM((half, dim), F32), pltpu.VMEM((2, half, tf), BF16),
        pltpu.VMEM((deep, inner, tn), BF16), pltpu.VMEM((deep, dim, tf), BF16), pltpu.VMEM((deep, dim, tf), BF16),
        pltpu.VMEM((deep, tf, dim), BF16),
        DMA((2,)), DMA((deep,)), DMA((deep,)), DMA((deep,)), DMA((deep,)),
    ]
    params = pltpu.CompilerParams(collective_id=cid, has_side_effects=True, vmem_limit_bytes=VMEM_LIMIT)
    body = functools.partial(layer_kernel, layer, last, n_dev)
    if last:
        return pl.pallas_call(
            body,
            in_specs=[ANY, ANY, WHOLE] + [ANY] * 4,
            out_specs=ANY,
            out_shape=jax.ShapeDtypeStruct(x.shape, BF16),
            scratch_shapes=work + [pltpu.VMEM((3, rows, dim), BF16), DMA((3,)), DMA((3,)), DMA((3,)), DMA((slots,))],
            compiler_params=params,
        )(o2, x2, ln_w, w_o, w_gate, w_up, w_down)
    qk_w, trig, w_q, w_k, w_v = more
    hd = qk_w.shape[-1]
    nq, nk = w_q.shape[-1] // hd, w_k.shape[-1] // hd
    q_shape, kv_shape = (slots, rows, nq * hd), (blocks, rows, nk * hd)
    return pl.pallas_call(
        body,
        in_specs=[ANY, ANY, WHOLE, WHOLE, WHOLE] + [ANY] * 7,
        out_specs=[ANY] * 4,
        out_shape=[jax.ShapeDtypeStruct(a, BF16) for a in (x.shape, q_shape, kv_shape, kv_shape)],
        scratch_shapes=work + [
            pltpu.VMEM((deep, dim, hd), BF16), DMA((deep,)),
            pltpu.VMEM((2, 3, rows, nq * hd), BF16), pltpu.VMEM((2, 3, rows, nk * hd), BF16), pltpu.VMEM((2, 3, rows, nk * hd), BF16),
            pltpu.VMEM((2, 3, 2, rows, hd // 2), F32),
            DMA((slots,)), DMA((slots,)), DMA((2, 3, slots)), DMA((2, blocks)), DMA((2, 2)),
        ],
        compiler_params=params,
    )(o2, x2, ln_w, qk_w, trig, w_o, w_gate, w_up, w_down, w_k, w_v, w_q)


def rope_table(rows, blocks, hd):
    half = hd // 2
    pos = jnp.concatenate([jnp.arange(rows), rows * jnp.arange(blocks)]).astype(F32)
    out = []
    for base, scale in ((LOCAL_BASE, 1.0), (GLOBAL_BASE, GLOBAL_SCALE)):
        freq = base ** (-2.0 * jnp.arange(half, dtype=F32) / hd)
        ang = (pos / scale)[:, None] * freq[None, :]
        out.append(jnp.stack([jnp.cos(ang), jnp.sin(ang)]))
    return jnp.stack(out)


def solution(mesh):
    n_dev = mesh.shape["cp"]

    def device_fn(x_loc, ln_w, qk_w, w_q, w_k, w_v, w_o, w_gate, w_up, w_down):
        rows, hd = x_loc.shape[1], qk_w.shape[-1]
        trig = rope_table(rows, n_dev, hd)
        x, o = first(n_dev, WINDOW, x_loc, ln_w, qk_w, trig, w_q, w_k, w_v)
        mlp = (w_o, w_gate, w_up, w_down)
        x, q, k, v = after_attention(0, False, n_dev, 1, o, x, ln_w, *mlp, more=(qk_w, trig, w_q, w_k, w_v))
        o = attention(None, hd, q, k, v)
        return after_attention(1, True, n_dev, 2, o, x, ln_w, *mlp)

    act_part = P("dp", "cp", None)
    return jax.shard_map(device_fn, mesh=mesh, in_specs=(act_part,) + (P(),) * 9, out_specs=act_part, check_vma=False)
```

```python
import functools

import jax
import jax.numpy as jnp
from jax import lax
from jax.experimental import pallas as pl
from jax.experimental.pallas import tpu as pltpu
from jax.sharding import PartitionSpec as P

WINDOW = 1024
NORM_EPS = 1e-6
LOCAL_BASE = 10000.0
GLOBAL_BASE = 1000000.0
GLOBAL_SCALE = 8.0
NEG = -1e30

ROW_CHIP = (0, 3, 4, 1, 5, 6)
SPECIAL = (2, 7)
VMEM_LIMIT = 64 * 1024 * 1024 - 128 * 1024
MESH = pl.DeviceIdType.MESH
BF16, F32 = jnp.bfloat16, jnp.float32
ANY = pl.BlockSpec(memory_space=pl.ANY)
WHOLE = pl.BlockSpec(memory_space=pltpu.VMEM)
DMA = pltpu.SemaphoreType.DMA


def pick(idx, table):
    out = jnp.int32(table[-1])
    for i in range(len(table) - 2, -1, -1):
        out = jnp.where(idx == i, jnp.int32(table[i]), out)
    return out


def placement():
    me = lax.axis_index("cp")
    chip, core = me // 2, me % 2
    roles = [0] * 8
    rows = [0] * 8
    for b, c in enumerate(ROW_CHIP):
        rows[c] = b
    for i, c in enumerate(SPECIAL):
        roles[c] = 1
        rows[c] = 3 * i
    return me, chip, core, pick(chip, roles), pick(chip, rows)


def slot_place(s, core, special, row):
    k = s % 2
    blk = jnp.where(special == 1, 2 * k + (k + core) % 2, 4 + 2 * s + (s + core) % 2)
    b = jnp.where(special == 1, row + s // 2, row)
    return b, blk


EARLY_ORDER = (2, 5, 1, 4, 0, 3)


def arrival():
    out = []
    for dev in range(16):
        chip, core = dev // 2, dev % 2
        if chip in SPECIAL:
            out += [4, 5, 2, 3, 0, 1]
            continue
        b = ROW_CHIP.index(chip)
        for step in range(6):
            out += [(j - 4) // 2 for j in range(4, 16) if (j + step) % 6 == b and (j + 1) // 2 % 2 == core]
    return out


def home_of(b, blk):
    core = ((blk + 1) // 2) % 2
    half = blk // 2
    chip = jnp.where(blk < 4, pick(b // 3, SPECIAL), pick(b, ROW_CHIP))
    slot = jnp.where(blk < 4, (b % 3) * 2 + half, half - 2)
    return chip * 2 + core, slot


def chunk_slot(ch, i, special, row):
    b = jnp.where(special == 1, row + i, row)
    return 2 * i + (b + ch) % 2


def kv_index(s, core, special, row):
    _, blk = slot_place(s, core, special, row)
    return jnp.where(special == 1, (s // 2) * 4 + blk, blk)


def served(row, r):
    return jnp.where(row == 0, ROW_CHIP[r], ROW_CHIP[r + 3])


def signal_group(n_dev):
    me = lax.axis_index("cp")
    barrier = pltpu.get_barrier_semaphore()
    for d in range(1, n_dev):
        pl.semaphore_signal(barrier, inc=1, device_id={"cp": lax.rem(me + d, n_dev)}, device_id_type=MESH)


def wait_group(n_dev):
    pl.semaphore_wait(pltpu.get_barrier_semaphore(), n_dev - 1)


def remote(src, dst, send, recv, dev):
    return pltpu.make_async_remote_copy(
        src_ref=src, dst_ref=dst, send_sem=send, recv_sem=recv, device_id={"cp": dev}, device_id_type=MESH
    )


def local(src, dst, sem):
    return pltpu.make_async_copy(src, dst, sem)


def norm_rows(vals, gain):
    inv = lax.rsqrt(jnp.mean(vals * vals, axis=-1, keepdims=True) + NORM_EPS)
    return vals * inv * (1.0 + gain)


def norm_turn(raw, gain, cos, sin):
    half = raw.shape[-1] // 2
    vals = norm_rows(raw.astype(BF16).astype(F32), gain)
    first, second = vals[:, :half], vals[:, half:]
    return jnp.concatenate([first * cos - second * sin, second * cos + first * sin], axis=-1).astype(BF16)


class KeyValues:
    def __init__(self, k_all, v_all, send, recv, fwd, in_place=False):
        self.in_place = in_place
        self.both = ((0, k_all), (1, v_all))
        self.send, self.recv, self.fwd = send, recv, fwd

    def here(self):
        _, chip, self.core, self.special, self.row = placement()
        self.mate = chip * 2 + 1 - self.core

    def _copies(self, s, stage):
        idx = kv_index(s, self.core, self.special, self.row)
        _, blk = slot_place(s, self.core, self.special, self.row)
        dev = served(self.row, 0) * 2 + self.core
        for r in (1, 2):
            dev = jnp.where(s // 2 == r, served(self.row, r) * 2 + self.core, dev)
        out = []
        for x, full in self.both:
            src = full.at[idx] if self.in_place else stage[x]
            out.append((
                None if self.in_place else local(src, full.at[idx], self.send.at[x, 0, s]),
                remote(src, full.at[idx], self.send.at[x, 1, s], self.recv.at[x, idx], self.mate),
                remote(src, full.at[blk], self.send.at[x, 2, s], self.recv.at[x, blk], dev),
            ))
        return out

    def start(self, s, stage, rows_too=True):
        self.here()
        for own, mate, row in self._copies(s, stage):

            @pl.when((self.special == 1) & rows_too)
            def _():
                row.start()

            mate.start()
            if own is not None:
                own.start()

    def start_rows(self, s):
        self.here()

        @pl.when(self.special == 1)
        def _():
            for _, _, row in self._copies(s, None):
                row.start()

    def wait_sent(self, s, stage):
        self.here()
        for own, mate, row in self._copies(s, stage):
            if own is not None:
                own.wait()
            mate.wait_send()

            @pl.when(self.special == 1)
            def _():
                row.wait_send()

    def wait_mate(self, slots):
        self.here()
        for x, full in self.both:
            for s in range(slots):
                idx = kv_index(s, 1 - self.core, self.special, self.row)
                remote(full.at[idx], full.at[idx], self.fwd.at[x, 0], self.recv.at[x, idx], self.mate).wait_recv()

    def wait_special(self):
        self.here()

        @pl.when(self.special == 0)
        def _():
            for k in range(2):
                blk = 2 * k + (k + self.core) % 2
                for x, full in self.both:
                    remote(full.at[blk], full.at[blk], self.fwd.at[x, k], self.recv.at[x, blk], self.mate).wait_recv()
                    remote(full.at[blk], full.at[blk], self.fwd.at[x, k], self.recv.at[x, blk], self.mate).start()
            for x, full in self.both:
                for k in range(2):
                    blk = 2 * k + (k + 1 - self.core) % 2
                    remote(full.at[blk], full.at[blk], self.fwd.at[x, k], self.recv.at[x, blk], self.mate).wait()


class Trig:
    def __init__(self, ref, layer, rows):
        self.ref, self.layer, self.rows = ref, layer, rows

    def of(self, blk):
        cu, su = (self.ref[self.layer, j, : self.rows, :] for j in range(2))
        cb, sb = (self.ref[self.layer, j, pl.ds(self.rows + blk, 1), :] for j in range(2))
        return cu * cb - su * sb, su * cb + cu * sb


class Attention:
    per, lanes = 4, 128

    def __init__(self, window_blocks, hd, qbuf, kbuf, vbuf, sbuf, wacc, wm, wl, bias, o_ref, osem):
        self.window_blocks, self.hd = window_blocks, hd
        self.qbuf, self.kbuf, self.vbuf, self.sbuf, self.bias = qbuf, kbuf, vbuf, sbuf, bias
        self.wacc, self.wm, self.wl, self.o_ref, self.osem = wacc, wm, wl, o_ref, osem
        self.slots, self.rows = qbuf.shape[:2]
        self.nk = kbuf.shape[-1] // hd
        self.rep = qbuf.shape[-1] // kbuf.shape[-1]
        self.tile = self.per * self.rows
        self.group = wacc.shape[1] // (self.rep * self.rows)

    def fill_bias(self):
        rows, tile, bias = self.rows, self.tile, self.bias
        qi = lax.broadcasted_iota(jnp.int32, (rows, tile), 0)
        ki = lax.broadcasted_iota(jnp.int32, (rows, tile), 1)
        bias[0] = jnp.zeros((rows, tile), F32)
        for j in range(self.per):
            bias[1 + j] = jnp.where(ki <= qi + j * rows, 0.0, NEG)
            if self.window_blocks is not None:
                bias[1 + self.per + j] = jnp.where(ki > qi + j * rows, 0.0, NEG)

    def start_tile(self, blk):
        if self.window_blocks is None:
            return jnp.int32(0)
        return jnp.maximum(blk - self.window_blocks, 0) // self.per

    def part(self, buf, t, base, g):
        block = buf.at[pl.ds(base + self.per * t, self.per)]
        return block[:, :, g * self.hd : (g + 1) * self.hd].reshape(self.tile, self.hd)

    def edge(self, t, blk):
        per = self.per
        out = jnp.where(t == blk // per, 1 + blk % per, 0)
        if self.window_blocks is not None:
            old = blk - self.window_blocks
            out = jnp.where((old >= 0) & (t == old // per), 1 + per + old % per, out)
        return out

    def scores(self, s, t, base, blks):
        rows, rep, hd, group = self.rows, self.rep, self.hd, self.group
        offs = [self.bias[self.edge(t, blk)][None] for blk in blks]
        out = []
        for g in range(self.nk):
            heads = [self.qbuf[s + j, :, h * hd : (h + 1) * hd] for j in range(group) for h in range(g * rep, (g + 1) * rep)]
            q = jnp.concatenate(heads, axis=0)
            sc = lax.dot_general(q, self.part(self.kbuf, t, base, g), (((1,), (1,)), ((), ())), preferred_element_type=F32)
            sc = sc.reshape(group, rep, rows, self.tile)
            sc = jnp.concatenate([sc[j] + offs[j] for j in range(group)], axis=0)
            out.append(sc.reshape(group * rep * rows, self.tile))
        return out

    def columns(self, val, op):
        return functools.reduce(op, [val[:, j * self.lanes : (j + 1) * self.lanes] for j in range(self.tile // self.lanes)])

    def spread(self, val):
        return jnp.concatenate([val] * (self.tile // self.lanes), axis=1)

    def row_max(self, val):
        return jnp.broadcast_to(jnp.max(val, axis=-1, keepdims=True), val.shape)

    def passes(self, s, blks, base, first, last):
        for g in range(self.nk):
            self.wm[g] = jnp.full(self.wm.shape[1:], NEG, F32)
            self.wl[g] = jnp.zeros(self.wl.shape[1:], F32)
            self.wacc[g] = jnp.zeros(self.wacc.shape[1:], F32)

        @pl.loop(first, last)
        def _(t):
            for g, sc in enumerate(self.scores(s, t, base, blks)):
                self.sbuf[g, t - first] = sc
                self.wm[g] = jnp.maximum(self.wm[g], self.columns(sc, jnp.maximum))

        for g in range(self.nk):
            self.wm[g] = self.row_max(self.wm[g])

        @pl.loop(first, last)
        def _(t):
            for g in range(self.nk):
                p = jnp.exp(self.sbuf[g, t - first] - self.spread(self.wm[g]))
                self.wl[g] += self.columns(p, jnp.add)
                self.wacc[g] += jnp.dot(p.astype(BF16), self.part(self.vbuf, t, base, g), preferred_element_type=F32)

    def merge(self, s, blk, old, old_sum, old_acc):
        for g, sc in enumerate(self.scores(s, 0, 0, [blk])):
            new = self.row_max(jnp.maximum(old[g], self.columns(sc, jnp.maximum)))
            p = jnp.exp(sc - self.spread(new))
            alpha = jnp.exp(old[g] - new)
            self.wl[g] = alpha * old_sum[g] + self.columns(p, jnp.add)
            part = jnp.dot(p.astype(BF16), self.part(self.vbuf, 0, 0, g), preferred_element_type=F32)
            self.wacc[g] = jnp.concatenate([alpha] * (self.hd // self.lanes), axis=1) * old_acc[g] + part

    def finish(self, s):
        for g in range(self.nk):
            out = (self.wacc[g] / jnp.sum(self.wl[g], axis=-1, keepdims=True)).astype(BF16)
            for j in range(self.group):
                for h in range(self.rep):
                    lo, r = (g * self.rep + h) * self.hd, (j * self.rep + h) * self.rows
                    self.qbuf[s + j, :, lo : lo + self.hd] = out[r : r + self.rows]
        for j in range(self.group):
            local(self.qbuf.at[s + j], self.o_ref.at[s + j], self.osem.at[s + j]).start()

    def wait_out(self):
        for s in range(self.slots):
            local(self.qbuf.at[s], self.o_ref.at[s], self.osem.at[s]).wait()


def first_kernel(n_dev, window_blocks, x_ref, ln_ref, qk_ref, trig_ref, wq_ref, wk_ref, wv_ref,
                 h_ref, o_ref, xbuf, abuf, wq, wk, wv, qbuf, kbuf, vbuf, sbuf, wacc, wm, wl, bias, mx, sm, acc,
                 wsem, xsend, xrecv, hsem, osem, ksend, krecv, fsem):
    me, chip, core, special, row = placement()
    n, rows, dim = x_ref.shape
    hd = qk_ref.shape[-1]
    nq, nk = wq.shape[-1] // hd, wk.shape[-1] // hd
    homes = [home_of(jnp.int32(b), me) for b in range(n)]
    keys = KeyValues(kbuf, vbuf, ksend, krecv, fsem, in_place=True)
    att = Attention(window_blocks, hd, qbuf, kbuf, vbuf, sbuf, wacc, wm, wl, bias, o_ref, osem)

    signal_group(n_dev)
    for b, (dev, slot) in enumerate(homes):

        @pl.when(dev == me)
        def _():
            local(x_ref.at[b], xbuf.at[slot], xrecv.at[slot]).start()

    for j, (src, dst) in enumerate(((wk_ref, wk), (wv_ref, wv), (wq_ref, wq))):
        start_parts(src.at[0], dst, wsem.at[j])
    wait_group(n_dev)
    for step in range(n):
        b = jnp.where(me < 4, EARLY_ORDER[step], lax.rem(me + step, n))
        dev, slot = home_of(b, me)

        @pl.when(dev != me)
        def _():
            remote(x_ref.at[b], xbuf.at[slot], xsend.at[b], xrecv.at[slot], dev).start()

    att.fill_bias()
    trig = Trig(trig_ref, 0, rows)
    gain = ln_ref[0, 0:1, :].astype(F32)
    k_gain = qk_ref[0, 1:2, :].astype(F32)
    q_gain = qk_ref[0, 0:1, :].astype(F32)
    for j, (src, dst) in enumerate(((wk_ref, wk), (wv_ref, wv), (wq_ref, wq))):
        local(src.at[0], dst, wsem.at[j]).wait()
    order = arrival()

    def col(h):
        return pl.ds(h * hd if isinstance(h, int) else pl.multiple_of(h * hd, hd), hd)

    def product(w, h):
        return jnp.dot(abuf[...], w[:, col(h)], preferred_element_type=F32)

    @pl.loop(0, n // 2)
    def _(pair):
        places = [pick(me * n + 2 * pair + j, order) for j in range(2)]
        turn, idx = [], []
        for j, s in enumerate(places):
            local(xbuf.at[s], xbuf.at[s], xrecv.at[s]).wait()
            local(xbuf.at[s], h_ref.at[s], hsem.at[s]).start()
            abuf[j * rows : (j + 1) * rows, :] = norm_rows(xbuf[s].astype(F32), gain).astype(BF16)
            turn.append(trig.of(slot_place(s, core, special, row)[1]))
            idx.append(kv_index(s, core, special, row))

        @pl.loop(0, nk)
        def _(h):
            k_raw, v_raw = product(wk, h), product(wv, h)
            for j in range(2):
                part = slice(j * rows, (j + 1) * rows)
                kbuf[idx[j], :, col(h)] = norm_turn(k_raw[part], k_gain, *turn[j])
                vbuf[idx[j], :, col(h)] = v_raw[part].astype(BF16)

        def query(h):
            raw = product(wq, h)
            for j, s in enumerate(places):
                part = slice(j * rows, (j + 1) * rows)
                qbuf[s, :, col(h)] = norm_turn(raw[part], q_gain, *turn[j]) * BF16(hd**-0.5)

        query(0)
        for s in places:
            keys.start(s, None, pair == 0)
        pl.loop(1, nq)(query)

    for s in (2, 0, 3, 1):
        keys.start_rows(s)
    keys.wait_mate(n)

    @pl.loop(0, n)
    def _(s):
        _, blk = slot_place(s, core, special, row)
        base = jnp.where(special == 1, (s // 2) * att.per, 0)
        att.passes(s, [blk], base, jnp.where(special == 1, 0, jnp.maximum(att.start_tile(blk), 1)), blk // att.per + 1)
        more = (special == 0) & (s < mx.shape[0])

        @pl.when(more)
        def _():
            for g in range(nk):
                mx[s, g] = wm[g]
                sm[s, g] = wl[g]
                acc[s, g] = wacc[g]

        @pl.when(jnp.logical_not(more))
        def _():
            att.finish(s)

    keys.wait_special()

    @pl.when(special == 0)
    def _():
        @pl.loop(0, mx.shape[0])
        def _(s):
            _, blk = slot_place(s, core, special, row)
            att.merge(s, blk, *[[ref[s, g] for g in range(nk)] for ref in (mx, sm, acc)])
            att.finish(s)

    att.wait_out()
    for s in range(n):
        keys.wait_sent(s, None)
        local(xbuf.at[s], h_ref.at[s], hsem.at[s]).wait()
    for b, (dev, slot) in enumerate(homes):

        @pl.when(dev != me)
        def _():
            remote(x_ref.at[b], xbuf.at[slot], xsend.at[b], xrecv.at[slot], dev).wait_send()


def attention_scratch(tiles, group, rows, nq, nk, hd):
    wide = group * nq // nk * rows
    return [
        pltpu.VMEM((nk, tiles, wide, 4 * rows), F32),
        pltpu.VMEM((nk, wide, hd), F32), pltpu.VMEM((nk, wide, 128), F32), pltpu.VMEM((nk, wide, 128), F32),
        pltpu.VMEM((9, rows, 4 * rows), F32),
    ]


def first(n_dev, window, x, ln_w, qk_w, trig, w_q, w_k, w_v):
    n, rows, dim = x.shape
    hd = qk_w.shape[-1]
    nq, nk = w_q.shape[-1] // hd, w_k.shape[-1] // hd
    blocks, late, wide = 16, 4, nq // nk * rows
    q_shape, kv_shape = (n, rows, nq * hd), (blocks, rows, nk * hd)
    return pl.pallas_call(
        functools.partial(first_kernel, n_dev, window // rows),
        out_shape=[jax.ShapeDtypeStruct(a, BF16) for a in (x.shape, q_shape)],
        in_specs=[ANY, WHOLE, WHOLE, WHOLE, ANY, ANY, ANY],
        out_specs=[ANY] * 2,
        scratch_shapes=[
            pltpu.VMEM(x.shape, BF16), pltpu.VMEM((2 * rows, dim), BF16),
            pltpu.VMEM(w_q.shape[1:], BF16), pltpu.VMEM(w_k.shape[1:], BF16), pltpu.VMEM(w_v.shape[1:], BF16),
            pltpu.VMEM(q_shape, BF16), pltpu.VMEM(kv_shape, BF16), pltpu.VMEM(kv_shape, BF16),
            *attention_scratch(3, 1, rows, nq, nk, hd),
            pltpu.VMEM((late, nk, wide, 128), F32), pltpu.VMEM((late, nk, wide, 128), F32), pltpu.VMEM((late, nk, wide, hd), F32),
            DMA((3,)), DMA((n,)), DMA((n,)), DMA((n,)), DMA((n,)), DMA((2, 3, n)), DMA((2, blocks)), DMA((2, 2)),
        ],
        compiler_params=pltpu.CompilerParams(collective_id=0, has_side_effects=True, vmem_limit_bytes=VMEM_LIMIT),
    )(x, ln_w, qk_w, trig, w_q, w_k, w_v)


def attn_kernel(window_blocks, hd, q_ref, k_ref, v_ref, o_ref, kbuf, vbuf, qbuf, sbuf, wacc, wm, wl, bias, qsem, ksem, osem):
    _, _, core, special, row = placement()
    att = Attention(window_blocks, hd, qbuf, kbuf, vbuf, sbuf, wacc, wm, wl, bias, o_ref, osem)
    per = att.per
    tiles = k_ref.shape[0] // per

    def loads(t):
        part = pl.ds(t * per, per)
        return [local(k_ref.at[part], kbuf.at[part], ksem.at[0, t]), local(v_ref.at[part], vbuf.at[part], ksem.at[1, t])]

    for s in range(att.slots):
        local(q_ref.at[s], qbuf.at[s], qsem.at[s]).start()
    for t in range(tiles):
        for c in loads(t):
            c.start()
    att.fill_bias()
    group = att.group

    @pl.loop(0, att.slots // group)
    def _(i):
        for t in range(tiles):

            @pl.when(i == max(t - 1, 0))
            def _():
                for c in loads(t):
                    c.wait()

        s = i * group
        blks = [slot_place(s + j, core, special, row)[1] for j in range(group)]
        for j in range(group):
            local(q_ref.at[s + j], qbuf.at[s + j], qsem.at[s + j]).wait()
        base = jnp.where(special == 1, i * per, 0)
        att.passes(s, blks, base, att.start_tile(blks[0]), blks[0] // per + 1)
        att.finish(s)

    att.wait_out()


def attention(window, hd, q, k, v):
    slots, rows = q.shape[:2]
    blocks = k.shape[0]
    nq, nk = q.shape[-1] // hd, k.shape[-1] // hd
    return pl.pallas_call(
        functools.partial(attn_kernel, None if window is None else window // rows, hd),
        out_shape=jax.ShapeDtypeStruct(q.shape, BF16),
        in_specs=[ANY] * 3,
        out_specs=ANY,
        scratch_shapes=[
            pltpu.VMEM(k.shape, BF16), pltpu.VMEM(v.shape, BF16), pltpu.VMEM(q.shape, BF16),
            *attention_scratch(blocks // 4, 2, rows, nq, nk, hd),
            DMA((slots,)), DMA((2, blocks // 4)), DMA((slots,)),
        ],
        compiler_params=pltpu.CompilerParams(vmem_limit_bytes=VMEM_LIMIT),
    )(q, k, v)


def start_parts(src, dst, sem, parts=4):
    n = src.shape[0]
    if n % (parts * 16):
        local(src, dst, sem).start()
        return
    for j in range(parts):
        part = pl.ds(j * (n // parts), n // parts)
        local(src.at[part], dst.at[part], sem).start()


class Ring:
    def __init__(self, buf, sem, count, source):
        self.buf, self.sem, self.count, self.source = buf, sem, count, source
        self.depth = buf.shape[0]

    def begin(self):
        for t in range(min(self.depth, self.count)):
            self.start(t, t)

    def start(self, t, slot):
        def put(ref):
            start_parts(ref, self.buf.at[slot], self.sem.at[slot])

        self.source(t, put)

    def get(self, t):
        slot = lax.rem(t, self.depth) if not isinstance(t, int) else t % self.depth
        local(self.buf.at[slot], self.buf.at[slot], self.sem.at[slot]).wait()
        return self.buf.at[slot]

    def free(self, t):
        new = t + self.depth
        if isinstance(t, int):
            if new < self.count:
                self.start(new, t % self.depth)
            return

        @pl.when(new < self.count)
        def _():
            self.start(new, lax.rem(t, self.depth))


def layer_kernel(layer, last, n_dev, *refs):
    if last:
        (o_ref, x_ref, ln_ref, wo_ref, wg_ref, wu_ref, wd_ref, out_ref,
         obuf, y_ref, att, c_ref, acc, act, wo, wg, wu, wd, isem, osem, gsem, usem, dsem,
         ybuf, ysend, yrecv, osend, orecv) = refs
    else:
        (o_ref, x_ref, ln_ref, qk_ref, trig_ref, wo_ref, wg_ref, wu_ref, wd_ref, wk_ref, wv_ref, wq_ref,
         h_ref, q_ref, k_all, v_all,
         obuf, y_ref, att, c_ref, acc, act, wo, wg, wu, wd, isem, osem, gsem, usem, dsem,
         wn, nsem, qst, kst, vst, tbuf, hsem, qsem, ksend, krecv, fsem) = refs
        keys = KeyValues(k_all, v_all, ksend, krecv, fsem)
        hd = qk_ref.shape[-1]
        nk, nq = wk_ref.shape[-1] // hd, wq_ref.shape[-1] // hd
    rows = acc.shape[0] // 3
    tn, tf = wo.shape[-1], wg.shape[-1]
    n_o, n_f = wo_ref.shape[-1] // tn, wg_ref.shape[-1] // tf

    def cols(t, width):
        start = t * width
        return pl.ds(start if isinstance(t, int) else pl.multiple_of(start, width), width)

    def tile_f(t):
        return (t % n_f) if isinstance(t, int) else lax.rem(t, n_f)

    o_ring = Ring(wo, osem, n_o, lambda t, put: put(wo_ref.at[layer, :, cols(t, tn)]))
    g_ring = Ring(wg, gsem, 2 * n_f, lambda t, put: put(wg_ref.at[layer, :, cols(tile_f(t), tf)]))
    u_ring = Ring(wu, usem, 2 * n_f, lambda t, put: put(wu_ref.at[layer, :, cols(tile_f(t), tf)]))
    d_ring = Ring(wd, dsem, 2 * n_f, lambda t, put: put(wd_ref.at[layer, cols(tile_f(t), tf), :]))

    in_o = local(o_ref, obuf, isem.at[0])
    in_x = local(x_ref, y_ref, isem.at[1])
    start_parts(o_ref, obuf, isem.at[0], 6)
    o_ring.begin()
    start_parts(x_ref, y_ref, isem.at[1], 6)
    for r in (g_ring, u_ring, d_ring):
        r.begin()
    signal_group(n_dev)

    def slot_of(ch, m):
        _, _, _, special, row = placement()
        return chunk_slot(ch, m, special, row)

    def place_of(ch, m):
        _, _, core, special, row = placement()
        return slot_place(chunk_slot(ch, m, special, row), core, special, row)

    def slot_rows(s):
        return pl.ds(pl.multiple_of(s * rows, rows), rows)

    def own_rows(m):
        return pl.ds(m * rows if isinstance(m, int) else pl.multiple_of(m * rows, rows), rows)

    def y_at(ch, m):
        return y_ref.at[slot_rows(slot_of(ch, m))]

    def gain(which, l=layer):
        return ln_ref[l, which : which + 1, :].astype(F32)

    def c_of(y):
        return norm_rows(y.astype(F32), gain(2)).astype(BF16)

    in_o.wait()

    @pl.loop(0, n_o)
    def _(t):
        tile = o_ring.get(t)
        att[:, cols(t, tn)] = jnp.dot(obuf[...], tile[...], preferred_element_type=F32).astype(BF16)
        o_ring.free(t)

    in_x.wait()

    @pl.loop(0, 6)
    def _(j):
        ch, m = j // 3, lax.rem(j, 3)
        r = slot_rows(slot_of(ch, m))
        y = y_ref[r, :].astype(F32) + norm_rows(att[r, :].astype(F32), gain(1))
        y = y.astype(BF16)
        y_ref[r, :] = y
        c_ref[ch, own_rows(m), :] = c_of(y)

    def up(ch, g_tile, u_tile):
        gate = jnp.dot(c_ref[ch], g_tile[...], preferred_element_type=F32)
        val = jnp.dot(c_ref[ch], u_tile[...], preferred_element_type=F32)
        return (jax.nn.gelu(gate, approximate=True) * val).astype(BF16)

    def mlp(ch, after_first):
        base = ch * n_f
        act[0] = up(ch, g_ring.get(base), u_ring.get(base))
        acc[...] = jnp.zeros(acc.shape, F32)
        g_ring.free(base)
        u_ring.free(base)
        after_first(ch)

        @pl.loop(1, n_f)
        def _(t):
            new = lax.rem(t, 2)
            g_tile, u_tile, d_tile = g_ring.get(base + t), u_ring.get(base + t), d_ring.get(base + t - 1)
            acc[...] += jnp.dot(act[1 - new], d_tile[...], preferred_element_type=F32)
            act[new] = up(ch, g_tile, u_tile)
            g_ring.free(base + t)
            u_ring.free(base + t)
            d_ring.free(base + t - 1)

        t = base + n_f - 1
        acc[...] += jnp.dot(act[(n_f - 1) % 2], d_ring.get(t)[...], preferred_element_type=F32)
        d_ring.free(t)

    def result(m, y):
        val = acc[own_rows(m), :].astype(BF16).astype(F32)
        return (y.astype(F32) + norm_rows(val, gain(3))).astype(BF16)

    if last:
        me = lax.axis_index("cp")

        def sent(ch, m):
            b, blk = place_of(ch, m)
            src = y_at(ch, m)
            if ch == 0:
                far = lambda: remote(src, out_ref.at[b], osend.at[m], orecv.at[b], blk)
                return blk, far, lambda: local(src, out_ref.at[b], orecv.at[b])
            return blk, lambda: remote(src, ybuf.at[b // 2], ysend.at[m], yrecv.at[b // 2], blk), None

        def owned(ch, m):
            turn = (me // 2) % 2
            b = 2 * m + (turn if ch == 0 else 1 - turn)
            return b, home_of(b, me)[0]

        def send_streams():
            wait_group(n_dev)
            for m in range(3):
                dev, far, _ = sent(1, m)

                @pl.when(dev != me)
                def _():
                    far().start()

        def send_results():
            for m in range(3):
                dev, far, near = sent(0, m)

                @pl.when(dev != me)
                def _():
                    far().start()

                @pl.when(dev == me)
                def _():
                    near().start()

        def after_first(ch):
            pl.when(ch == 0)(send_streams)
            pl.when(ch == 1)(send_results)

        @pl.loop(0, 2)
        def _(ch):
            mlp(ch, after_first)

            @pl.when(ch == 0)
            def _():
                @pl.loop(0, 3)
                def _(m):
                    y_at(0, m)[...] = result(m, y_at(0, m)[...])

                for m in range(3):
                    _, dev = owned(1, m)

                    @pl.when(dev != me)
                    def _():
                        remote(ybuf.at[m], ybuf.at[m], ysend.at[m], yrecv.at[m], me).wait_recv()

                for m in range(3):
                    b, blk = place_of(1, m)

                    @pl.when(blk == me)
                    def _():
                        ybuf[b // 2] = y_at(1, m)[...]

                @pl.loop(0, 3)
                def _(m):
                    c_ref[1, own_rows(m), :] = c_of(ybuf[m])

        @pl.loop(0, 3)
        def _(m):
            ybuf[m] = result(m, ybuf[m])

        for m in range(3):
            b, _ = owned(1, m)
            local(ybuf.at[m], out_ref.at[b], orecv.at[b]).start()
        for ch in range(2):
            for m in range(3):
                dev, far, _ = sent(ch, m)

                @pl.when(dev != me)
                def _():
                    far().wait_send()

        for b in range(6):
            local(out_ref.at[b], out_ref.at[b], orecv.at[b]).wait()
        return

    def source(t, put):
        head = lax.rem(t // 2, nk)
        cases = (
            ((t < 4 * nk) & (t % 2 == 0), lambda: put(wk_ref.at[layer + 1, :, cols(head, hd)])),
            ((t < 4 * nk) & (t % 2 == 1), lambda: put(wv_ref.at[layer + 1, :, cols(head, hd)])),
            (t >= 4 * nk, lambda: put(wq_ref.at[layer + 1, :, cols(t - 4 * nk, hd)])),
        )
        for cond, do in cases:
            pl.when(cond)(do)

    n_ring = Ring(wn, nsem, 4 * nk + nq, source)
    n_ring.begin()
    k_gain, q_gain = (qk_ref[layer + 1, j : j + 1, :].astype(F32) for j in (1, 0))

    trig = Trig(trig_ref, layer + 1, rows)

    @pl.loop(0, 6)
    def _(j):
        ch, m = j // 3, lax.rem(j, 3)
        tbuf[ch, m, 0], tbuf[ch, m, 1] = trig.of(place_of(ch, m)[1])

    def turn(ch, m):
        return tbuf[ch, m, 0], tbuf[ch, m, 1]

    def send_keys(ch):
        for m in range(3):
            keys.start(slot_of(ch, m), (kst.at[ch, m], vst.at[ch, m]))

    def keys_and_values(ch):
        @pl.loop(0, 3)
        def _(m):
            h = result(m, y_at(ch, m)[...])
            y_at(ch, m)[...] = h
            c_ref[ch, own_rows(m), :] = norm_rows(h.astype(F32), gain(0, layer + 1)).astype(BF16)

        @pl.loop(0, nk)
        def _(h):
            t = 2 * (ch * nk + h)
            k_tile, v_tile = n_ring.get(t), n_ring.get(t + 1)
            k_raw = jnp.dot(c_ref[ch], k_tile[...], preferred_element_type=F32)
            v_raw = jnp.dot(c_ref[ch], v_tile[...], preferred_element_type=F32)
            for m in range(3):
                part = slice(m * rows, (m + 1) * rows)
                kst[ch, m, :, cols(h, hd)] = norm_turn(k_raw[part], k_gain, *turn(ch, m))
                vst[ch, m, :, cols(h, hd)] = v_raw[part].astype(BF16)
            n_ring.free(t)
            n_ring.free(t + 1)

        for m in range(3):
            s = slot_of(ch, m)
            local(y_at(ch, m), h_ref.at[s], hsem.at[s]).start()

    def query(h):
        t = 4 * nk + h
        tile = n_ring.get(t)
        for ch in range(2):
            raw = jnp.dot(c_ref[ch], tile[...], preferred_element_type=F32)
            for m in range(3):
                out = norm_turn(raw[m * rows : (m + 1) * rows], q_gain, *turn(ch, m))
                qst[ch, m, :, cols(h, hd)] = out * BF16(hd**-0.5)
        n_ring.free(t)

    def first_keys():
        wait_group(n_dev)
        send_keys(0)

    @pl.loop(0, 2)
    def _(ch):
        mlp(ch, lambda ch: pl.when(ch == 1)(first_keys))
        keys_and_values(ch)

    query(0)
    send_keys(1)
    pl.loop(1, nq)(query)
    for ch in range(2):
        for m in range(3):
            s = slot_of(ch, m)
            local(qst.at[ch, m], q_ref.at[s], qsem.at[s]).start()
    for ch in range(2):
        for m in range(3):
            s = slot_of(ch, m)
            keys.wait_sent(s, (kst.at[ch, m], vst.at[ch, m]))
            local(qst.at[ch, m], q_ref.at[s], qsem.at[s]).wait()
            local(y_at(ch, m), h_ref.at[s], hsem.at[s]).wait()
    keys.wait_mate(6)
    keys.wait_special()


def after_attention(layer, last, n_dev, cid, o, x, ln_w, w_o, w_gate, w_up, w_down, more=()):
    slots, rows, dim = x.shape
    inner, ff = w_o.shape[1], w_gate.shape[-1]
    total = slots * rows
    half = total // 2
    blocks = 16
    tn, tf = min(256, dim), min(768 if last and ff % 768 == 0 else 512, ff)
    deep = 3
    o2, x2 = o.reshape(total, inner), x.reshape(total, dim)
    work = [
        pltpu.VMEM((total, inner), BF16), pltpu.VMEM((total, dim), BF16),
        pltpu.VMEM((total, dim), BF16), pltpu.VMEM((2, half, dim), BF16),
        pltpu.VMEM((half, dim), F32), pltpu.VMEM((2, half, tf), BF16),
        pltpu.VMEM((deep, inner, tn), BF16), pltpu.VMEM((deep, dim, tf), BF16), pltpu.VMEM((deep, dim, tf), BF16),
        pltpu.VMEM((deep, tf, dim), BF16),
        DMA((2,)), DMA((deep,)), DMA((deep,)), DMA((deep,)), DMA((deep,)),
    ]
    params = pltpu.CompilerParams(collective_id=cid, has_side_effects=True, vmem_limit_bytes=VMEM_LIMIT)
    body = functools.partial(layer_kernel, layer, last, n_dev)
    if last:
        return pl.pallas_call(
            body,
            in_specs=[ANY, ANY, WHOLE] + [ANY] * 4,
            out_specs=ANY,
            out_shape=jax.ShapeDtypeStruct(x.shape, BF16),
            scratch_shapes=work + [pltpu.VMEM((3, rows, dim), BF16), DMA((3,)), DMA((3,)), DMA((3,)), DMA((slots,))],
            compiler_params=params,
        )(o2, x2, ln_w, w_o, w_gate, w_up, w_down)
    qk_w, trig, w_q, w_k, w_v = more
    hd = qk_w.shape[-1]
    nq, nk = w_q.shape[-1] // hd, w_k.shape[-1] // hd
    q_shape, kv_shape = (slots, rows, nq * hd), (blocks, rows, nk * hd)
    return pl.pallas_call(
        body,
        in_specs=[ANY, ANY, WHOLE, WHOLE, WHOLE] + [ANY] * 7,
        out_specs=[ANY] * 4,
        out_shape=[jax.ShapeDtypeStruct(a, BF16) for a in (x.shape, q_shape, kv_shape, kv_shape)],
        scratch_shapes=work + [
            pltpu.VMEM((4, dim, hd), BF16), DMA((4,)),
            pltpu.VMEM((2, 3, rows, nq * hd), BF16), pltpu.VMEM((2, 3, rows, nk * hd), BF16), pltpu.VMEM((2, 3, rows, nk * hd), BF16),
            pltpu.VMEM((2, 3, 2, rows, hd // 2), F32),
            DMA((slots,)), DMA((slots,)), DMA((2, 3, slots)), DMA((2, blocks)), DMA((2, 2)),
        ],
        compiler_params=params,
    )(o2, x2, ln_w, qk_w, trig, w_o, w_gate, w_up, w_down, w_k, w_v, w_q)


def rope_table(rows, blocks, hd):
    half = hd // 2
    pos = jnp.concatenate([jnp.arange(rows), rows * jnp.arange(blocks)]).astype(F32)
    out = []
    for base, scale in ((LOCAL_BASE, 1.0), (GLOBAL_BASE, GLOBAL_SCALE)):
        freq = base ** (-2.0 * jnp.arange(half, dtype=F32) / hd)
        ang = (pos / scale)[:, None] * freq[None, :]
        out.append(jnp.stack([jnp.cos(ang), jnp.sin(ang)]))
    return jnp.stack(out)


def solution(mesh):
    n_dev = mesh.shape["cp"]

    def device_fn(x_loc, ln_w, qk_w, w_q, w_k, w_v, w_o, w_gate, w_up, w_down):
        rows, hd = x_loc.shape[1], qk_w.shape[-1]
        trig = rope_table(rows, n_dev, hd)
        x, o = first(n_dev, WINDOW, x_loc, ln_w, qk_w, trig, w_q, w_k, w_v)
        mlp = (w_o, w_gate, w_up, w_down)
        x, q, k, v = after_attention(0, False, n_dev, 1, o, x, ln_w, *mlp, more=(qk_w, trig, w_q, w_k, w_v))
        o = attention(None, hd, q, k, v)
        return after_attention(1, True, n_dev, 2, o, x, ln_w, *mlp)

    act_part = P("dp", "cp", None)
    return jax.shard_map(device_fn, mesh=mesh, in_specs=(act_part,) + (P(),) * 9, out_specs=act_part, check_vma=False)
```
